32 devices in a mesh: uly: 2 (over y), blk: 16 (over z, x, core).
Axes of the slice: x: 2, y: 2, z: 4, core: 2. Of those that a mesh axis runs over, the one named last changes fastest.
Arguments:
- query_inputs: bfloat16 [4096, 2048], P(('blk', 'uly')), may hold values from -6 to 6
- key_inputs: bfloat16 [4096, 1024], P(('blk', 'uly')), may hold values from -6 to 6
- value_inputs: bfloat16 [4096, 1024], P(('blk', 'uly')), may hold values from -6 to 6
- forward_out: bfloat16 [4096, 2048], P(('blk', 'uly')), may hold values from -6 to 6
- output_gradient: bfloat16 [4096, 2048], P(('blk', 'uly')), may hold values from -4 to 4
- lse_parts: float32 [4096, 16, 2], P(('blk', 'uly')), may hold values from 3 to 247
- segment_ids: int32 [4096], P(('blk', 'uly')), may hold values from 0 to 31, never falling along the last dimension, each value on 1 to 512 neighbouring positions
Outputs:
- query_grad: bfloat16 [4096, 2048], P(('blk', 'uly'))
- key_grad: bfloat16 [4096, 1024], P(('blk', 'uly'))
- value_grad: bfloat16 [4096, 1024], P(('blk', 'uly'))
The draws below stay inside these ranges and needn't reach their ends.
Inputs may be any that keep to these rules, and one draw needn't show every extreme that they name: `segment_ids`: never falls along the sequence; every document holds 1 to 512 tokens, and some document exactly 512.
All inputs are finite; a program needn't handle non-finite values.
Results may differ from the reference program's by a relative error of at most 0.0051.
Values may be sent and summed in bfloat16 or wider, within the bound.
A program may use at most 128 MiB of HBM per device.

```python
import math
import jax
import jax.numpy as jnp
import numpy as np
from jax import lax

HEAD_SIZE = 128
QUERY_HEADS = 16
KEY_VALUE_HEADS = 8
QBLOCK = 512
SEQUENCE_TOKENS = 4096
DOCUMENT_LIMIT = 512
SEGS = 32


def draw_lse_parts(key, part):
    first_key = jax.random.fold_in(key, 0)
    shape_all = (SEQUENCE_TOKENS, QUERY_HEADS, 2)
    return jnp.clip(5.0 + 0.8 * jax.random.normal(first_key, shape_all, jnp.float32), 3.0, 7.0)


def shard_levels(key, dims, cuts, least, top_value):
    def one(dim, shards_of):
        draws = jax.random.uniform(jax.random.fold_in(jax.random.fold_in(key, 6), dim), (shards_of,), jnp.float32, least / len(cuts), top_value / len(cuts))
        return jnp.repeat(jnp.exp(draws), dims[dim] // shards_of).reshape((-1,) + (1,) * (len(dims) - dim - 1))

    loudness = one(*cuts[0])
    for cut in cuts[1:]:
        loudness = loudness * one(*cut)
    return loudness


def split_up(count, total, most, slope):
    loads = [(1 << 20) // math.isqrt(grade ** slope) + 1 for grade in range(2, count + 1)]
    rest, counts = total - most - (count - 1), [1] * (count - 1)
    while rest > 0:
        candidates = [i for i in range(count - 1) if counts[i] < most]
        pool, budget = sum([loads[i] for i in candidates]), rest
        for i in candidates:
            extra = min(most - counts[i], max(1, budget * loads[i] // pool), rest)
            counts[i] = counts[i] + extra
            rest = rest - extra
    return np.array([most] + counts)


def ragged_sizes(rng, number_of, total, bound, slope):
    if number_of == 2:
        one = jax.random.randint(rng, (), max(1, total - bound), min(bound, total - 1) + 1)
        return jnp.stack([one, total - one])
    sizes = jnp.asarray(split_up(number_of, total, bound, slope), jnp.int32)
    pairs = (number_of - 1) // 2
    donor, taker = sizes[1:1 + 2 * pairs:2], sizes[2:2 + 2 * pairs:2]
    room = jnp.minimum(donor - 1, bound - taker)
    passed = jax.random.randint(jax.random.fold_in(rng, 1), (pairs,), 0, 1 << 20) % (room + 1)
    sizes = sizes.at[1:1 + 2 * pairs:2].set(donor - passed).at[2:2 + 2 * pairs:2].set(taker + passed)
    return sizes[jax.random.permutation(jax.random.fold_in(rng, 2), number_of)]


def scatter_about(rng, extent, deviation, limit, cuts=(), kind=jnp.bfloat16):
    array = jax.random.normal(rng, extent, jnp.float32) * deviation
    if len(cuts) > 0:
        array = shard_levels(rng, extent, cuts, -0.22, 0.18) * array
    return jnp.clip(array, min=-limit, max=limit).astype(kind)


def setup_inputs(seed: int = 0) -> dict:
    keys = jax.random.split(jax.random.key(seed), 8)
    return {
        "query_inputs": scatter_about(keys[0], (SEQUENCE_TOKENS, QUERY_HEADS * HEAD_SIZE), 1.0, 6.0, ((0, 32),)),
        "key_inputs": scatter_about(keys[1], (SEQUENCE_TOKENS, KEY_VALUE_HEADS * HEAD_SIZE), 1.0, 6.0, ((0, 32),)),
        "value_inputs": scatter_about(keys[2], (SEQUENCE_TOKENS, KEY_VALUE_HEADS * HEAD_SIZE), 1.0, 6.0, ((0, 32),)),
        "forward_out": scatter_about(keys[3], (SEQUENCE_TOKENS, QUERY_HEADS * HEAD_SIZE), 0.5, 6.0, ((0, 32),)),
        "output_gradient": scatter_about(keys[4], (SEQUENCE_TOKENS, QUERY_HEADS * HEAD_SIZE), 0.25, 4.0, ((0, 32),)),
        "lse_parts": draw_lse_parts(jax.random.fold_in(keys[7], 71), 0),
        "segment_ids": jnp.searchsorted(jnp.cumsum(ragged_sizes(keys[6], SEGS, SEQUENCE_TOKENS, DOCUMENT_LIMIT, 2)), jnp.arange(SEQUENCE_TOKENS), side="right").astype(jnp.int32),
    }


def merge_parts(partials):
    highest = lax.optimization_barrier(jnp.max(partials, axis=-1))
    return highest + jnp.log(lax.optimization_barrier(jnp.sum(jnp.exp(partials - highest[..., None]), axis=-1)))

def round_trip(values_in):
    rounded = lax.optimization_barrier(values_in.astype(jnp.bfloat16))
    return rounded.astype(jnp.float32)

def reference(query_inputs, key_inputs, value_inputs, forward_out, output_gradient, lse_parts, segment_ids):
    token_count = query_inputs.shape[0]
    group_width = QUERY_HEADS // KEY_VALUE_HEADS
    score_scale = 1.0 / math.sqrt(HEAD_SIZE)
    rows_per_block = min(QBLOCK, token_count)
    lookback_span = DOCUMENT_LIMIT + rows_per_block
    logsumexp_rows = merge_parts(lse_parts)
    products = output_gradient.astype(jnp.float32) * forward_out.astype(jnp.float32)
    row_deltas = lax.optimization_barrier(jnp.sum(products.reshape(token_count, QUERY_HEADS, HEAD_SIZE), axis=-1))
    key_with_padding = jnp.pad(key_inputs, ((DOCUMENT_LIMIT, 0), (0, 0)))
    value_with_padding = jnp.pad(value_inputs, ((DOCUMENT_LIMIT, 0), (0, 0)))
    ids_padded = jnp.concatenate([jnp.full((DOCUMENT_LIMIT,), -1, jnp.int32), segment_ids.astype(jnp.int32)])

    def block_step(carried, block_index):
        key_gradient_running, value_gradient_running = carried
        leading_row = (block_index * rows_per_block).astype(jnp.int32)
        query_quad = lax.dynamic_slice_in_dim(query_inputs, leading_row, rows_per_block, 0).astype(jnp.float32).reshape(rows_per_block, KEY_VALUE_HEADS, group_width, HEAD_SIZE)
        gradient_quad = lax.dynamic_slice_in_dim(output_gradient, leading_row, rows_per_block, 0).astype(jnp.float32).reshape(rows_per_block, KEY_VALUE_HEADS, group_width, HEAD_SIZE)
        logsumexp_cube = lax.dynamic_slice_in_dim(logsumexp_rows, leading_row, rows_per_block, 0).reshape(rows_per_block, KEY_VALUE_HEADS, group_width).transpose(1, 2, 0)[..., None]
        delta_cube = lax.dynamic_slice_in_dim(row_deltas, leading_row, rows_per_block, 0).reshape(rows_per_block, KEY_VALUE_HEADS, group_width).transpose(1, 2, 0)[..., None]
        key_cube = lax.dynamic_slice_in_dim(key_with_padding, leading_row, lookback_span, 0).astype(jnp.float32).reshape(lookback_span, KEY_VALUE_HEADS, HEAD_SIZE)
        value_cube = lax.dynamic_slice_in_dim(value_with_padding, leading_row, lookback_span, 0).astype(jnp.float32).reshape(lookback_span, KEY_VALUE_HEADS, HEAD_SIZE)
        query_ids = lax.dynamic_slice_in_dim(segment_ids.astype(jnp.int32), leading_row, rows_per_block, 0)
        key_ids = lax.dynamic_slice_in_dim(ids_padded, leading_row, lookback_span, 0)
        query_pos = leading_row + DOCUMENT_LIMIT + jnp.arange(rows_per_block, dtype=jnp.int32)
        key_pos = leading_row + jnp.arange(lookback_span, dtype=jnp.int32)
        allowed = (key_pos[None, :] <= query_pos[:, None]) & (key_ids[None, :] == query_ids[:, None])
        scores = jnp.einsum('mhgd,nhd->hgmn', query_quad, key_cube) * score_scale
        weights = jnp.where(allowed, jnp.exp(scores - logsumexp_cube), 0.0)
        value_portion = jnp.einsum('hgmn,mhgd->nhd', round_trip(weights), gradient_quad)
        prob_grad = jnp.einsum('mhgd,nhd->hgmn', gradient_quad, value_cube)
        score_grad = round_trip(weights * (prob_grad - delta_cube))
        query_part = jnp.einsum('hgmn,nhd->mhgd', score_grad, key_cube) * score_scale
        key_portion = jnp.einsum('hgmn,mhgd->nhd', score_grad, query_quad) * score_scale
        key_window_rows = lax.dynamic_slice_in_dim(key_gradient_running, leading_row, lookback_span, 0) + key_portion.reshape(lookback_span, KEY_VALUE_HEADS * HEAD_SIZE)
        value_window_rows = lax.dynamic_slice_in_dim(value_gradient_running, leading_row, lookback_span, 0) + value_portion.reshape(lookback_span, KEY_VALUE_HEADS * HEAD_SIZE)
        key_gradient_running = lax.dynamic_update_slice_in_dim(key_gradient_running, key_window_rows, leading_row, 0)
        value_gradient_running = lax.dynamic_update_slice_in_dim(value_gradient_running, value_window_rows, leading_row, 0)
        return ((key_gradient_running, value_gradient_running), query_part.reshape(rows_per_block, QUERY_HEADS * HEAD_SIZE).astype(jnp.bfloat16))
    initial_running = (jnp.zeros((token_count + DOCUMENT_LIMIT, KEY_VALUE_HEADS * HEAD_SIZE), jnp.float32), jnp.zeros((token_count + DOCUMENT_LIMIT, KEY_VALUE_HEADS * HEAD_SIZE), jnp.float32))
    final_acc, query_blocks = lax.scan(block_step, initial_running, jnp.arange(token_count // rows_per_block, dtype=jnp.int32))
    query_grad = query_blocks.reshape(token_count, QUERY_HEADS * HEAD_SIZE)
    key_grad = final_acc[0][DOCUMENT_LIMIT:].astype(jnp.bfloat16)
    value_grad = final_acc[1][DOCUMENT_LIMIT:].astype(jnp.bfloat16)
    return (query_grad, key_grad, value_grad)
```

```python
import functools
import math

import jax
import jax.numpy as jnp
from jax import lax
from jax.experimental import pallas as pl
from jax.experimental.pallas import tpu as pltpu
from jax.sharding import PartitionSpec as P

HEAD_SIZE = 128
QUERY_HEADS = 16
KEY_VALUE_HEADS = 8
GROUP = QUERY_HEADS // KEY_VALUE_HEADS
TILE = 256
FAR = -1e30


def dot_nt(a, b):
    return lax.dot_general(a, b, (((1,), (1,)), ((), ())), preferred_element_type=jnp.float32)


def dot_nn(a, b):
    return lax.dot_general(a, b, (((1,), (0,)), ((), ())), preferred_element_type=jnp.float32)


def dot_tn(a, b):
    return lax.dot_general(a, b, (((0,), (0,)), ((), ())), preferred_element_type=jnp.float32)


def kernel(
    uly_count, blk_count,
    q_hbm, do_hbm, k_hbm, v_hbm, out_hbm, lp_hbm, ids_hbm,
    dq_ref, dkv_ref,
    qdb, kvb, statb, idb, bias,
    dqacc, acc0, acc2, dqs, ret1, ret2, in1, in2, dkvs,
    do_ref, kv_ref, out_ref, lp_ref, ids_ref, stat_ref,
    loc_sem,
    kv_s, kv_r, qd_s, qd_r, st_s, st_r, id_s, id_r,
    h2_s, h2_r, h2i_s, h2i_r, pt_s, pt_r, pti_s, pti_r,
    r1_s, r1_r, r2_s, r2_r, oq_s, oq_r, okv_s, okv_r,
):
    U, B = uly_count, blk_count
    T = q_hbm.shape[0]
    R = T * U
    KH = KEY_VALUE_HEADS // U
    D = HEAD_SIZE
    GD = GROUP * D
    G = KH * GROUP
    scale = 1.0 / math.sqrt(D)
    u = lax.axis_index("uly")
    b = lax.axis_index("blk")
    odd = lax.rem(b, 2)
    even = odd == 0
    mate = b + 1 - 2 * odd

    def at(blk, uly):
        return {"blk": blk, "uly": uly}

    def rcopy(src, dst, ssem, rsem, dev):
        return pltpu.make_async_remote_copy(
            src_ref=src, dst_ref=dst, send_sem=ssem, recv_sem=rsem,
            device_id=dev, device_id_type=pl.DeviceIdType.MESH,
        )

    def cols(first, width):
        return pl.ds(pl.multiple_of(first, 128), width)

    def rows(place):
        return pl.ds(pl.multiple_of(place * T, T), T)

    has_up2 = b + 2 < B
    has_down2 = b >= 2
    sends_mate = jnp.logical_or(even, b >= 3)

    def load(src, dst, sem):
        return pltpu.make_async_copy(src, dst, loc_sem.at[sem])

    own_cols = cols(u * KH * D, KH * D)
    own_kv = [
        load(src.at[:, own_cols], kvb.at[0, i, rows(u), :], 0)
        for i, src in enumerate((k_hbm, v_hbm))
    ]
    load_ids = load(ids_hbm, ids_ref, 1)
    load_kv = [load(src, kv_ref.at[i], 2) for i, src in enumerate((k_hbm, v_hbm))]
    load_do = load(do_hbm, do_ref, 3)
    load_out = load(out_hbm, out_ref, 4)
    load_lp = load(lp_hbm, lp_ref, 5)
    for copy in own_kv + [load_ids] + load_kv + [load_do, load_out, load_lp]:
        copy.start()

    barrier = pltpu.get_barrier_semaphore()
    for k in range(1, U):
        pl.semaphore_signal(
            barrier, inc=1, device_id=at(b, lax.rem(u + k, U)), device_id_type=pl.DeviceIdType.MESH
        )
    pl.semaphore_signal(barrier, inc=1, device_id=at(mate, u), device_id_type=pl.DeviceIdType.MESH)

    @pl.when(has_up2)
    def _():
        pl.semaphore_signal(
            barrier, inc=1, device_id=at(b + 2, u), device_id_type=pl.DeviceIdType.MESH
        )

    @pl.when(has_down2)
    def _():
        pl.semaphore_signal(
            barrier, inc=1, device_id=at(b - 2, u), device_id_type=pl.DeviceIdType.MESH
        )

    expected = U + has_up2.astype(jnp.int32) + has_down2.astype(jnp.int32)
    pl.semaphore_wait(barrier, expected)

    own_q = [
        load(src.at[:, cols(u * KH * GD, KH * GD)], qdb.at[i, rows(u), :], 6)
        for i, src in enumerate((q_hbm, do_hbm))
    ]
    own_id = load(ids_hbm, idb.at[0, u], 7)

    def id_in(k, place, dev):
        return rcopy(ids_ref, idb.at[0, place], id_s.at[k - 1], id_r.at[k - 1], dev)

    def st_in(k, place, peer, dev):
        return rcopy(stat_ref.at[peer], statb.at[place], st_s.at[k - 1], st_r.at[k - 1], dev)

    def kv_in(k, j, place, peer, dev):
        return rcopy(
            kv_ref.at[:, :, cols((peer * KH + j) * D, D)],
            kvb.at[0, :, rows(place), cols(j * D, D)],
            kv_s.at[k - 1], kv_r.at[j, k - 1], dev,
        )

    def qd_in(k, which, j, place, peer, dev):
        ref = (q_hbm, do_ref)[which]
        return rcopy(
            ref.at[:, cols((peer * KH + j) * GD, GD)],
            qdb.at[which, rows(place), cols(j * GD, GD)],
            qd_s.at[which, k - 1], qd_r.at[j, k - 1], dev,
        )

    def await_bytes(ref, sem):
        pltpu.make_async_copy(ref, ref, sem).wait()

    def h2(j, place):
        return rcopy(
            kvb.at[0, :, rows(place), cols(j * D, D)], kvb.at[2, :, rows(place), cols(j * D, D)],
            h2_s.at[0], h2_r.at[j], at(b + 2, u),
        )

    peers = [(k, lax.rem(u + k, U), lax.rem(u + U - k, U)) for k in range(1, U)]
    await_bytes(kvb.at[0, :, rows(u), :], loc_sem.at[0])

    @pl.when(has_up2)
    def _():
        for j in range(KH):
            h2(j, u).start()

    load_ids.wait()
    for k, to, _ in peers:
        id_in(k, u, at(b, to)).start()
    await_bytes(kv_ref, loc_sem.at[2])

    def send_kv(j):
        for k, to, _ in peers:
            kv_in(k, j, u, to, at(b, to)).start()

    def send_qd(j):
        for k, to, _ in peers:
            for which in range(2):
                qd_in(k, which, j, u, to, at(b, to)).start()

    for j in range(min(2, KH)):
        send_kv(j)
    for copy in [own_id] + own_q:
        copy.start()

    load_do.wait()
    load_out.wait()
    load_lp.wait()
    send_qd(0)
    lane = lax.broadcasted_iota(jnp.int32, (T, 128), 1)
    table = jnp.zeros((T, 128), jnp.float32)
    for h in range(U * G):
        piece = slice(h * D, (h + 1) * D)
        total = jnp.sum(
            do_ref[:, piece].astype(jnp.float32) * out_ref[:, piece].astype(jnp.float32),
            axis=1, keepdims=True,
        )
        table = jnp.where(lane == h, total, table)
    table = table.T
    part0, part1 = lp_ref[:, 0, :], lp_ref[:, 1, :]
    highest = jnp.maximum(part0, part1)
    lse_rows = highest + jnp.log(jnp.exp(part0 - highest) + jnp.exp(part1 - highest))
    for p in range(U):
        stat_ref[p, :G, :] = lse_rows[p * G:(p + 1) * G]
        stat_ref[p, G:2 * G, :] = table[p * G:(p + 1) * G]
    statb[u] = stat_ref[u]

    for k, to, _ in peers:
        st_in(k, u, to, at(b, to)).start()
    for j in range(2, KH):
        send_kv(j)
    for j in range(1, KH):
        send_qd(j)

    def h2id():
        return rcopy(idb.at[0], idb.at[2], h2i_s.at[0], h2i_r.at[0], at(b + 2, u))

    def pt(j):
        return rcopy(
            kvb.at[2 * odd, :, :, cols(j * D, D)], kvb.at[1, :, :, cols(j * D, D)],
            pt_s.at[0], pt_r.at[j], at(mate, u),
        )

    def ptid():
        return rcopy(idb.at[2 * odd], idb.at[1], pti_s.at[0], pti_r.at[0], at(mate, u))

    own_id.wait()
    for k, _, frm in peers:
        id_in(k, frm, at(b, frm)).wait_recv()

    @pl.when(has_up2)
    def _():
        h2id().start()

    @pl.when(even)
    def _():
        ptid().start()

    def forward(j):
        for k, _, frm in peers:
            kv_in(k, j, frm, frm, at(b, frm)).wait_recv()

        @pl.when(has_up2)
        def _():
            for k, _, frm in peers:
                h2(j, frm).start()

        @pl.when(even)
        def _():
            pt(j).start()

    def make_bias(hop):
        for kp in range(U):
            key_ids = jnp.broadcast_to(idb[hop, kp, 0:1, :].astype(jnp.float32), (T, T)).T
            for qp in range(U):
                query_ids = idb[0, qp, 0:1, :].astype(jnp.float32)
                good = key_ids == query_ids
                if hop == 0:
                    kpos = lax.broadcasted_iota(jnp.int32, (T, T), 0) + kp * T
                    qpos = lax.broadcasted_iota(jnp.int32, (T, T), 1) + qp * T
                    good = jnp.logical_and(good, kpos <= qpos)
                bias[hop, kp * T:(kp + 1) * T, qp * T:(qp + 1) * T] = jnp.where(good, 0.0, FAR)

    make_bias(0)
    forward(0)
    if KH > 1:
        forward(1)

    @pl.when(has_down2)
    def _():
        h2id().wait_recv()
        make_bias(2)

        @pl.when(odd == 1)
        def _():
            ptid().start()

    def arrive2(j):
        @pl.when(has_down2)
        def _():
            await_bytes(kvb.at[2, :, :, cols(j * D, D)], h2_r.at[j])

            @pl.when(odd == 1)
            def _():
                pt(j).start()

    @pl.when(b >= 1)
    def _():
        ptid().wait_recv()
        make_bias(1)

    await_bytes(qdb.at[:, rows(u), :], loc_sem.at[6])
    for k, _, frm in peers:
        st_in(k, frm, frm, at(b, frm)).wait_recv()
    if KH > 2:
        forward(2)
    arrive2(0)

    tile = min(TILE, R)
    steps = R // tile
    per = tile // T if tile >= T else 1

    def stat_row(row, qt):
        parts = [statb[qt * per + i, pl.ds(row, 1), :] for i in range(per)]
        return parts[0] if per == 1 else jnp.concatenate(parts, axis=1)

    def hop_grads(hop, j, acc):
        def key_step(kt, _):
            krow = pl.ds(pl.multiple_of(kt * tile, tile), tile)
            kc = kvb[hop, 0, krow, cols(j * D, D)]
            vc = kvb[hop, 1, krow, cols(j * D, D)]

            def query_step(qt, carry):
                dk, dv = carry
                qrow = pl.ds(pl.multiple_of(qt * tile, tile), tile)
                for g in range(GROUP):
                    qc = qdb[0, qrow, cols(j * GD + g * D, D)]
                    dc = qdb[1, qrow, cols(j * GD + g * D, D)]
                    head = j * GROUP + g
                    lse = stat_row(head, qt)
                    delta = stat_row(G + head, qt)
                    w = jnp.exp(dot_nt(kc, qc) * scale - lse + bias[hop, krow, qrow])
                    dv = dv + dot_nn(w.astype(jnp.bfloat16), dc)
                    ds = (w * (dot_nt(vc, dc) - delta)).astype(jnp.bfloat16)
                    dk = dk + dot_nn(ds, qc)
                    part = dot_tn(ds, kc)
                    dqacc[qrow, g * D:(g + 1) * D] += part
                return dk, dv

            zero = jnp.zeros((tile, D), jnp.float32)
            if steps == 1:
                dk, dv = query_step(0, (zero, zero))
            else:
                dk, dv = lax.fori_loop(0, steps, query_step, (zero, zero))
            acc[j, 0, krow, :] = (dk * scale).astype(acc.dtype)
            acc[j, 1, krow, :] = dv.astype(acc.dtype)
            return 0

        if steps == 1:
            key_step(0, 0)
        else:
            lax.fori_loop(0, steps, key_step, 0)

    def give1(j):
        return rcopy(ret1.at[j], in1.at[j], r1_s.at[0], r1_r.at[j], at(mate, u))

    def give2(j):
        return rcopy(ret2.at[j], in2.at[j], r2_s.at[0], r2_r.at[j], at(b - 2, u))

    def oq(k, j, place, dev):
        return rcopy(
            dqs.at[j, rows(place), :], dq_ref.at[:, cols((u * KH + j) * GD, GD)],
            oq_s.at[k - 1], oq_r.at[k - 1], dev,
        )

    def okv(k, j, place, dev):
        return rcopy(
            dkvs.at[j, :, rows(place), :], dkv_ref.at[:, :, cols((u * KH + j) * D, D)],
            okv_s.at[k - 1], okv_r.at[k - 1], dev,
        )

    def compute(j):
        for k, _, frm in peers:
            await_bytes(qdb.at[:, rows(frm), cols(j * GD, GD)], qd_r.at[j, k - 1])
        dqacc[...] = jnp.zeros_like(dqacc)

        @pl.when(b >= 1)
        def _():
            pt(j).wait_recv()
            hop_grads(1, j, ret1)
            give1(j).start()

        @pl.when(j + 3 < KH)
        def _():
            forward(jnp.minimum(j + 3, KH - 1))

        @pl.when(j + 1 < KH)
        def _():
            arrive2(jnp.minimum(j + 1, KH - 1))

        @pl.when(has_down2)
        def _():
            hop_grads(2, j, acc2)

        stage_a(j)
        hop_grads(0, j, acc0)

        dqs[j] = (dqacc[...] * scale).astype(jnp.bfloat16)
        for k, to, _ in peers:
            oq(k, j, to, at(b, to)).start()
        dq_ref[:, cols((u * KH + j) * GD, GD)] = dqs[j, rows(u), :]

    def stage_a(j):
        @pl.when(jnp.logical_and(odd == 1, has_down2))
        def _():
            give1(j).wait_recv()
            ret2[j] = (acc2[j] + in1[j].astype(jnp.float32)).astype(jnp.bfloat16)

        @pl.when(jnp.logical_and(even, has_down2))
        def _():
            ret2[j] = acc2[j].astype(jnp.bfloat16)

        @pl.when(has_down2)
        def _():
            give2(j).start()

    def stage_b(j):
        @pl.when(even)
        def _():
            give1(j).wait_recv()
            acc0[j] += in1[j].astype(jnp.float32)

        @pl.when(has_up2)
        def _():
            give2(j).wait_recv()
            acc0[j] += in2[j].astype(jnp.float32)

        dkvs[j] = acc0[j].astype(jnp.bfloat16)
        for k, to, _ in peers:
            okv(k, j, to, at(b, to)).start()
        dkv_ref[:, :, cols((u * KH + j) * D, D)] = dkvs[j, :, rows(u), :]

    def head_step(j, _):
        compute(j)

        @pl.when(j >= 2)
        def _():
            stage_b(jnp.maximum(j - 2, 0))

        return 0

    lax.fori_loop(0, KH, head_step, 0)
    if KH >= 2:
        stage_b(KH - 2)
    stage_b(KH - 1)

    for k, to, _ in peers:
        id_in(k, u, at(b, to)).wait_send()
        st_in(k, u, to, at(b, to)).wait_send()
        await_bytes(kv_ref.at[:, :, cols(to * KH * D, KH * D)], kv_s.at[k - 1])
        for which in range(2):
            await_bytes(qdb.at[which, rows(0), :], qd_s.at[which, k - 1])

    @pl.when(has_up2)
    def _():
        h2id().wait_send()
        await_bytes(kvb.at[0], h2_s.at[0])

    @pl.when(sends_mate)
    def _():
        ptid().wait_send()
        await_bytes(kvb.at[0], pt_s.at[0])

    @pl.when(b >= 1)
    def _():
        await_bytes(ret1, r1_s.at[0])

    @pl.when(has_down2)
    def _():
        await_bytes(ret2, r2_s.at[0])

    for k, to, frm in peers:
        await_bytes(dqs.at[:, rows(to), :], oq_s.at[k - 1])
        await_bytes(dkvs.at[:, :, rows(to), :], okv_s.at[k - 1])
        await_bytes(dq_ref.at[:, cols(frm * KH * GD, KH * GD)], oq_r.at[k - 1])
        await_bytes(dkv_ref.at[:, :, cols(frm * KH * D, KH * D)], okv_r.at[k - 1])


def close_kernel(q_in, kv_in, q_out, k_out, v_out, sem):
    half = q_in.shape[0] // 2
    moves = [
        (q_in.at[pl.ds(0, half)], q_out.at[pl.ds(0, half)]),
        (q_in.at[pl.ds(half, half)], q_out.at[pl.ds(half, half)]),
        (kv_in.at[0], k_out),
        (kv_in.at[1], v_out),
    ]
    copies = [pltpu.make_async_copy(src, dst, sem.at[i]) for i, (src, dst) in enumerate(moves)]
    for copy in copies:
        copy.start()
    for copy in copies:
        copy.wait()


def per_device(uly_count, blk_count, q, k, v, out, grad, lse_parts, segment_ids):
    U, B = uly_count, blk_count
    T = q.shape[0]
    R = T * U
    KH = KEY_VALUE_HEADS // U
    G = KH * GROUP
    D = HEAD_SIZE
    stat_rows = -(-2 * G // 8) * 8
    parts = lse_parts.transpose(1, 2, 0)
    ids = segment_ids.reshape(1, T)
    bf, f32 = jnp.bfloat16, jnp.float32
    n = max(U - 1, 1)
    dma = pltpu.SemaphoreType.DMA
    sems = []
    for send, recv in [
        ((n,), (KH, n)), ((2, n), (KH, n)), ((n,), (n,)), ((n,), (n,)),
        ((1,), (KH,)), ((1,), (1,)), ((1,), (KH,)), ((1,), (1,)),
        ((1,), (KH,)), ((1,), (KH,)), ((n,), (n,)), ((n,), (n,)),
    ]:
        sems += [dma(send), dma(recv)]
    vm = pltpu.VMEM
    in_vmem = pl.BlockSpec(memory_space=pltpu.VMEM)
    in_hbm = pl.BlockSpec(memory_space=pltpu.HBM)
    results = pl.pallas_call(
        functools.partial(kernel, U, B),
        out_shape=(vm(q.shape, bf), vm((2,) + k.shape, bf)),
        in_specs=[in_hbm] * 7,
        out_specs=(in_vmem, in_vmem),
        scratch_shapes=[
            vm((2, R, G * D), bf),
            vm((3, 2, R, KH * D), bf),
            vm((U, stat_rows, T), f32),
            vm((3, U, 1, T), jnp.int32),
            vm((3, R, R), f32),
            vm((R, GROUP * D), f32),
            vm((KH, 2, R, D), f32),
            vm((KH, 2, R, D), f32),
            vm((KH, R, GROUP * D), bf),
            vm((KH, 2, R, D), bf),
            vm((KH, 2, R, D), bf),
            vm((KH, 2, R, D), bf),
            vm((KH, 2, R, D), bf),
            vm((KH, 2, R, D), bf),
            vm(q.shape, bf),
            vm((2,) + k.shape, bf),
            vm(q.shape, bf),
            vm(parts.shape, f32),
            vm((1, T), jnp.int32),
            vm((U, stat_rows, T), f32),
            dma((8,)),
        ] + sems,
        compiler_params=pltpu.CompilerParams(
            collective_id=0, has_side_effects=True, vmem_limit_bytes=56 << 20
        ),
    )(q, grad, k, v, out, parts, ids)
    results = [pltpu.with_memory_space_constraint(r, pltpu.VMEM) for r in results]
    return pl.pallas_call(
        close_kernel,
        out_shape=tuple(jax.ShapeDtypeStruct(r.shape, r.dtype) for r in (q, k, v)),
        in_specs=[in_vmem] * 2,
        out_specs=(in_hbm,) * 3,
        scratch_shapes=[dma((4,))],
        compiler_params=pltpu.CompilerParams(vmem_limit_bytes=8 << 20),
    )(*results)


def solution(mesh):
    spec = P(("blk", "uly"), None)
    body = functools.partial(per_device, mesh.shape["uly"], mesh.shape["blk"])
    return jax.shard_map(
        body,
        mesh=mesh,
        in_specs=(spec, spec, spec, spec, spec, P(("blk", "uly"), None, None), P(("blk", "uly"))),
        out_specs=(spec, spec, spec),
        check_vma=False,
    )
```

```python
import functools
import math

import jax
import jax.numpy as jnp
from jax import lax
from jax.experimental import pallas as pl
from jax.experimental.pallas import tpu as pltpu
from jax.sharding import PartitionSpec as P

HEAD_SIZE = 128
QUERY_HEADS = 16
KEY_VALUE_HEADS = 8
GROUP = QUERY_HEADS // KEY_VALUE_HEADS
TILE = 256
FAR = -1e30
LOG2_E = math.log2(math.e)


def dot_nt(a, b):
    return lax.dot_general(a, b, (((1,), (1,)), ((), ())), preferred_element_type=jnp.float32)


def dot_nn(a, b):
    return lax.dot_general(a, b, (((1,), (0,)), ((), ())), preferred_element_type=jnp.float32)


def dot_tn(a, b):
    return lax.dot_general(a, b, (((0,), (0,)), ((), ())), preferred_element_type=jnp.float32)


def kernel(
    uly_count, blk_count,
    q_hbm, do_hbm, k_hbm, v_hbm, out_hbm, lp_hbm, ids_hbm,
    dq_ref, dkv_ref,
    qdb, kvb, statb, idb, bias,
    dqacc, acc0, acc2, dqs, ret1, ret2, in1, in2, dkvs,
    do_ref, kv_ref, out_ref, lp_ref, ids_ref, stat_ref,
    loc_sem, ready,
    kv_s, kv_r, qd_s, qd_r, st_s, st_r, id_s, id_r,
    h2_s, h2_r, h2i_s, h2i_r, pt_s, pt_r, pti_s, pti_r,
    r1_s, r1_r, r2_s, r2_r, oq_s, oq_r, okv_s, okv_r,
):
    U, B = uly_count, blk_count
    T = q_hbm.shape[0]
    R = T * U
    KH = KEY_VALUE_HEADS // U
    D = HEAD_SIZE
    GD = GROUP * D
    G = KH * GROUP
    scale = 1.0 / math.sqrt(D)
    u = lax.axis_index("uly")
    b = lax.axis_index("blk")
    odd = lax.rem(b, 2)
    even = odd == 0
    mate = b + 1 - 2 * odd

    def at(blk, uly):
        return {"blk": blk, "uly": uly}

    def rcopy(src, dst, ssem, rsem, dev):
        return pltpu.make_async_remote_copy(
            src_ref=src, dst_ref=dst, send_sem=ssem, recv_sem=rsem,
            device_id=dev, device_id_type=pl.DeviceIdType.MESH,
        )

    def cols(first, width):
        return pl.ds(pl.multiple_of(first, 128), width)

    def rows(place):
        return pl.ds(pl.multiple_of(place * T, T), T)

    has_up2 = b + 2 < B
    has_down2 = b >= 2
    sends_mate = jnp.logical_or(even, b >= 3)

    def load(src, dst, sem):
        return pltpu.make_async_copy(src, dst, loc_sem.at[sem])

    own_cols = cols(u * KH * D, KH * D)
    own_kv = [
        load(src.at[:, own_cols], kvb.at[0, i, rows(u), :], 0)
        for i, src in enumerate((k_hbm, v_hbm))
    ]
    load_ids = load(ids_hbm, ids_ref, 1)
    load_kv = [load(src, kv_ref.at[i], 2) for i, src in enumerate((k_hbm, v_hbm))]
    load_do = load(do_hbm, do_ref, 3)
    load_out = load(out_hbm, out_ref, 4)
    load_lp = load(lp_hbm, lp_ref, 5)
    for copy in own_kv + [load_ids] + load_kv + [load_do, load_out, load_lp]:
        copy.start()

    first = b < 2
    barrier = pltpu.get_barrier_semaphore()
    for k in range(1, U):
        pl.semaphore_signal(
            barrier, inc=1, device_id=at(b, lax.rem(u + k, U)), device_id_type=pl.DeviceIdType.MESH
        )
    pl.semaphore_signal(barrier, inc=1, device_id=at(mate, u), device_id_type=pl.DeviceIdType.MESH)

    @pl.when(has_up2)
    def _():
        pl.semaphore_signal(
            barrier, inc=1, device_id=at(b + 2, u), device_id_type=pl.DeviceIdType.MESH
        )

    @pl.when(b >= 4)
    def _():
        pl.semaphore_signal(
            barrier, inc=1, device_id=at(b - 2, u), device_id_type=pl.DeviceIdType.MESH
        )

    met_up2 = jnp.logical_and(has_up2, b >= 2)
    expected = U + has_down2.astype(jnp.int32) + met_up2.astype(jnp.int32)
    pl.semaphore_wait(barrier, expected)

    @pl.when(jnp.logical_and(has_down2, b < 4))
    def _():
        pl.semaphore_signal(
            ready, inc=1, device_id=at(b - 2, u), device_id_type=pl.DeviceIdType.MESH
        )

    own_q = [
        load(src.at[:, cols(u * KH * GD, KH * GD)], qdb.at[i, rows(u), :], 6)
        for i, src in enumerate((q_hbm, do_hbm))
    ]
    own_id = load(ids_hbm, idb.at[0, u], 7)

    def id_in(k, place, dev):
        return rcopy(ids_ref, idb.at[0, place], id_s.at[k - 1], id_r.at[k - 1], dev)

    def st_in(k, place, peer, dev):
        return rcopy(stat_ref.at[peer], statb.at[place], st_s.at[k - 1], st_r.at[k - 1], dev)

    def kv_in(k, j, place, peer, dev):
        return rcopy(
            kv_ref.at[:, :, cols((peer * KH + j) * D, D)],
            kvb.at[0, :, rows(place), cols(j * D, D)],
            kv_s.at[k - 1], kv_r.at[j, k - 1], dev,
        )

    def qd_in(k, which, j, place, peer, dev):
        ref = (q_hbm, do_ref)[which]
        return rcopy(
            ref.at[:, cols((peer * KH + j) * GD, GD)],
            qdb.at[which, rows(place), cols(j * GD, GD)],
            qd_s.at[which, k - 1], qd_r.at[j, k - 1], dev,
        )

    def await_bytes(ref, sem):
        pltpu.make_async_copy(ref, ref, sem).wait()

    def h2(j, place):
        return rcopy(
            kvb.at[0, :, rows(place), cols(j * D, D)], kvb.at[2, :, rows(place), cols(j * D, D)],
            h2_s.at[0], h2_r.at[j], at(b + 2, u),
        )

    peers = [(k, lax.rem(u + k, U), lax.rem(u + U - k, U)) for k in range(1, U)]
    await_bytes(kvb.at[0, :, rows(u), :], loc_sem.at[0])

    @pl.when(met_up2)
    def _():
        for j in range(KH):
            h2(j, u).start()

    load_ids.wait()
    for k, to, _ in peers:
        id_in(k, u, at(b, to)).start()
    await_bytes(kv_ref, loc_sem.at[2])

    def send_kv(j):
        for k, to, _ in peers:
            kv_in(k, j, u, to, at(b, to)).start()

    def send_qd(j):
        for k, to, _ in peers:
            for which in range(2):
                qd_in(k, which, j, u, to, at(b, to)).start()

    for j in range(min(2, KH)):
        send_kv(j)
    for copy in [own_id] + own_q:
        copy.start()

    load_do.wait()
    load_out.wait()
    load_lp.wait()
    send_qd(0)
    lane = lax.broadcasted_iota(jnp.int32, (T, 128), 1)
    table = jnp.zeros((T, 128), jnp.float32)
    for h in range(U * G):
        piece = slice(h * D, (h + 1) * D)
        total = jnp.sum(
            do_ref[:, piece].astype(jnp.float32) * out_ref[:, piece].astype(jnp.float32),
            axis=1, keepdims=True,
        )
        table = jnp.where(lane == h, total, table)
    table = table.T
    part0, part1 = lp_ref[:, 0, :], lp_ref[:, 1, :]
    highest = jnp.maximum(part0, part1)
    lse_rows = highest + jnp.log(jnp.exp(part0 - highest) + jnp.exp(part1 - highest))
    for p in range(U):
        stat_ref[p, :G, :] = lse_rows[p * G:(p + 1) * G] * LOG2_E
        stat_ref[p, G:2 * G, :] = table[p * G:(p + 1) * G]
    statb[u] = stat_ref[u]

    for k, to, _ in peers:
        st_in(k, u, to, at(b, to)).start()
    for j in range(2, KH):
        send_kv(j)
    for j in range(1, KH):
        send_qd(j)

    @pl.when(jnp.logical_and(first, has_up2))
    def _():
        pl.semaphore_wait(ready, 1)
        for j in range(KH):
            h2(j, u).start()

    def h2id():
        return rcopy(idb.at[0], idb.at[2], h2i_s.at[0], h2i_r.at[0], at(b + 2, u))

    def pt(j):
        return rcopy(
            kvb.at[2 * odd, :, :, cols(j * D, D)], kvb.at[1, :, :, cols(j * D, D)],
            pt_s.at[0], pt_r.at[j], at(mate, u),
        )

    def ptid():
        return rcopy(idb.at[2 * odd], idb.at[1], pti_s.at[0], pti_r.at[0], at(mate, u))

    own_id.wait()
    for k, _, frm in peers:
        id_in(k, frm, at(b, frm)).wait_recv()

    @pl.when(has_up2)
    def _():
        h2id().start()

    @pl.when(even)
    def _():
        ptid().start()

    def forward(j):
        for k, _, frm in peers:
            kv_in(k, j, frm, frm, at(b, frm)).wait_recv()

        @pl.when(has_up2)
        def _():
            for k, _, frm in peers:
                h2(j, frm).start()

        @pl.when(even)
        def _():
            pt(j).start()

    def make_bias(hop):
        for kp in range(U):
            key_ids = jnp.broadcast_to(idb[hop, kp, 0:1, :].astype(jnp.float32), (T, T)).T
            for qp in range(U):
                query_ids = idb[0, qp, 0:1, :].astype(jnp.float32)
                good = key_ids == query_ids
                if hop == 0:
                    kpos = lax.broadcasted_iota(jnp.int32, (T, T), 0) + kp * T
                    qpos = lax.broadcasted_iota(jnp.int32, (T, T), 1) + qp * T
                    good = jnp.logical_and(good, kpos <= qpos)
                bias[hop, kp * T:(kp + 1) * T, qp * T:(qp + 1) * T] = jnp.where(good, 0.0, FAR)

    make_bias(0)
    forward(0)
    if KH > 1:
        forward(1)

    @pl.when(has_down2)
    def _():
        h2id().wait_recv()
        make_bias(2)

        @pl.when(odd == 1)
        def _():
            ptid().start()

    def arrive2(j):
        @pl.when(has_down2)
        def _():
            await_bytes(kvb.at[2, :, :, cols(j * D, D)], h2_r.at[j])

            @pl.when(odd == 1)
            def _():
                pt(j).start()

    @pl.when(b >= 1)
    def _():
        ptid().wait_recv()
        make_bias(1)

    await_bytes(qdb.at[:, rows(u), :], loc_sem.at[6])
    for k, _, frm in peers:
        st_in(k, frm, frm, at(b, frm)).wait_recv()
    if KH > 2:
        forward(2)
    arrive2(0)

    tile = min(TILE, R)
    steps = R // tile
    per = tile // T if tile >= T else 1

    def stat_row(row, qt):
        parts = [statb[qt * per + i, pl.ds(row, 1), :] for i in range(per)]
        return parts[0] if per == 1 else jnp.concatenate(parts, axis=1)

    def hop_grads(hop, j, acc):
        def key_step(kt, _):
            krow = pl.ds(pl.multiple_of(kt * tile, tile), tile)
            kc = kvb[hop, 0, krow, cols(j * D, D)]
            vc = kvb[hop, 1, krow, cols(j * D, D)]

            def query_step(qt, carry):
                dk, dv = carry
                qrow = pl.ds(pl.multiple_of(qt * tile, tile), tile)
                heads = [cols(j * GD + g * D, D) for g in range(GROUP)]
                weights, score_grads = [], []
                for g in range(GROUP):
                    lse = stat_row(j * GROUP + g, qt)
                    delta = stat_row(G + j * GROUP + g, qt)
                    w = jnp.exp2(
                        dot_nt(kc, qdb[0, qrow, heads[g]]) * (scale * LOG2_E) - lse + bias[hop, krow, qrow]
                    )
                    ds = w * (dot_nt(vc, qdb[1, qrow, heads[g]]) - delta)
                    score_grads.append(ds.astype(jnp.bfloat16))
                    weights.append(w.astype(jnp.bfloat16))
                queries = jnp.concatenate([qdb[0, qrow, heads[g]] for g in range(GROUP)], axis=0)
                cotangents = jnp.concatenate([qdb[1, qrow, heads[g]] for g in range(GROUP)], axis=0)
                dv = dot_nn(jnp.concatenate(weights, axis=1), cotangents) + dv
                dk = dot_nn(jnp.concatenate(score_grads, axis=1), queries) + dk
                for g in range(GROUP):
                    dqacc[qrow, g * D:(g + 1) * D] += dot_tn(score_grads[g], kc)
                return dk, dv

            if steps == 1:
                dk, dv = query_step(0, (0.0, 0.0))
            else:
                zero = jnp.zeros((tile, D), jnp.float32)
                dk, dv = lax.fori_loop(0, steps, query_step, (zero, zero))
            acc[j, 0, krow, :] = (dk * scale).astype(acc.dtype)
            acc[j, 1, krow, :] = dv.astype(acc.dtype)
            return 0

        if steps == 1:
            key_step(0, 0)
        else:
            lax.fori_loop(0, steps, key_step, 0)

    def give1(j):
        return rcopy(ret1.at[j], in1.at[j], r1_s.at[0], r1_r.at[j], at(mate, u))

    def give2(j):
        return rcopy(ret2.at[j], in2.at[j], r2_s.at[0], r2_r.at[j], at(b - 2, u))

    def oq(k, j, place, dev):
        return rcopy(
            dqs.at[j, rows(place), :], dq_ref.at[:, cols((u * KH + j) * GD, GD)],
            oq_s.at[k - 1], oq_r.at[k - 1], dev,
        )

    def okv(k, j, place, dev):
        return rcopy(
            dkvs.at[j, :, rows(place), :], dkv_ref.at[:, :, cols((u * KH + j) * D, D)],
            okv_s.at[k - 1], okv_r.at[k - 1], dev,
        )

    def compute(j):
        for k, _, frm in peers:
            await_bytes(qdb.at[:, rows(frm), cols(j * GD, GD)], qd_r.at[j, k - 1])
        dqacc[...] = jnp.zeros_like(dqacc)

        @pl.when(b >= 1)
        def _():
            pt(j).wait_recv()
            hop_grads(1, j, ret1)
            give1(j).start()

        @pl.when(j + 3 < KH)
        def _():
            forward(jnp.minimum(j + 3, KH - 1))

        @pl.when(j + 1 < KH)
        def _():
            arrive2(jnp.minimum(j + 1, KH - 1))

        @pl.when(has_down2)
        def _():
            hop_grads(2, j, acc2)

        stage_a(j)
        hop_grads(0, j, acc0)

        dqs[j] = (dqacc[...] * scale).astype(jnp.bfloat16)
        for k, to, _ in peers:
            oq(k, j, to, at(b, to)).start()
        dq_ref[:, cols((u * KH + j) * GD, GD)] = dqs[j, rows(u), :]

    def stage_a(j):
        @pl.when(jnp.logical_and(odd == 1, has_down2))
        def _():
            give1(j).wait_recv()
            ret2[j] = (acc2[j] + in1[j].astype(jnp.float32)).astype(jnp.bfloat16)

        @pl.when(jnp.logical_and(even, has_down2))
        def _():
            ret2[j] = acc2[j].astype(jnp.bfloat16)

        @pl.when(has_down2)
        def _():
            give2(j).start()

    def stage_b(j):
        @pl.when(even)
        def _():
            give1(j).wait_recv()
            acc0[j] += in1[j].astype(jnp.float32)

        @pl.when(has_up2)
        def _():
            give2(j).wait_recv()
            acc0[j] += in2[j].astype(jnp.float32)

        dkvs[j] = acc0[j].astype(jnp.bfloat16)
        for k, to, _ in peers:
            okv(k, j, to, at(b, to)).start()
        dkv_ref[:, :, cols((u * KH + j) * D, D)] = dkvs[j, :, rows(u), :]

    def head_step(j, _):
        compute(j)

        @pl.when(j >= 2)
        def _():
            stage_b(jnp.maximum(j - 2, 0))

        return 0

    lax.fori_loop(0, KH, head_step, 0)
    if KH >= 2:
        stage_b(KH - 2)
    stage_b(KH - 1)

    for k, to, _ in peers:
        id_in(k, u, at(b, to)).wait_send()
        st_in(k, u, to, at(b, to)).wait_send()
        await_bytes(kv_ref.at[:, :, cols(to * KH * D, KH * D)], kv_s.at[k - 1])
        for which in range(2):
            await_bytes(qdb.at[which, rows(0), :], qd_s.at[which, k - 1])

    @pl.when(has_up2)
    def _():
        h2id().wait_send()
        await_bytes(kvb.at[0], h2_s.at[0])

    @pl.when(sends_mate)
    def _():
        ptid().wait_send()
        await_bytes(kvb.at[0], pt_s.at[0])

    @pl.when(b >= 1)
    def _():
        await_bytes(ret1, r1_s.at[0])

    @pl.when(has_down2)
    def _():
        await_bytes(ret2, r2_s.at[0])

    for k, to, frm in peers:
        await_bytes(dqs.at[:, rows(to), :], oq_s.at[k - 1])
        await_bytes(dkvs.at[:, :, rows(to), :], okv_s.at[k - 1])
        await_bytes(dq_ref.at[:, cols(frm * KH * GD, KH * GD)], oq_r.at[k - 1])
        await_bytes(dkv_ref.at[:, :, cols(frm * KH * D, KH * D)], okv_r.at[k - 1])


def close_kernel(q_in, kv_in, q_out, k_out, v_out, sem):
    half = q_in.shape[0] // 2
    moves = [
        (q_in.at[pl.ds(0, half)], q_out.at[pl.ds(0, half)]),
        (q_in.at[pl.ds(half, half)], q_out.at[pl.ds(half, half)]),
        (kv_in.at[0], k_out),
        (kv_in.at[1], v_out),
    ]
    copies = [pltpu.make_async_copy(src, dst, sem.at[i]) for i, (src, dst) in enumerate(moves)]
    for copy in copies:
        copy.start()
    for copy in copies:
        copy.wait()


def per_device(uly_count, blk_count, q, k, v, out, grad, lse_parts, segment_ids):
    U, B = uly_count, blk_count
    T = q.shape[0]
    R = T * U
    KH = KEY_VALUE_HEADS // U
    G = KH * GROUP
    D = HEAD_SIZE
    stat_rows = -(-2 * G // 8) * 8
    parts = lse_parts.transpose(1, 2, 0)
    ids = segment_ids.reshape(1, T)
    bf, f32 = jnp.bfloat16, jnp.float32
    n = max(U - 1, 1)
    dma = pltpu.SemaphoreType.DMA
    sems = []
    for send, recv in [
        ((n,), (KH, n)), ((2, n), (KH, n)), ((n,), (n,)), ((n,), (n,)),
        ((1,), (KH,)), ((1,), (1,)), ((1,), (KH,)), ((1,), (1,)),
        ((1,), (KH,)), ((1,), (KH,)), ((n,), (n,)), ((n,), (n,)),
    ]:
        sems += [dma(send), dma(recv)]
    vm = pltpu.VMEM
    in_vmem = pl.BlockSpec(memory_space=pltpu.VMEM)
    in_hbm = pl.BlockSpec(memory_space=pltpu.HBM)
    results = pl.pallas_call(
        functools.partial(kernel, U, B),
        out_shape=(vm(q.shape, bf), vm((2,) + k.shape, bf)),
        in_specs=[in_hbm] * 7,
        out_specs=(in_vmem, in_vmem),
        scratch_shapes=[
            vm((2, R, G * D), bf),
            vm((3, 2, R, KH * D), bf),
            vm((U, stat_rows, T), f32),
            vm((3, U, 1, T), jnp.int32),
            vm((3, R, R), f32),
            vm((R, GROUP * D), f32),
            vm((KH, 2, R, D), f32),
            vm((KH, 2, R, D), f32),
            vm((KH, R, GROUP * D), bf),
            vm((KH, 2, R, D), bf),
            vm((KH, 2, R, D), bf),
            vm((KH, 2, R, D), bf),
            vm((KH, 2, R, D), bf),
            vm((KH, 2, R, D), bf),
            vm(q.shape, bf),
            vm((2,) + k.shape, bf),
            vm(q.shape, bf),
            vm(parts.shape, f32),
            vm((1, T), jnp.int32),
            vm((U, stat_rows, T), f32),
            dma((8,)),
            pltpu.SemaphoreType.REGULAR,
        ] + sems,
        compiler_params=pltpu.CompilerParams(
            collective_id=0, has_side_effects=True, vmem_limit_bytes=56 << 20
        ),
    )(q, grad, k, v, out, parts, ids)
    results = [pltpu.with_memory_space_constraint(r, pltpu.VMEM) for r in results]
    return pl.pallas_call(
        close_kernel,
        out_shape=tuple(jax.ShapeDtypeStruct(r.shape, r.dtype) for r in (q, k, v)),
        in_specs=[in_vmem] * 2,
        out_specs=(in_hbm,) * 3,
        scratch_shapes=[dma((4,))],
        compiler_params=pltpu.CompilerParams(vmem_limit_bytes=8 << 20),
    )(*results)


def solution(mesh):
    spec = P(("blk", "uly"), None)
    body = functools.partial(per_device, mesh.shape["uly"], mesh.shape["blk"])
    return jax.shard_map(
        body,
        mesh=mesh,
        in_specs=(spec, spec, spec, spec, spec, P(("blk", "uly"), None, None), P(("blk", "uly"))),
        out_specs=(spec, spec, spec),
        check_vma=False,
    )
```

```python
import functools
import math

import jax
import jax.numpy as jnp
from jax import lax
from jax.experimental import pallas as pl
from jax.experimental.pallas import tpu as pltpu
from jax.sharding import PartitionSpec as P

HEAD_SIZE = 128
QUERY_HEADS = 16
KEY_VALUE_HEADS = 8
GROUP = QUERY_HEADS // KEY_VALUE_HEADS
TILE = 256
FAR = -1e30
LOG2_E = math.log2(math.e)


def dot_nt(a, b):
    return lax.dot_general(a, b, (((1,), (1,)), ((), ())), preferred_element_type=jnp.float32)


def dot_nn(a, b):
    return lax.dot_general(a, b, (((1,), (0,)), ((), ())), preferred_element_type=jnp.float32)


def dot_tn(a, b):
    return lax.dot_general(a, b, (((0,), (0,)), ((), ())), preferred_element_type=jnp.float32)


def kernel(
    uly_count, blk_count,
    q_hbm, do_hbm, k_hbm, v_hbm, out_hbm, lp_hbm, ids_hbm,
    dq_ref, dkv_ref,
    qdb, kvb, statb, idb, bias,
    dqacc, acc0, acc2, dqs, ret1, ret2, in1, in2, dkvs,
    do_ref, kv_ref, out_ref, lp_ref, ids_ref, stat_ref,
    q_ref, kx, loc1, part, px, dqt,
    loc_sem, ready, kx_s, kx_r, px_s, px_r,
    kv_s, kv_r, qd_s, qd_r, st_s, st_r, id_s, id_r,
    h2_s, h2_r, h2i_s, h2i_r, pt_s, pt_r, pti_s, pti_r,
    r1_s, r1_r, r2_s, r2_r, oq_s, oq_r, okv_s, okv_r,
):
    U, B = uly_count, blk_count
    T = q_hbm.shape[0]
    R = T * U
    KH = KEY_VALUE_HEADS // U
    D = HEAD_SIZE
    GD = GROUP * D
    G = KH * GROUP
    scale = 1.0 / math.sqrt(D)
    u = lax.axis_index("uly")
    b = lax.axis_index("blk")
    odd = lax.rem(b, 2)
    even = odd == 0
    mate = b + 1 - 2 * odd

    def at(blk, uly):
        return {"blk": blk, "uly": uly}

    def rcopy(src, dst, ssem, rsem, dev):
        return pltpu.make_async_remote_copy(
            src_ref=src, dst_ref=dst, send_sem=ssem, recv_sem=rsem,
            device_id=dev, device_id_type=pl.DeviceIdType.MESH,
        )

    def cols(first, width):
        return pl.ds(pl.multiple_of(first, 128), width)

    def rows(place):
        return pl.ds(pl.multiple_of(place * T, T), T)

    has_up2 = b + 2 < B
    has_down2 = b >= 2
    sends_mate = jnp.logical_or(even, b >= 3)

    def load(src, dst, sem):
        return pltpu.make_async_copy(src, dst, loc_sem.at[sem])

    own_cols = cols(u * KH * D, KH * D)
    own_kv = [
        load(src.at[:, own_cols], kvb.at[0, i, rows(u), :], 0)
        for i, src in enumerate((k_hbm, v_hbm))
    ]
    load_ids = load(ids_hbm, ids_ref, 1)
    load_kv = [load(src, kv_ref.at[i], 2) for i, src in enumerate((k_hbm, v_hbm))]
    load_do = load(do_hbm, do_ref, 3)
    load_out = load(out_hbm, out_ref, 4)
    load_lp = load(lp_hbm, lp_ref, 5)
    for copy in load_kv + [load_ids] + own_kv + [load_do, load_out, load_lp]:
        copy.start()

    first = b < 2
    alone = jnp.logical_and(b == 0, U == 2)
    grouped = jnp.logical_not(alone)
    barrier = pltpu.get_barrier_semaphore()
    for k in range(1, U):
        pl.semaphore_signal(
            barrier, inc=1, device_id=at(b, lax.rem(u + k, U)), device_id_type=pl.DeviceIdType.MESH
        )
    pl.semaphore_signal(barrier, inc=1, device_id=at(mate, u), device_id_type=pl.DeviceIdType.MESH)

    @pl.when(has_up2)
    def _():
        pl.semaphore_signal(
            barrier, inc=1, device_id=at(b + 2, u), device_id_type=pl.DeviceIdType.MESH
        )

    @pl.when(b >= 4)
    def _():
        pl.semaphore_signal(
            barrier, inc=1, device_id=at(b - 2, u), device_id_type=pl.DeviceIdType.MESH
        )

    met_up2 = jnp.logical_and(has_up2, b >= 2)
    expected = U + has_down2.astype(jnp.int32) + met_up2.astype(jnp.int32)
    pl.semaphore_wait(barrier, expected)

    @pl.when(jnp.logical_and(has_down2, b < 4))
    def _():
        pl.semaphore_signal(
            ready, inc=1, device_id=at(b - 2, u), device_id_type=pl.DeviceIdType.MESH
        )

    own_q = [
        load(src.at[:, cols(u * KH * GD, KH * GD)], qdb.at[i, rows(u), :], 6)
        for i, src in enumerate((q_hbm, do_hbm))
    ]
    own_id = load(ids_hbm, idb.at[0, u], 7)
    load_q = load(q_hbm, q_ref, 6)

    def id_in(k, place, dev):
        return rcopy(ids_ref, idb.at[0, place], id_s.at[k - 1], id_r.at[k - 1], dev)

    def st_in(k, place, peer, dev):
        return rcopy(stat_ref.at[peer], statb.at[place], st_s.at[k - 1], st_r.at[k - 1], dev)

    def kv_in(k, j, place, peer, dev):
        return rcopy(
            kv_ref.at[:, :, cols((peer * KH + j) * D, D)],
            kvb.at[0, :, rows(place), cols(j * D, D)],
            kv_s.at[k - 1], kv_r.at[j, k - 1], dev,
        )

    def qd_in(k, which, j, place, peer, dev):
        ref = (q_hbm, do_ref)[which]
        return rcopy(
            ref.at[:, cols((peer * KH + j) * GD, GD)],
            qdb.at[which, rows(place), cols(j * GD, GD)],
            qd_s.at[which, k - 1], qd_r.at[j, k - 1], dev,
        )

    def await_bytes(ref, sem):
        pltpu.make_async_copy(ref, ref, sem).wait()

    def h2(j, place):
        return rcopy(
            kvb.at[0, :, rows(place), cols(j * D, D)], kvb.at[2, :, rows(place), cols(j * D, D)],
            h2_s.at[0], h2_r.at[j], at(b + 2, u),
        )

    peers = [(k, lax.rem(u + k, U), lax.rem(u + U - k, U)) for k in range(1, U)]
    await_bytes(kvb.at[0, :, rows(u), :], loc_sem.at[0])

    @pl.when(met_up2)
    def _():
        for j in range(KH):
            h2(j, u).start()

    load_ids.wait()
    for k, to, _ in peers:
        id_in(k, u, at(b, to)).start()
    await_bytes(kv_ref, loc_sem.at[2])

    def send_kv(j):
        for k, to, _ in peers:
            kv_in(k, j, u, to, at(b, to)).start()

    def send_qd(j):
        for k, to, _ in peers:
            for which in range(2):
                qd_in(k, which, j, u, to, at(b, to)).start()

    for j in range(min(2, KH)):
        send_kv(j)
    own_id.start()

    @pl.when(grouped)
    def _():
        for copy in own_q:
            copy.start()

    @pl.when(alone)
    def _():
        load_q.start()

    load_do.wait()
    load_out.wait()
    load_lp.wait()

    @pl.when(grouped)
    def _():
        send_qd(0)

    lane = lax.broadcasted_iota(jnp.int32, (T, 128), 1)
    table = jnp.zeros((T, 128), jnp.float32)
    for h in range(U * G):
        piece = slice(h * D, (h + 1) * D)
        total = jnp.sum(
            do_ref[:, piece].astype(jnp.float32) * out_ref[:, piece].astype(jnp.float32),
            axis=1, keepdims=True,
        )
        table = jnp.where(lane == h, total, table)
    table = table.T
    part0, part1 = lp_ref[:, 0, :], lp_ref[:, 1, :]
    highest = jnp.maximum(part0, part1)
    lse_rows = highest + jnp.log(jnp.exp(part0 - highest) + jnp.exp(part1 - highest))
    for p in range(U):
        stat_ref[p, :G, :] = lse_rows[p * G:(p + 1) * G] * LOG2_E
        stat_ref[p, G:2 * G, :] = table[p * G:(p + 1) * G]
    statb[u] = stat_ref[u]

    @pl.when(grouped)
    def _():
        for k, to, _ in peers:
            st_in(k, u, to, at(b, to)).start()

    for j in range(2, KH):
        send_kv(j)

    @pl.when(grouped)
    def _():
        for j in range(1, KH):
            send_qd(j)

    def kx_in():
        return rcopy(kv_ref.at[:, :, pl.ds(0, KH * D)], kx, kx_s.at[0], kx_r.at[0], at(b, 1 - u))

    def px_in():
        return rcopy(part, px, px_s.at[0], px_r.at[0], at(b, 1 - u))

    @pl.when(jnp.logical_and(alone, u == 0))
    def _():
        kx_in().start()

    @pl.when(jnp.logical_and(first, has_up2))
    def _():
        pl.semaphore_wait(ready, 1)
        for j in range(KH):
            h2(j, u).start()

    def h2id():
        return rcopy(idb.at[0], idb.at[2], h2i_s.at[0], h2i_r.at[0], at(b + 2, u))

    def pt(j):
        return rcopy(
            kvb.at[2 * odd, :, :, cols(j * D, D)], kvb.at[1, :, :, cols(j * D, D)],
            pt_s.at[0], pt_r.at[j], at(mate, u),
        )

    def ptid():
        return rcopy(idb.at[2 * odd], idb.at[1], pti_s.at[0], pti_r.at[0], at(mate, u))

    own_id.wait()
    for k, _, frm in peers:
        id_in(k, frm, at(b, frm)).wait_recv()

    @pl.when(has_up2)
    def _():
        h2id().start()

    @pl.when(even)
    def _():
        ptid().start()

    def forward(j):
        for k, _, frm in peers:
            kv_in(k, j, frm, frm, at(b, frm)).wait_recv()

        @pl.when(has_up2)
        def _():
            for k, _, frm in peers:
                h2(j, frm).start()

        @pl.when(even)
        def _():
            pt(j).start()

    def make_bias(hop):
        for kp in range(U):
            key_ids = jnp.broadcast_to(idb[hop, kp, 0:1, :].astype(jnp.float32), (T, T)).T
            for qp in range(U):
                query_ids = idb[0, qp, 0:1, :].astype(jnp.float32)
                good = key_ids == query_ids
                if hop == 0:
                    kpos = lax.broadcasted_iota(jnp.int32, (T, T), 0) + kp * T
                    qpos = lax.broadcasted_iota(jnp.int32, (T, T), 1) + qp * T
                    good = jnp.logical_and(good, kpos <= qpos)
                bias[hop, kp * T:(kp + 1) * T, qp * T:(qp + 1) * T] = jnp.where(good, 0.0, FAR)

    make_bias(0)
    forward(0)
    if KH > 1:
        forward(1)

    @pl.when(has_down2)
    def _():
        h2id().wait_recv()
        make_bias(2)

        @pl.when(odd == 1)
        def _():
            ptid().start()

    def arrive2(j):
        @pl.when(has_down2)
        def _():
            await_bytes(kvb.at[2, :, :, cols(j * D, D)], h2_r.at[j])

            @pl.when(odd == 1)
            def _():
                pt(j).start()

    @pl.when(b >= 1)
    def _():
        ptid().wait_recv()
        make_bias(1)

    @pl.when(grouped)
    def _():
        await_bytes(qdb.at[:, rows(u), :], loc_sem.at[6])
        for k, _, frm in peers:
            st_in(k, frm, frm, at(b, frm)).wait_recv()

    if KH > 2:
        forward(2)
    arrive2(0)

    tile = min(TILE, R)
    steps = R // tile
    per = tile // T if tile >= T else 1

    def stat_row(row, qt):
        parts = [statb[qt * per + i, pl.ds(row, 1), :] for i in range(per)]
        return parts[0] if per == 1 else jnp.concatenate(parts, axis=1)

    def hop_grads(hop, j, acc):
        def key_step(kt, _):
            krow = pl.ds(pl.multiple_of(kt * tile, tile), tile)
            kc = kvb[hop, 0, krow, cols(j * D, D)]
            vc = kvb[hop, 1, krow, cols(j * D, D)]

            def query_step(qt, carry):
                dk, dv = carry
                qrow = pl.ds(pl.multiple_of(qt * tile, tile), tile)
                heads = [cols(j * GD + g * D, D) for g in range(GROUP)]
                weights, score_grads = [], []
                for g in range(GROUP):
                    lse = stat_row(j * GROUP + g, qt)
                    delta = stat_row(G + j * GROUP + g, qt)
                    w = jnp.exp2(
                        dot_nt(kc, qdb[0, qrow, heads[g]]) * (scale * LOG2_E) - lse + bias[hop, krow, qrow]
                    )
                    ds = w * (dot_nt(vc, qdb[1, qrow, heads[g]]) - delta)
                    score_grads.append(ds.astype(jnp.bfloat16))
                    weights.append(w.astype(jnp.bfloat16))
                queries = jnp.concatenate([qdb[0, qrow, heads[g]] for g in range(GROUP)], axis=0)
                cotangents = jnp.concatenate([qdb[1, qrow, heads[g]] for g in range(GROUP)], axis=0)
                dv = dot_nn(jnp.concatenate(weights, axis=1), cotangents) + dv
                dk = dot_nn(jnp.concatenate(score_grads, axis=1), queries) + dk
                for g in range(GROUP):
                    dqacc[qrow, g * D:(g + 1) * D] += dot_tn(score_grads[g], kc)
                return dk, dv

            if steps == 1:
                dk, dv = query_step(0, (0.0, 0.0))
            else:
                zero = jnp.zeros((tile, D), jnp.float32)
                dk, dv = lax.fori_loop(0, steps, query_step, (zero, zero))
            acc[j, 0, krow, :] = (dk * scale).astype(acc.dtype)
            acc[j, 1, krow, :] = dv.astype(acc.dtype)
            return 0

        if steps == 1:
            key_step(0, 0)
        else:
            lax.fori_loop(0, steps, key_step, 0)

    def give1(j):
        return rcopy(ret1.at[j], in1.at[j], r1_s.at[0], r1_r.at[j], at(mate, u))

    def give2(j):
        return rcopy(ret2.at[j], in2.at[j], r2_s.at[0], r2_r.at[j], at(b - 2, u))

    def straight(j, place):
        return rcopy(
            ret2.at[j, :, rows(place), :], in2.at[j, :, rows(u), :],
            r2_s.at[0], r2_r.at[j], at(0, place),
        )

    def oq(k, j, place, dev):
        return rcopy(
            dqs.at[j, rows(place), :], dq_ref.at[:, cols((u * KH + j) * GD, GD)],
            oq_s.at[k - 1], oq_r.at[k - 1], dev,
        )

    def okv(k, j, place, dev):
        return rcopy(
            dkvs.at[j, :, rows(place), :], dkv_ref.at[:, :, cols((u * KH + j) * D, D)],
            okv_s.at[k - 1], okv_r.at[k - 1], dev,
        )

    def compute(j):
        for k, _, frm in peers:
            await_bytes(qdb.at[:, rows(frm), cols(j * GD, GD)], qd_r.at[j, k - 1])
        dqacc[...] = jnp.zeros_like(dqacc)

        @pl.when(b >= 1)
        def _():
            pt(j).wait_recv()
            hop_grads(1, j, ret1)
            give1(j).start()

        @pl.when(j + 3 < KH)
        def _():
            forward(jnp.minimum(j + 3, KH - 1))

        @pl.when(j + 1 < KH)
        def _():
            arrive2(jnp.minimum(j + 1, KH - 1))

        @pl.when(has_down2)
        def _():
            hop_grads(2, j, acc2)

        stage_a(j)
        hop_grads(0, j, acc0)

        dqs[j] = (dqacc[...] * scale).astype(jnp.bfloat16)
        for k, to, _ in peers:
            oq(k, j, to, at(b, to)).start()
        dq_ref[:, cols((u * KH + j) * GD, GD)] = dqs[j, rows(u), :]

    def stage_a(j):
        @pl.when(jnp.logical_and(odd == 1, has_down2))
        def _():
            give1(j).wait_recv()
            ret2[j] = (acc2[j] + in1[j].astype(jnp.float32)).astype(jnp.bfloat16)

        @pl.when(jnp.logical_and(even, has_down2))
        def _():
            ret2[j] = acc2[j].astype(jnp.bfloat16)

        to_alone = jnp.logical_and(b == 2, U == 2)

        @pl.when(jnp.logical_and(has_down2, jnp.logical_not(to_alone)))
        def _():
            give2(j).start()

        @pl.when(to_alone)
        def _():
            straight(j, u).start()
            straight(j, 1 - u).start()

    def stage_b(j):
        @pl.when(even)
        def _():
            give1(j).wait_recv()
            acc0[j] += in1[j].astype(jnp.float32)

        @pl.when(has_up2)
        def _():
            give2(j).wait_recv()
            acc0[j] += in2[j].astype(jnp.float32)

        dkvs[j] = acc0[j].astype(jnp.bfloat16)
        for k, to, _ in peers:
            okv(k, j, to, at(b, to)).start()
        dkv_ref[:, :, cols((u * KH + j) * D, D)] = dkvs[j, :, rows(u), :]

    def head_step(j, _):
        compute(j)

        @pl.when(j >= 2)
        def _():
            stage_b(jnp.maximum(j - 2, 0))

        return 0

    def alone_block(h, kc, vc, mask):
        heads = [cols(h * GD + g * D, D) for g in range(GROUP)]
        plane = h // KH
        row = (h - plane * KH) * GROUP
        weights, score_grads = [], []
        for g in range(GROUP):
            lse = stat_ref[plane, pl.ds(row + g, 1), :]
            delta = stat_ref[plane, pl.ds(G + row + g, 1), :]
            w = jnp.exp2(dot_nt(kc, q_ref[:, heads[g]]) * (scale * LOG2_E) - lse + mask)
            ds = w * (dot_nt(vc, do_ref[:, heads[g]]) - delta)
            score_grads.append(ds.astype(jnp.bfloat16))
            weights.append(w.astype(jnp.bfloat16))
        queries = jnp.concatenate([q_ref[:, c] for c in heads], axis=0)
        cotangents = jnp.concatenate([do_ref[:, c] for c in heads], axis=0)
        dv = dot_nn(jnp.concatenate(weights, axis=1), cotangents)
        dk = dot_nn(jnp.concatenate(score_grads, axis=1), queries) * scale
        return dk, dv, [dot_tn(ds, kc) * scale for ds in score_grads]

    def alone_step(j, _):
        for side in range(2):
            plane = u if side == 0 else 1 - u
            h = plane * KH + j
            head = cols(h * D, D)
            dk, dv, dq = alone_block(
                h, kv_ref[0, :, head], kv_ref[1, :, head], bias[0, rows(u), rows(u)]
            )
            for g in range(GROUP):
                dqt[:, g * D:(g + 1) * D] = dq[g]
            if side == 0:
                acc0[j, 0, rows(u), :] = dk
                acc0[j, 1, rows(u), :] = dv
            else:
                loc1[j, 0] = dk
                loc1[j, 1] = dv

            @pl.when(u == 1)
            def _():
                if side == 0:
                    near = cols(j * D, D)
                    kc, vc = kvb[0, 0, rows(0), near], kvb[0, 1, rows(0), near]
                else:
                    kc, vc = kx[0, :, head], kx[1, :, head]
                dk, dv, dq = alone_block(h, kc, vc, bias[0, rows(0), rows(1)])
                for g in range(GROUP):
                    dqt[:, g * D:(g + 1) * D] += dq[g]
                if side == 0:
                    acc0[j, 0, rows(0), :] = dk
                    acc0[j, 1, rows(0), :] = dv
                else:
                    part[j, 0] = dk.astype(jnp.bfloat16)
                    part[j, 1] = dv.astype(jnp.bfloat16)

            if side == 0:
                @pl.when(u == 0)
                def _():
                    acc0[j, :, rows(1), :] = jnp.zeros((2, T, D), jnp.float32)

            dq_ref[:, cols(h * GD, GD)] = dqt[...].astype(jnp.bfloat16)
        return 0

    def alone_merge(j, _):
        give1(j).wait_recv()
        acc0[j] += in1[j].astype(jnp.float32)
        dkvs[j] = acc0[j].astype(jnp.bfloat16)
        okv(1, j, 1 - u, at(b, 1 - u)).start()
        return 0

    def alone_finish(j, _):
        mine = cols((u * KH + j) * D, D)
        other = cols(((1 - u) * KH + j) * D, D)

        @pl.when(has_up2)
        def _():
            await_bytes(in2.at[j], r2_r.at[j])
            acc0[j, :, rows(u), :] += in2[j, :, rows(u), :].astype(jnp.float32)
            loc1[j] += in2[j, :, rows(1 - u), :].astype(jnp.float32)

        dkv_ref[:, :, mine] = acc0[j, :, rows(u), :].astype(jnp.bfloat16)
        dkv_ref[:, :, other] = (dkv_ref[:, :, other].astype(jnp.float32) + loc1[j]).astype(jnp.bfloat16)
        return 0

    @pl.when(grouped)
    def _():
        lax.fori_loop(0, KH, head_step, 0)
        if KH >= 2:
            stage_b(KH - 2)
        stage_b(KH - 1)

    if U == 2:
        @pl.when(alone)
        def _():
            load_q.wait()
            for j in range(3, KH):
                forward(j)

            @pl.when(u == 1)
            def _():
                kx_in().wait_recv()

            lax.fori_loop(0, KH, alone_step, 0)

            @pl.when(u == 1)
            def _():
                px_in().start()

            @pl.when(u == 0)
            def _():
                px_in().wait_recv()
                for j in range(KH):
                    acc0[j, :, rows(0), :] += px[j].astype(jnp.float32)

            lax.fori_loop(0, KH, alone_merge, 0)
            await_bytes(dkv_ref.at[:, :, cols((1 - u) * KH * D, KH * D)], okv_r.at[0])
            lax.fori_loop(0, KH, alone_finish, 0)

            @pl.when(u == 0)
            def _():
                kx_in().wait_send()

            @pl.when(u == 1)
            def _():
                px_in().wait_send()

    for k, to, _ in peers:
        id_in(k, u, at(b, to)).wait_send()
        await_bytes(kv_ref.at[:, :, cols(to * KH * D, KH * D)], kv_s.at[k - 1])

    @pl.when(grouped)
    def _():
        for k, to, _ in peers:
            st_in(k, u, to, at(b, to)).wait_send()
            for which in range(2):
                await_bytes(qdb.at[which, rows(0), :], qd_s.at[which, k - 1])

    @pl.when(has_up2)
    def _():
        h2id().wait_send()
        await_bytes(kvb.at[0], h2_s.at[0])

    @pl.when(sends_mate)
    def _():
        ptid().wait_send()
        await_bytes(kvb.at[0], pt_s.at[0])

    @pl.when(b >= 1)
    def _():
        await_bytes(ret1, r1_s.at[0])

    @pl.when(has_down2)
    def _():
        await_bytes(ret2, r2_s.at[0])

    for k, to, _ in peers:
        await_bytes(dkvs.at[:, :, rows(to), :], okv_s.at[k - 1])

    @pl.when(grouped)
    def _():
        for k, to, frm in peers:
            await_bytes(dqs.at[:, rows(to), :], oq_s.at[k - 1])
            await_bytes(dq_ref.at[:, cols(frm * KH * GD, KH * GD)], oq_r.at[k - 1])
            await_bytes(dkv_ref.at[:, :, cols(frm * KH * D, KH * D)], okv_r.at[k - 1])


def close_kernel(q_in, kv_in, q_out, k_out, v_out, sem):
    half = q_in.shape[0] // 2
    moves = [
        (q_in.at[pl.ds(0, half)], q_out.at[pl.ds(0, half)]),
        (q_in.at[pl.ds(half, half)], q_out.at[pl.ds(half, half)]),
        (kv_in.at[0], k_out),
        (kv_in.at[1], v_out),
    ]
    copies = [pltpu.make_async_copy(src, dst, sem.at[i]) for i, (src, dst) in enumerate(moves)]
    for copy in copies:
        copy.start()
    for copy in copies:
        copy.wait()


def per_device(uly_count, blk_count, q, k, v, out, grad, lse_parts, segment_ids):
    U, B = uly_count, blk_count
    T = q.shape[0]
    R = T * U
    KH = KEY_VALUE_HEADS // U
    G = KH * GROUP
    D = HEAD_SIZE
    GD = GROUP * D
    stat_rows = -(-2 * G // 8) * 8
    parts = lse_parts.transpose(1, 2, 0)
    ids = segment_ids.reshape(1, T)
    bf, f32 = jnp.bfloat16, jnp.float32
    n = max(U - 1, 1)
    dma = pltpu.SemaphoreType.DMA
    sems = []
    for send, recv in [
        ((n,), (KH, n)), ((2, n), (KH, n)), ((n,), (n,)), ((n,), (n,)),
        ((1,), (KH,)), ((1,), (1,)), ((1,), (KH,)), ((1,), (1,)),
        ((1,), (KH,)), ((1,), (KH,)), ((n,), (n,)), ((n,), (n,)),
    ]:
        sems += [dma(send), dma(recv)]
    vm = pltpu.VMEM
    in_vmem = pl.BlockSpec(memory_space=pltpu.VMEM)
    in_hbm = pl.BlockSpec(memory_space=pltpu.HBM)
    results = pl.pallas_call(
        functools.partial(kernel, U, B),
        out_shape=(vm(q.shape, bf), vm((2,) + k.shape, bf)),
        in_specs=[in_hbm] * 7,
        out_specs=(in_vmem, in_vmem),
        scratch_shapes=[
            vm((2, R, G * D), bf),
            vm((3, 2, R, KH * D), bf),
            vm((U, stat_rows, T), f32),
            vm((3, U, 1, T), jnp.int32),
            vm((3, R, R), f32),
            vm((R, GROUP * D), f32),
            vm((KH, 2, R, D), f32),
            vm((KH, 2, R, D), f32),
            vm((KH, R, GROUP * D), bf),
            vm((KH, 2, R, D), bf),
            vm((KH, 2, R, D), bf),
            vm((KH, 2, R, D), bf),
            vm((KH, 2, R, D), bf),
            vm((KH, 2, R, D), bf),
            vm(q.shape, bf),
            vm((2,) + k.shape, bf),
            vm(q.shape, bf),
            vm(parts.shape, f32),
            vm((1, T), jnp.int32),
            vm((U, stat_rows, T), f32),
            vm(q.shape, bf),
            vm((2, T, KH * D), bf),
            vm((KH, 2, T, D), f32),
            vm((KH, 2, T, D), bf),
            vm((KH, 2, T, D), bf),
            vm((T, GD), f32),
            dma((8,)),
            pltpu.SemaphoreType.REGULAR,
            dma((1,)),
            dma((1,)),
            dma((1,)),
            dma((1,)),
        ] + sems,
        compiler_params=pltpu.CompilerParams(
            collective_id=0, has_side_effects=True, vmem_limit_bytes=56 << 20
        ),
    )(q, grad, k, v, out, parts, ids)
    results = [pltpu.with_memory_space_constraint(r, pltpu.VMEM) for r in results]
    return pl.pallas_call(
        close_kernel,
        out_shape=tuple(jax.ShapeDtypeStruct(r.shape, r.dtype) for r in (q, k, v)),
        in_specs=[in_vmem] * 2,
        out_specs=(in_hbm,) * 3,
        scratch_shapes=[dma((4,))],
        compiler_params=pltpu.CompilerParams(vmem_limit_bytes=8 << 20),
    )(*results)


def solution(mesh):
    spec = P(("blk", "uly"), None)
    body = functools.partial(per_device, mesh.shape["uly"], mesh.shape["blk"])
    return jax.shard_map(
        body,
        mesh=mesh,
        in_specs=(spec, spec, spec, spec, spec, P(("blk", "uly"), None, None), P(("blk", "uly"))),
        out_specs=(spec, spec, spec),
        check_vma=False,
    )
```

```python
import functools
import math

import jax
import jax.numpy as jnp
from jax import lax
from jax.experimental import pallas as pl
from jax.experimental.pallas import tpu as pltpu
from jax.sharding import PartitionSpec as P

HEAD_SIZE = 128
QUERY_HEADS = 16
KEY_VALUE_HEADS = 8
GROUP = QUERY_HEADS // KEY_VALUE_HEADS
TILE = 256
FAR = -1e30
LOG2_E = math.log2(math.e)


def dot_nt(a, b):
    return lax.dot_general(a, b, (((1,), (1,)), ((), ())), preferred_element_type=jnp.float32)


def dot_nn(a, b):
    return lax.dot_general(a, b, (((1,), (0,)), ((), ())), preferred_element_type=jnp.float32)


def dot_tn(a, b):
    return lax.dot_general(a, b, (((0,), (0,)), ((), ())), preferred_element_type=jnp.float32)


def kernel(
    uly_count, blk_count,
    q_hbm, do_hbm, k_hbm, v_hbm, out_hbm, lp_hbm, ids_hbm,
    dq_ref, dkv_ref,
    qdb, kvb, statb, idb, bias,
    dqacc, acc0, acc2, dqs, ret1, ret2, in1, in2, dkvs,
    do_ref, kv_ref, out_ref, lp_ref, ids_ref, stat_ref,
    q_ref, kx, loc1, part, px, dqt,
    loc_sem, ready, kx_s, kx_r, px_s, px_r,
    kv_s, kv_r, qd_s, qd_r, st_s, st_r, id_s, id_r,
    h2_s, h2_r, h2i_s, h2i_r, pt_s, pt_r, pti_s, pti_r,
    r1_s, r1_r, r2_s, r2_r, oq_s, oq_r, okv_s, okv_r,
):
    U, B = uly_count, blk_count
    T = q_hbm.shape[0]
    R = T * U
    KH = KEY_VALUE_HEADS // U
    D = HEAD_SIZE
    GD = GROUP * D
    G = KH * GROUP
    scale = 1.0 / math.sqrt(D)
    u = lax.axis_index("uly")
    b = lax.axis_index("blk")
    odd = lax.rem(b, 2)
    even = odd == 0
    mate = b + 1 - 2 * odd

    def at(blk, uly):
        return {"blk": blk, "uly": uly}

    def rcopy(src, dst, ssem, rsem, dev):
        return pltpu.make_async_remote_copy(
            src_ref=src, dst_ref=dst, send_sem=ssem, recv_sem=rsem,
            device_id=dev, device_id_type=pl.DeviceIdType.MESH,
        )

    def cols(first, width):
        return pl.ds(pl.multiple_of(first, 128), width)

    def rows(place):
        return pl.ds(pl.multiple_of(place * T, T), T)

    has_up2 = b + 2 < B
    has_down2 = b >= 2
    sends_mate = jnp.logical_or(even, b >= 3)

    def load(src, dst, sem):
        return pltpu.make_async_copy(src, dst, loc_sem.at[sem])

    own_cols = cols(u * KH * D, KH * D)
    own_kv = [
        load(src.at[:, own_cols], kvb.at[0, i, rows(u), :], 0)
        for i, src in enumerate((k_hbm, v_hbm))
    ]
    load_ids = load(ids_hbm, ids_ref, 1)
    load_kv = [load(src, kv_ref.at[i], 2) for i, src in enumerate((k_hbm, v_hbm))]
    load_do = load(do_hbm, do_ref, 3)
    load_out = load(out_hbm, out_ref, 4)
    load_lp = load(lp_hbm, lp_ref, 5)
    for copy in load_kv + [load_ids] + own_kv + [load_do, load_out, load_lp]:
        copy.start()

    first = b < 2
    alone = jnp.logical_and(b == 0, U == 2)
    grouped = jnp.logical_not(alone)
    barrier = pltpu.get_barrier_semaphore()
    for k in range(1, U):
        pl.semaphore_signal(
            barrier, inc=1, device_id=at(b, lax.rem(u + k, U)), device_id_type=pl.DeviceIdType.MESH
        )
    pl.semaphore_signal(barrier, inc=1, device_id=at(mate, u), device_id_type=pl.DeviceIdType.MESH)

    @pl.when(has_up2)
    def _():
        pl.semaphore_signal(
            barrier, inc=1, device_id=at(b + 2, u), device_id_type=pl.DeviceIdType.MESH
        )

    @pl.when(b >= 4)
    def _():
        pl.semaphore_signal(
            barrier, inc=1, device_id=at(b - 2, u), device_id_type=pl.DeviceIdType.MESH
        )

    met_up2 = jnp.logical_and(has_up2, b >= 2)
    expected = U + has_down2.astype(jnp.int32) + met_up2.astype(jnp.int32)
    pl.semaphore_wait(barrier, expected)

    @pl.when(jnp.logical_and(has_down2, b < 4))
    def _():
        pl.semaphore_signal(
            ready, inc=1, device_id=at(b - 2, u), device_id_type=pl.DeviceIdType.MESH
        )

    own_q = [
        load(src.at[:, cols(u * KH * GD, KH * GD)], qdb.at[i, rows(u), :], 6)
        for i, src in enumerate((q_hbm, do_hbm))
    ]
    own_id = load(ids_hbm, idb.at[0, u], 7)
    load_q = load(q_hbm, q_ref, 6)

    def id_in(k, place, dev):
        return rcopy(ids_ref, idb.at[0, place], id_s.at[k - 1], id_r.at[k - 1], dev)

    def st_in(k, place, peer, dev):
        return rcopy(stat_ref.at[peer], statb.at[place], st_s.at[k - 1], st_r.at[k - 1], dev)

    def kv_in(k, j, place, peer, dev):
        return rcopy(
            kv_ref.at[:, :, cols((peer * KH + j) * D, D)],
            kvb.at[0, :, rows(place), cols(j * D, D)],
            kv_s.at[k - 1], kv_r.at[j, k - 1], dev,
        )

    def qd_in(k, which, j, place, peer, dev):
        ref = (q_hbm, do_ref)[which]
        return rcopy(
            ref.at[:, cols((peer * KH + j) * GD, GD)],
            qdb.at[which, rows(place), cols(j * GD, GD)],
            qd_s.at[which, k - 1], qd_r.at[j, k - 1], dev,
        )

    def await_bytes(ref, sem):
        pltpu.make_async_copy(ref, ref, sem).wait()

    def h2(j, place):
        return rcopy(
            kvb.at[0, :, rows(place), cols(j * D, D)], kvb.at[2, :, rows(place), cols(j * D, D)],
            h2_s.at[0], h2_r.at[j], at(b + 2, u),
        )

    peers = [(k, lax.rem(u + k, U), lax.rem(u + U - k, U)) for k in range(1, U)]
    await_bytes(kvb.at[0, :, rows(u), :], loc_sem.at[0])

    @pl.when(met_up2)
    def _():
        for j in range(KH):
            h2(j, u).start()

    load_ids.wait()
    for k, to, _ in peers:
        id_in(k, u, at(b, to)).start()
    await_bytes(kv_ref, loc_sem.at[2])

    def send_kv(j):
        for k, to, _ in peers:
            kv_in(k, j, u, to, at(b, to)).start()

    def send_qd(j):
        for k, to, _ in peers:
            for which in range(2):
                qd_in(k, which, j, u, to, at(b, to)).start()

    for j in range(min(2, KH)):
        send_kv(j)
    own_id.start()

    @pl.when(grouped)
    def _():
        for copy in own_q:
            copy.start()

    @pl.when(alone)
    def _():
        load_q.start()

    load_do.wait()
    load_out.wait()
    load_lp.wait()

    @pl.when(grouped)
    def _():
        send_qd(0)

    lane = lax.broadcasted_iota(jnp.int32, (T, 128), 1)
    table = jnp.zeros((T, 128), jnp.float32)
    for h in range(U * G):
        piece = slice(h * D, (h + 1) * D)
        total = jnp.sum(
            do_ref[:, piece].astype(jnp.float32) * out_ref[:, piece].astype(jnp.float32),
            axis=1, keepdims=True,
        )
        table = jnp.where(lane == h, total, table)
    table = table.T
    part0, part1 = lp_ref[:, 0, :], lp_ref[:, 1, :]
    highest = jnp.maximum(part0, part1)
    lse_rows = highest + jnp.log(jnp.exp(part0 - highest) + jnp.exp(part1 - highest))
    for p in range(U):
        stat_ref[p, :G, :] = lse_rows[p * G:(p + 1) * G] * LOG2_E
        stat_ref[p, G:2 * G, :] = table[p * G:(p + 1) * G]
    statb[u] = stat_ref[u]

    @pl.when(grouped)
    def _():
        for k, to, _ in peers:
            st_in(k, u, to, at(b, to)).start()

    for j in range(2, KH):
        send_kv(j)

    @pl.when(grouped)
    def _():
        for j in range(1, KH):
            send_qd(j)

    def kx_in(j):
        head = cols(j * D, D)
        return rcopy(
            kv_ref.at[:, :, head], kx.at[:, :, head], kx_s.at[0], kx_r.at[j], at(b, 1 - u)
        )

    def px_in(j):
        return rcopy(part.at[j], px.at[j], px_s.at[0], px_r.at[0], at(b, 1 - u))

    @pl.when(jnp.logical_and(alone, u == 0))
    def _():
        for j in range(KH):
            kx_in(j).start()

    @pl.when(jnp.logical_and(first, has_up2))
    def _():
        pl.semaphore_wait(ready, 1)
        for j in range(KH):
            h2(j, u).start()

    def h2id():
        return rcopy(idb.at[0], idb.at[2], h2i_s.at[0], h2i_r.at[0], at(b + 2, u))

    def pt(j):
        return rcopy(
            kvb.at[2 * odd, :, :, cols(j * D, D)], kvb.at[1, :, :, cols(j * D, D)],
            pt_s.at[0], pt_r.at[j], at(mate, u),
        )

    def ptid():
        return rcopy(idb.at[2 * odd], idb.at[1], pti_s.at[0], pti_r.at[0], at(mate, u))

    own_id.wait()
    for k, _, frm in peers:
        id_in(k, frm, at(b, frm)).wait_recv()

    @pl.when(has_up2)
    def _():
        h2id().start()

    @pl.when(even)
    def _():
        ptid().start()

    def forward(j):
        for k, _, frm in peers:
            kv_in(k, j, frm, frm, at(b, frm)).wait_recv()

        @pl.when(has_up2)
        def _():
            for k, _, frm in peers:
                h2(j, frm).start()

        @pl.when(even)
        def _():
            pt(j).start()

    def make_bias(hop):
        for kp in range(U):
            key_ids = jnp.broadcast_to(idb[hop, kp, 0:1, :].astype(jnp.float32), (T, T)).T
            for qp in range(U):
                query_ids = idb[0, qp, 0:1, :].astype(jnp.float32)
                good = key_ids == query_ids
                if hop == 0:
                    kpos = lax.broadcasted_iota(jnp.int32, (T, T), 0) + kp * T
                    qpos = lax.broadcasted_iota(jnp.int32, (T, T), 1) + qp * T
                    good = jnp.logical_and(good, kpos <= qpos)
                bias[hop, kp * T:(kp + 1) * T, qp * T:(qp + 1) * T] = jnp.where(good, 0.0, FAR)

    make_bias(0)
    forward(0)
    if KH > 1:
        forward(1)

    @pl.when(has_down2)
    def _():
        h2id().wait_recv()
        make_bias(2)

        @pl.when(odd == 1)
        def _():
            ptid().start()

    def arrive2(j):
        @pl.when(has_down2)
        def _():
            await_bytes(kvb.at[2, :, :, cols(j * D, D)], h2_r.at[j])

            @pl.when(odd == 1)
            def _():
                pt(j).start()

    @pl.when(b >= 1)
    def _():
        ptid().wait_recv()
        make_bias(1)

    @pl.when(grouped)
    def _():
        await_bytes(qdb.at[:, rows(u), :], loc_sem.at[6])
        for k, _, frm in peers:
            st_in(k, frm, frm, at(b, frm)).wait_recv()

    if KH > 2:
        forward(2)
    arrive2(0)

    tile = min(TILE, R)
    steps = R // tile
    per = tile // T if tile >= T else 1

    def stat_row(row, qt):
        parts = [statb[qt * per + i, pl.ds(row, 1), :] for i in range(per)]
        return parts[0] if per == 1 else jnp.concatenate(parts, axis=1)

    def hop_grads(hop, j, acc):
        def key_step(kt, _):
            krow = pl.ds(pl.multiple_of(kt * tile, tile), tile)
            kc = kvb[hop, 0, krow, cols(j * D, D)]
            vc = kvb[hop, 1, krow, cols(j * D, D)]

            def query_step(qt, carry):
                dk, dv = carry
                qrow = pl.ds(pl.multiple_of(qt * tile, tile), tile)
                heads = [cols(j * GD + g * D, D) for g in range(GROUP)]
                weights, score_grads = [], []
                for g in range(GROUP):
                    lse = stat_row(j * GROUP + g, qt)
                    delta = stat_row(G + j * GROUP + g, qt)
                    w = jnp.exp2(
                        dot_nt(kc, qdb[0, qrow, heads[g]]) * (scale * LOG2_E) - lse + bias[hop, krow, qrow]
                    )
                    ds = w * (dot_nt(vc, qdb[1, qrow, heads[g]]) - delta)
                    score_grads.append(ds.astype(jnp.bfloat16))
                    weights.append(w.astype(jnp.bfloat16))
                queries = jnp.concatenate([qdb[0, qrow, heads[g]] for g in range(GROUP)], axis=0)
                cotangents = jnp.concatenate([qdb[1, qrow, heads[g]] for g in range(GROUP)], axis=0)
                dv = dot_nn(jnp.concatenate(weights, axis=1), cotangents) + dv
                dk = dot_nn(jnp.concatenate(score_grads, axis=1), queries) + dk
                for g in range(GROUP):
                    dqacc[qrow, g * D:(g + 1) * D] += dot_tn(score_grads[g], kc)
                return dk, dv

            if steps == 1:
                dk, dv = query_step(0, (0.0, 0.0))
            else:
                zero = jnp.zeros((tile, D), jnp.float32)
                dk, dv = lax.fori_loop(0, steps, query_step, (zero, zero))
            acc[j, 0, krow, :] = (dk * scale).astype(acc.dtype)
            acc[j, 1, krow, :] = dv.astype(acc.dtype)
            return 0

        if steps == 1:
            key_step(0, 0)
        else:
            lax.fori_loop(0, steps, key_step, 0)

    def give1(j):
        return rcopy(ret1.at[j], in1.at[j], r1_s.at[0], r1_r.at[j], at(mate, u))

    def give2(j):
        return rcopy(ret2.at[j], in2.at[j], r2_s.at[0], r2_r.at[j], at(b - 2, u))

    def straight(j, place):
        return rcopy(
            ret2.at[j, :, rows(place), :], in2.at[j, :, rows(u), :],
            r2_s.at[0], r2_r.at[j], at(0, place),
        )

    def oq(k, j, place, dev):
        return rcopy(
            dqs.at[j, rows(place), :], dq_ref.at[:, cols((u * KH + j) * GD, GD)],
            oq_s.at[k - 1], oq_r.at[k - 1], dev,
        )

    def okv(k, j, place, dev):
        return rcopy(
            dkvs.at[j, :, rows(place), :], dkv_ref.at[:, :, cols((u * KH + j) * D, D)],
            okv_s.at[k - 1], okv_r.at[k - 1], dev,
        )

    def compute(j):
        for k, _, frm in peers:
            await_bytes(qdb.at[:, rows(frm), cols(j * GD, GD)], qd_r.at[j, k - 1])
        dqacc[...] = jnp.zeros_like(dqacc)

        @pl.when(b >= 1)
        def _():
            pt(j).wait_recv()
            hop_grads(1, j, ret1)
            give1(j).start()

        @pl.when(j + 3 < KH)
        def _():
            forward(jnp.minimum(j + 3, KH - 1))

        @pl.when(j + 1 < KH)
        def _():
            arrive2(jnp.minimum(j + 1, KH - 1))

        @pl.when(has_down2)
        def _():
            hop_grads(2, j, acc2)

        stage_a(j)
        hop_grads(0, j, acc0)

        dqs[j] = (dqacc[...] * scale).astype(jnp.bfloat16)
        for k, to, _ in peers:
            oq(k, j, to, at(b, to)).start()
        dq_ref[:, cols((u * KH + j) * GD, GD)] = dqs[j, rows(u), :]

    def stage_a(j):
        @pl.when(jnp.logical_and(odd == 1, has_down2))
        def _():
            give1(j).wait_recv()
            ret2[j] = (acc2[j] + in1[j].astype(jnp.float32)).astype(jnp.bfloat16)

        @pl.when(jnp.logical_and(even, has_down2))
        def _():
            ret2[j] = acc2[j].astype(jnp.bfloat16)

        to_alone = jnp.logical_and(b == 2, U == 2)

        @pl.when(jnp.logical_and(has_down2, jnp.logical_not(to_alone)))
        def _():
            give2(j).start()

        @pl.when(to_alone)
        def _():
            straight(j, u).start()
            straight(j, 1 - u).start()

    def stage_b(j):
        @pl.when(even)
        def _():
            give1(j).wait_recv()
            acc0[j] += in1[j].astype(jnp.float32)

        @pl.when(has_up2)
        def _():
            give2(j).wait_recv()
            acc0[j] += in2[j].astype(jnp.float32)

        dkvs[j] = acc0[j].astype(jnp.bfloat16)
        for k, to, _ in peers:
            okv(k, j, to, at(b, to)).start()
        dkv_ref[:, :, cols((u * KH + j) * D, D)] = dkvs[j, :, rows(u), :]

    def head_step(j, _):
        compute(j)

        @pl.when(jnp.logical_and(j >= 2, b >= 2))
        def _():
            stage_b(jnp.maximum(j - 2, 0))

        return 0

    def alone_block(h, kc, vc, mask):
        heads = [cols(h * GD + g * D, D) for g in range(GROUP)]
        plane = h // KH
        row = (h - plane * KH) * GROUP
        weights, score_grads = [], []
        for g in range(GROUP):
            lse = stat_ref[plane, pl.ds(row + g, 1), :]
            delta = stat_ref[plane, pl.ds(G + row + g, 1), :]
            w = jnp.exp2(dot_nt(kc, q_ref[:, heads[g]]) * (scale * LOG2_E) - lse + mask)
            ds = w * (dot_nt(vc, do_ref[:, heads[g]]) - delta)
            score_grads.append(ds.astype(jnp.bfloat16))
            weights.append(w.astype(jnp.bfloat16))
        queries = jnp.concatenate([q_ref[:, c] for c in heads], axis=0)
        cotangents = jnp.concatenate([do_ref[:, c] for c in heads], axis=0)
        dv = dot_nn(jnp.concatenate(weights, axis=1), cotangents)
        dk = dot_nn(jnp.concatenate(score_grads, axis=1), queries) * scale
        return dk, dv, [dot_tn(ds, kc) * scale for ds in score_grads]

    def alone_own(j, _):
        for side in range(2):
            h = (u if side == 0 else 1 - u) * KH + j
            head = cols(h * D, D)
            dk, dv, dq = alone_block(
                h, kv_ref[0, :, head], kv_ref[1, :, head], bias[0, rows(u), rows(u)]
            )
            for g in range(GROUP):
                dqt[side, j, :, g * D:(g + 1) * D] = dq[g]
            if side == 0:
                acc0[j, 0, rows(u), :] = dk
                acc0[j, 1, rows(u), :] = dv
            else:
                loc1[j, 0] = dk
                loc1[j, 1] = dv
        return 0

    def alone_store(j, _):
        for side in range(2):
            h = (u if side == 0 else 1 - u) * KH + j
            dq_ref[:, cols(h * GD, GD)] = dqt[side, j].astype(jnp.bfloat16)
        return 0

    def alone_near(j, _):
        head = cols(j * D, D)
        dk, dv, dq = alone_block(
            KH + j, kvb[0, 0, rows(0), head], kvb[0, 1, rows(0), head], bias[0, rows(0), rows(1)]
        )
        for g in range(GROUP):
            dqt[0, j, :, g * D:(g + 1) * D] += dq[g]
        acc0[j, 0, rows(0), :] = dk
        acc0[j, 1, rows(0), :] = dv
        return 0

    def alone_far(j, _):
        head = cols(j * D, D)
        kx_in(j).wait_recv()
        dk, dv, dq = alone_block(j, kx[0, :, head], kx[1, :, head], bias[0, rows(0), rows(1)])
        part[j, 0] = dk.astype(jnp.bfloat16)
        part[j, 1] = dv.astype(jnp.bfloat16)
        px_in(j).start()
        for g in range(GROUP):
            dqt[1, j, :, g * D:(g + 1) * D] += dq[g]
        return 0

    def alone_merge(j, _):
        give1(j).wait_recv()
        acc0[j] += in1[j].astype(jnp.float32)
        dkvs[j] = acc0[j].astype(jnp.bfloat16)
        okv(1, j, 1 - u, at(b, 1 - u)).start()
        return 0

    def alone_finish(j, _):
        mine = cols((u * KH + j) * D, D)
        other = cols(((1 - u) * KH + j) * D, D)

        @pl.when(has_up2)
        def _():
            await_bytes(in2.at[j], r2_r.at[j])
            acc0[j, :, rows(u), :] += in2[j, :, rows(u), :].astype(jnp.float32)
            loc1[j] += in2[j, :, rows(1 - u), :].astype(jnp.float32)

        dkv_ref[:, :, mine] = acc0[j, :, rows(u), :].astype(jnp.bfloat16)
        dkv_ref[:, :, other] = (dkv_ref[:, :, other].astype(jnp.float32) + loc1[j]).astype(jnp.bfloat16)
        return 0

    @pl.when(grouped)
    def _():
        lax.fori_loop(0, KH, head_step, 0)
        late = min(2, KH)

        def last_step(j, _):
            stage_b(j)
            return 0

        lax.fori_loop(jnp.where(first, 0, KH - late), KH, last_step, 0)

    if U == 2:
        @pl.when(alone)
        def _():
            load_q.wait()
            alone_own(0, 0)
            for j in range(3, KH):
                forward(j)
            lax.fori_loop(1, KH, alone_own, 0)

            @pl.when(u == 0)
            def _():
                for j in range(KH):
                    acc0[j, :, rows(1), :] = jnp.zeros((2, T, D), jnp.float32)

            @pl.when(u == 1)
            def _():
                lax.fori_loop(0, KH, alone_near, 0)
                lax.fori_loop(0, KH, alone_far, 0)

            lax.fori_loop(0, KH, alone_merge, 0)
            lax.fori_loop(0, KH, alone_store, 0)

            @pl.when(u == 0)
            def _():
                await_bytes(px, px_r.at[0])
                for j in range(KH):
                    acc0[j, :, rows(0), :] += px[j].astype(jnp.float32)

            await_bytes(dkv_ref.at[:, :, cols((1 - u) * KH * D, KH * D)], okv_r.at[0])
            lax.fori_loop(0, KH, alone_finish, 0)

            @pl.when(u == 0)
            def _():
                await_bytes(kx, kx_s.at[0])

            @pl.when(u == 1)
            def _():
                await_bytes(part, px_s.at[0])

    for k, to, _ in peers:
        id_in(k, u, at(b, to)).wait_send()
        await_bytes(kv_ref.at[:, :, cols(to * KH * D, KH * D)], kv_s.at[k - 1])

    @pl.when(grouped)
    def _():
        for k, to, _ in peers:
            st_in(k, u, to, at(b, to)).wait_send()
            for which in range(2):
                await_bytes(qdb.at[which, rows(0), :], qd_s.at[which, k - 1])

    @pl.when(has_up2)
    def _():
        h2id().wait_send()
        await_bytes(kvb.at[0], h2_s.at[0])

    @pl.when(sends_mate)
    def _():
        ptid().wait_send()
        await_bytes(kvb.at[0], pt_s.at[0])

    @pl.when(b >= 1)
    def _():
        await_bytes(ret1, r1_s.at[0])

    @pl.when(has_down2)
    def _():
        await_bytes(ret2, r2_s.at[0])

    for k, to, _ in peers:
        await_bytes(dkvs.at[:, :, rows(to), :], okv_s.at[k - 1])

    @pl.when(grouped)
    def _():
        for k, to, frm in peers:
            await_bytes(dqs.at[:, rows(to), :], oq_s.at[k - 1])
            await_bytes(dq_ref.at[:, cols(frm * KH * GD, KH * GD)], oq_r.at[k - 1])
            await_bytes(dkv_ref.at[:, :, cols(frm * KH * D, KH * D)], okv_r.at[k - 1])


def close_kernel(q_in, kv_in, q_out, k_out, v_out, sem):
    half = q_in.shape[0] // 2
    moves = [
        (q_in.at[pl.ds(0, half)], q_out.at[pl.ds(0, half)]),
        (q_in.at[pl.ds(half, half)], q_out.at[pl.ds(half, half)]),
        (kv_in.at[0], k_out),
        (kv_in.at[1], v_out),
    ]
    copies = [pltpu.make_async_copy(src, dst, sem.at[i]) for i, (src, dst) in enumerate(moves)]
    for copy in copies:
        copy.start()
    for copy in copies:
        copy.wait()


def per_device(uly_count, blk_count, q, k, v, out, grad, lse_parts, segment_ids):
    U, B = uly_count, blk_count
    T = q.shape[0]
    R = T * U
    KH = KEY_VALUE_HEADS // U
    G = KH * GROUP
    D = HEAD_SIZE
    GD = GROUP * D
    stat_rows = -(-2 * G // 8) * 8
    parts = lse_parts.transpose(1, 2, 0)
    ids = segment_ids.reshape(1, T)
    bf, f32 = jnp.bfloat16, jnp.float32
    n = max(U - 1, 1)
    dma = pltpu.SemaphoreType.DMA
    sems = []
    for send, recv in [
        ((n,), (KH, n)), ((2, n), (KH, n)), ((n,), (n,)), ((n,), (n,)),
        ((1,), (KH,)), ((1,), (1,)), ((1,), (KH,)), ((1,), (1,)),
        ((1,), (KH,)), ((1,), (KH,)), ((n,), (n,)), ((n,), (n,)),
    ]:
        sems += [dma(send), dma(recv)]
    vm = pltpu.VMEM
    in_vmem = pl.BlockSpec(memory_space=pltpu.VMEM)
    in_hbm = pl.BlockSpec(memory_space=pltpu.HBM)
    results = pl.pallas_call(
        functools.partial(kernel, U, B),
        out_shape=(vm(q.shape, bf), vm((2,) + k.shape, bf)),
        in_specs=[in_hbm] * 7,
        out_specs=(in_vmem, in_vmem),
        scratch_shapes=[
            vm((2, R, G * D), bf),
            vm((3, 2, R, KH * D), bf),
            vm((U, stat_rows, T), f32),
            vm((3, U, 1, T), jnp.int32),
            vm((3, R, R), f32),
            vm((R, GROUP * D), f32),
            vm((KH, 2, R, D), f32),
            vm((KH, 2, R, D), f32),
            vm((KH, R, GROUP * D), bf),
            vm((KH, 2, R, D), bf),
            vm((KH, 2, R, D), bf),
            vm((KH, 2, R, D), bf),
            vm((KH, 2, R, D), bf),
            vm((KH, 2, R, D), bf),
            vm(q.shape, bf),
            vm((2,) + k.shape, bf),
            vm(q.shape, bf),
            vm(parts.shape, f32),
            vm((1, T), jnp.int32),
            vm((U, stat_rows, T), f32),
            vm(q.shape, bf),
            vm((2, T, KH * D), bf),
            vm((KH, 2, T, D), f32),
            vm((KH, 2, T, D), bf),
            vm((KH, 2, T, D), bf),
            vm((2, KH, T, GD), f32),
            dma((8,)),
            pltpu.SemaphoreType.REGULAR,
            dma((1,)),
            dma((KH,)),
            dma((1,)),
            dma((1,)),
        ] + sems,
        compiler_params=pltpu.CompilerParams(
            collective_id=0, has_side_effects=True, vmem_limit_bytes=56 << 20
        ),
    )(q, grad, k, v, out, parts, ids)
    results = [pltpu.with_memory_space_constraint(r, pltpu.VMEM) for r in results]
    return pl.pallas_call(
        close_kernel,
        out_shape=tuple(jax.ShapeDtypeStruct(r.shape, r.dtype) for r in (q, k, v)),
        in_specs=[in_vmem] * 2,
        out_specs=(in_hbm,) * 3,
        scratch_shapes=[dma((4,))],
        compiler_params=pltpu.CompilerParams(vmem_limit_bytes=8 << 20),
    )(*results)


def solution(mesh):
    spec = P(("blk", "uly"), None)
    body = functools.partial(per_device, mesh.shape["uly"], mesh.shape["blk"])
    return jax.shard_map(
        body,
        mesh=mesh,
        in_specs=(spec, spec, spec, spec, spec, P(("blk", "uly"), None, None), P(("blk", "uly"))),
        out_specs=(spec, spec, spec),
        check_vma=False,
    )
```

```python
import functools
import math

import jax
import jax.numpy as jnp
from jax import lax
from jax.experimental import pallas as pl
from jax.experimental.pallas import tpu as pltpu
from jax.sharding import PartitionSpec as P

HEAD_SIZE = 128
QUERY_HEADS = 16
KEY_VALUE_HEADS = 8
GROUP = QUERY_HEADS // KEY_VALUE_HEADS
TILE = 256
FAR = -1e30
LOG2_E = math.log2(math.e)


def dot_nt(a, b):
    return lax.dot_general(a, b, (((1,), (1,)), ((), ())), preferred_element_type=jnp.float32)


def dot_nn(a, b):
    return lax.dot_general(a, b, (((1,), (0,)), ((), ())), preferred_element_type=jnp.float32)


def dot_tn(a, b):
    return lax.dot_general(a, b, (((0,), (0,)), ((), ())), preferred_element_type=jnp.float32)


def kernel(
    uly_count, blk_count,
    q_hbm, do_hbm, k_hbm, v_hbm, out_hbm, lp_hbm, ids_hbm,
    dq_ref, dkv_ref,
    qdb, kvb, statb, idb, bias,
    dqacc, acc0, acc2, dqs, ret1, ret2, in1, in2, dkvs,
    do_ref, kv_ref, out_ref, lp_ref, ids_ref, stat_ref,
    q_ref, kx, loc1, part, px, dqt,
    loc_sem, ready, relay,
    kv_s, kv_r, qd_s, qd_r, st_s, st_r, id_s, id_r,
    h2_s, h2_r, h2i_s, h2i_r, pt_s, pt_r, pti_s, pti_r,
    r1_s, r2_s, r2_r, oq_s, oq_r, okv_s, okv_r,
):
    U, B = uly_count, blk_count
    T = q_hbm.shape[0]
    R = T * U
    KH = KEY_VALUE_HEADS // U
    D = HEAD_SIZE
    GD = GROUP * D
    G = KH * GROUP
    scale = 1.0 / math.sqrt(D)
    u = lax.axis_index("uly")
    b = lax.axis_index("blk")
    odd = lax.rem(b, 2)
    even = odd == 0
    mate = b + 1 - 2 * odd

    def at(blk, uly):
        return {"blk": blk, "uly": uly}

    def rcopy(src, dst, ssem, rsem, dev):
        return pltpu.make_async_remote_copy(
            src_ref=src, dst_ref=dst, send_sem=ssem, recv_sem=rsem,
            device_id=dev, device_id_type=pl.DeviceIdType.MESH,
        )

    def cols(first, width):
        return pl.ds(pl.multiple_of(first, 128), width)

    def rows(place):
        return pl.ds(pl.multiple_of(place * T, T), T)

    has_up2 = b + 2 < B
    has_down2 = b >= 2
    sends_mate = jnp.logical_or(even, b >= 3)

    def load(src, dst, sem):
        return pltpu.make_async_copy(src, dst, loc_sem.at[sem])

    own_cols = cols(u * KH * D, KH * D)
    own_kv = [
        load(src.at[:, own_cols], kvb.at[0, i, rows(u), :], 0)
        for i, src in enumerate((k_hbm, v_hbm))
    ]
    load_ids = load(ids_hbm, ids_ref, 1)
    load_kv = [load(src, kv_ref.at[i], 2) for i, src in enumerate((k_hbm, v_hbm))]
    load_do = load(do_hbm, do_ref, 3)
    load_out = load(out_hbm, out_ref, 4)
    load_lp = load(lp_hbm, lp_ref, 5)
    for copy in load_kv + [load_ids] + own_kv + [load_do, load_out, load_lp]:
        copy.start()

    first = b < 2
    alone = jnp.logical_and(b == 0, U == 2)
    grouped = jnp.logical_not(alone)
    side_pair = lax.rem(b // 2, 2) == 1
    has_up4 = b + 4 < B
    barrier = pltpu.get_barrier_semaphore()

    def greet(sem, blk, uly):
        pl.semaphore_signal(
            sem, inc=1, device_id=at(blk, uly), device_id_type=pl.DeviceIdType.MESH
        )

    for k in range(1, U):
        greet(barrier, b, lax.rem(u + k, U))
    greet(barrier, mate, u)
    main_pair = jnp.logical_not(side_pair)
    hub = u == 0
    tree = u > 0

    @pl.when(jnp.logical_and(jnp.logical_or(hub, main_pair), has_up2))
    def _():
        greet(barrier, b + 2, u)

    @pl.when(jnp.logical_and(hub, has_down2))
    def _():
        greet(barrier, b - 2, u)

    @pl.when(jnp.logical_and(jnp.logical_and(tree, main_pair), has_up4))
    def _():
        greet(barrier, b + 4, u)

    met_up2 = jnp.logical_and(hub, has_up2)
    pl.semaphore_wait(barrier, U + has_down2.astype(jnp.int32) + met_up2.astype(jnp.int32))

    @pl.when(jnp.logical_and(tree, side_pair))
    def _():
        greet(ready, b - 2, u)

    @pl.when(jnp.logical_and(jnp.logical_and(tree, main_pair), b >= 4))
    def _():
        greet(relay, b - 4, u)

    own_q = [
        load(src.at[:, cols(u * KH * GD, KH * GD)], qdb.at[i, rows(u), :], 6)
        for i, src in enumerate((q_hbm, do_hbm))
    ]
    own_id = load(ids_hbm, idb.at[0, u], 7)
    load_q = load(q_hbm, q_ref, 6)

    def id_in(k, place, dev):
        return rcopy(ids_ref, idb.at[0, place], id_s.at[k - 1], id_r.at[k - 1], dev)

    def st_in(k, place, peer, dev):
        return rcopy(stat_ref.at[peer], statb.at[place], st_s.at[k - 1], st_r.at[k - 1], dev)

    def kv_in(k, j, place, peer, dev):
        return rcopy(
            kv_ref.at[:, :, cols((peer * KH + j) * D, D)],
            kvb.at[0, :, rows(place), cols(j * D, D)],
            kv_s.at[k - 1], kv_r.at[j, k - 1], dev,
        )

    def qd_in(k, which, j, place, peer, dev):
        ref = (q_hbm, do_ref)[which]
        return rcopy(
            ref.at[:, cols((peer * KH + j) * GD, GD)],
            qdb.at[which, rows(place), cols(j * GD, GD)],
            qd_s.at[k - 1], qd_r.at[j, k - 1], dev,
        )

    def await_bytes(ref, sem):
        pltpu.make_async_copy(ref, ref, sem).wait()

    def h2(j, place):
        return rcopy(
            kvb.at[0, :, rows(place), cols(j * D, D)], kvb.at[2, :, rows(place), cols(j * D, D)],
            h2_s.at[0], h2_r.at[j], at(b + 2, u),
        )

    peers = [(k, lax.rem(u + k, U), lax.rem(u + U - k, U)) for k in range(1, U)]
    soon = min(3, KH)

    @pl.when(hub)
    def _():
        await_bytes(kvb.at[0, :, rows(u), :], loc_sem.at[0])

        @pl.when(has_up2)
        def _():
            for j in range(soon):
                h2(j, u).start()

    load_ids.wait()
    for k, to, _ in peers:
        id_in(k, u, at(b, to)).start()
    await_bytes(kv_ref, loc_sem.at[2])

    def send_kv(j):
        for k, to, _ in peers:
            kv_in(k, j, u, to, at(b, to)).start()

    def send_qd(j):
        for k, to, _ in peers:
            for which in range(2):
                qd_in(k, which, j, u, to, at(b, to)).start()

    for j in range(soon):
        send_kv(j)
    own_id.start()

    @pl.when(grouped)
    def _():
        for copy in own_q:
            copy.start()

    @pl.when(alone)
    def _():
        load_q.start()

    load_do.wait()
    load_out.wait()
    load_lp.wait()

    @pl.when(grouped)
    def _():
        send_qd(0)

    lane = lax.broadcasted_iota(jnp.int32, (T, 128), 1)
    table = jnp.zeros((T, 128), jnp.float32)
    for h in range(U * G):
        piece = slice(h * D, (h + 1) * D)
        total = jnp.sum(
            do_ref[:, piece].astype(jnp.float32) * out_ref[:, piece].astype(jnp.float32),
            axis=1, keepdims=True,
        )
        table = jnp.where(lane == h, total, table)
    table = table.T
    part0, part1 = lp_ref[:, 0, :], lp_ref[:, 1, :]
    highest = jnp.maximum(part0, part1)
    lse_rows = highest + jnp.log(jnp.exp(part0 - highest) + jnp.exp(part1 - highest))
    for p in range(U):
        stat_ref[p, :G, :] = lse_rows[p * G:(p + 1) * G] * LOG2_E
        stat_ref[p, G:2 * G, :] = table[p * G:(p + 1) * G]
    statb[u] = stat_ref[u]

    @pl.when(grouped)
    def _():
        for k, to, _ in peers:
            st_in(k, u, to, at(b, to)).start()

    for j in range(soon, KH):
        send_kv(j)

    late_last = KH >= 3
    holds_back = jnp.logical_and(odd == 1, b >= 2)

    @pl.when(grouped)
    def _():
        for j in range(1, KH - 1 if late_last else KH):
            send_qd(j)

    if late_last:
        @pl.when(jnp.logical_and(grouped, jnp.logical_not(holds_back)))
        def _():
            send_qd(KH - 1)

    def kx_in(j):
        head = cols(j * D, D)
        return rcopy(
            kv_ref.at[:, :, head], kx.at[:, :, head], qd_s.at[0], qd_r.at[j, 0], at(b, 1 - u)
        )

    def px_in(j):
        return rcopy(part.at[j], px.at[j], qd_s.at[0], st_r.at[0], at(b, 1 - u))

    @pl.when(jnp.logical_and(alone, u == 0))
    def _():
        for j in range(KH):
            kx_in(j).start()

    @pl.when(tree)
    def _():
        await_bytes(kvb.at[0, :, rows(u), :], loc_sem.at[0])

        @pl.when(has_up2)
        def _():
            pl.semaphore_wait(ready, 1)
            for j in range(soon):
                h2(j, u).start()

    @pl.when(jnp.logical_and(jnp.logical_and(tree, main_pair), has_up4))
    def _():
        pl.semaphore_wait(relay, 1)
        greet(ready, b + 2, u)

    def h2id():
        return rcopy(idb.at[0], idb.at[2], h2i_s.at[0], h2i_r.at[0], at(b + 2, u))

    def pt(j):
        return rcopy(
            kvb.at[2 * odd, :, :, cols(j * D, D)], kvb.at[1, :, :, cols(j * D, D)],
            pt_s.at[0], pt_r.at[j], at(mate, u),
        )

    def ptid():
        return rcopy(idb.at[2 * odd], idb.at[1], pti_s.at[0], pti_r.at[0], at(mate, u))

    own_id.wait()
    for k, _, frm in peers:
        id_in(k, frm, at(b, frm)).wait_recv()

    @pl.when(has_up2)
    def _():
        h2id().start()

    @pl.when(even)
    def _():
        ptid().start()

    def forward(j):
        for k, _, frm in peers:
            kv_in(k, j, frm, frm, at(b, frm)).wait_recv()

        @pl.when(has_up2)
        def _():
            for k, _, frm in peers:
                h2(j, frm).start()

        @pl.when(even)
        def _():
            pt(j).start()

    def make_bias(hop):
        for kp in range(U):
            key_ids = jnp.broadcast_to(idb[hop, kp, 0:1, :].astype(jnp.float32), (T, T)).T
            for qp in range(U):
                query_ids = idb[0, qp, 0:1, :].astype(jnp.float32)
                good = key_ids == query_ids
                if hop == 0:
                    kpos = lax.broadcasted_iota(jnp.int32, (T, T), 0) + kp * T
                    qpos = lax.broadcasted_iota(jnp.int32, (T, T), 1) + qp * T
                    good = jnp.logical_and(good, kpos <= qpos)
                bias[hop, kp * T:(kp + 1) * T, qp * T:(qp + 1) * T] = jnp.where(good, 0.0, FAR)

    make_bias(0)
    forward(0)
    if KH > 1:
        forward(1)

    @pl.when(has_up2)
    def _():
        for j in range(soon, KH):
            h2(j, u).start()

    @pl.when(has_down2)
    def _():
        h2id().wait_recv()
        make_bias(2)

        @pl.when(odd == 1)
        def _():
            ptid().start()

    def arrive2(j):
        @pl.when(has_down2)
        def _():
            await_bytes(kvb.at[2, :, :, cols(j * D, D)], h2_r.at[j])

            @pl.when(odd == 1)
            def _():
                pt(j).start()

    @pl.when(b >= 1)
    def _():
        ptid().wait_recv()
        make_bias(1)

    @pl.when(grouped)
    def _():
        await_bytes(qdb.at[:, rows(u), :], loc_sem.at[6])
        for k, _, frm in peers:
            st_in(k, frm, frm, at(b, frm)).wait_recv()

    if KH > 2:
        forward(2)
    arrive2(0)

    tile = min(TILE, R)
    steps = R // tile
    per = tile // T if tile >= T else 1

    def stat_row(row, qt):
        parts = [statb[qt * per + i, pl.ds(row, 1), :] for i in range(per)]
        return parts[0] if per == 1 else jnp.concatenate(parts, axis=1)

    def hop_grads(hop, j, acc):
        def key_step(kt, _):
            krow = pl.ds(pl.multiple_of(kt * tile, tile), tile)
            kc = kvb[hop, 0, krow, cols(j * D, D)]
            vc = kvb[hop, 1, krow, cols(j * D, D)]

            def query_step(qt, carry):
                dk, dv = carry
                qrow = pl.ds(pl.multiple_of(qt * tile, tile), tile)
                heads = [cols(j * GD + g * D, D) for g in range(GROUP)]
                weights, score_grads = [], []
                for g in range(GROUP):
                    lse = stat_row(j * GROUP + g, qt)
                    delta = stat_row(G + j * GROUP + g, qt)
                    w = jnp.exp2(
                        dot_nt(kc, qdb[0, qrow, heads[g]]) * (scale * LOG2_E) - lse + bias[hop, krow, qrow]
                    )
                    ds = w * (dot_nt(vc, qdb[1, qrow, heads[g]]) - delta)
                    score_grads.append(ds.astype(jnp.bfloat16))
                    weights.append(w.astype(jnp.bfloat16))
                queries = jnp.concatenate([qdb[0, qrow, heads[g]] for g in range(GROUP)], axis=0)
                cotangents = jnp.concatenate([qdb[1, qrow, heads[g]] for g in range(GROUP)], axis=0)
                dv = dot_nn(jnp.concatenate(weights, axis=1), cotangents) + dv
                dk = dot_nn(jnp.concatenate(score_grads, axis=1), queries) + dk
                for g in range(GROUP):
                    dqacc[qrow, g * D:(g + 1) * D] += dot_tn(score_grads[g], kc)
                return dk, dv

            if steps == 1:
                dk, dv = query_step(0, (0.0, 0.0))
            else:
                zero = jnp.zeros((tile, D), jnp.float32)
                dk, dv = lax.fori_loop(0, steps, query_step, (zero, zero))
            acc[j, 0, krow, :] = (dk * scale).astype(acc.dtype)
            acc[j, 1, krow, :] = dv.astype(acc.dtype)
            return 0

        if steps == 1:
            key_step(0, 0)
        else:
            lax.fori_loop(0, steps, key_step, 0)

    def give1(j):
        return rcopy(ret1.at[j], in1.at[j], r1_s.at[0], kv_r.at[j, 0], at(mate, u))

    def give2(j):
        return rcopy(ret2.at[j], in2.at[j], r2_s.at[0], r2_r.at[j], at(b - 2, u))

    def give2_part(which):
        return rcopy(
            ret2.at[KH - 1, which], in2.at[KH - 1, which],
            r2_s.at[0], r2_r.at[KH - 1 + which], at(b - 2, u),
        )

    def straight(j, place):
        return rcopy(
            ret2.at[j, :, rows(place), :], in2.at[j, :, rows(u), :],
            r2_s.at[0], r2_r.at[j], at(0, place),
        )

    def oq(k, j, place, dev):
        return rcopy(
            dqs.at[j, rows(place), :], dq_ref.at[:, cols((u * KH + j) * GD, GD)],
            oq_s.at[k - 1], oq_r.at[k - 1], dev,
        )

    def okv(k, j, place, dev):
        return rcopy(
            dkvs.at[j, :, rows(place), :], dkv_ref.at[:, :, cols((u * KH + j) * D, D)],
            okv_s.at[k - 1], okv_r.at[k - 1], dev,
        )

    def send_oq(j):
        for k, to, _ in peers:
            oq(k, j, to, at(b, to)).start()

    def compute(j):
        for k, _, frm in peers:
            await_bytes(qdb.at[:, rows(frm), cols(j * GD, GD)], qd_r.at[j, k - 1])
        dqacc[...] = jnp.zeros_like(dqacc)

        @pl.when(b >= 1)
        def _():
            pt(j).wait_recv()
            hop_grads(1, j, ret1)
            give1(j).start()

        @pl.when(j + 3 < KH)
        def _():
            forward(jnp.minimum(j + 3, KH - 1))

        @pl.when(j + 1 < KH)
        def _():
            arrive2(jnp.minimum(j + 1, KH - 1))

        @pl.when(has_down2)
        def _():
            hop_grads(2, j, acc2)

        @pl.when(even)
        def _():
            stage_a(j)

        hop_grads(0, j, acc0)

        dqs[j] = (dqacc[...] * scale).astype(jnp.bfloat16)
        if late_last:
            @pl.when(jnp.logical_and(holds_back, j == KH - 3))
            def _():
                send_qd(KH - 1)
                for i in range(KH - 3):
                    send_oq(i)

            @pl.when(jnp.logical_or(jnp.logical_not(holds_back), j >= KH - 3))
            def _():
                send_oq(j)
        else:
            send_oq(j)
        dq_ref[:, cols((u * KH + j) * GD, GD)] = dqs[j, rows(u), :]

        @pl.when(odd == 1)
        def _():
            stage_a(j)

    def stage_a(j):
        @pl.when(jnp.logical_and(odd == 1, has_down2))
        def _():
            give1(j).wait_recv()
            ret2[j] = (acc2[j] + in1[j].astype(jnp.float32)).astype(jnp.bfloat16)

        @pl.when(jnp.logical_and(even, has_down2))
        def _():
            ret2[j] = acc2[j].astype(jnp.bfloat16)

        to_alone = jnp.logical_and(b == 2, U == 2)

        to_grouped = jnp.logical_and(has_down2, jnp.logical_not(to_alone))

        @pl.when(jnp.logical_and(to_grouped, j < KH - 1))
        def _():
            give2(j).start()

        @pl.when(jnp.logical_and(to_grouped, j == KH - 1))
        def _():
            for which in range(2):
                give2_part(which).start()

        @pl.when(to_alone)
        def _():
            straight(j, u).start()
            straight(j, 1 - u).start()

    def stage_b(j):
        @pl.when(even)
        def _():
            give1(j).wait_recv()
            acc0[j] += in1[j].astype(jnp.float32)

        @pl.when(has_up2)
        def _():
            give2(j).wait_recv()
            acc0[j] += in2[j].astype(jnp.float32)

        dkvs[j] = acc0[j].astype(jnp.bfloat16)
        for k, to, _ in peers:
            okv(k, j, to, at(b, to)).start()
        dkv_ref[:, :, cols((u * KH + j) * D, D)] = dkvs[j, :, rows(u), :]

    def stage_b_last():
        j = KH - 1

        @pl.when(even)
        def _():
            give1(j).wait_recv()
            acc0[j] += in1[j].astype(jnp.float32)

        for which in range(2):
            @pl.when(has_up2)
            def _():
                give2_part(which).wait_recv()
                acc0[j, which] += in2[j, which].astype(jnp.float32)

            dkvs[j, which] = acc0[j, which].astype(jnp.bfloat16)
            head = cols((u * KH + j) * D, D)
            for k, to, _ in peers:
                rcopy(
                    dkvs.at[j, which, rows(to), :], dkv_ref.at[which, :, head],
                    okv_s.at[k - 1], okv_r.at[k - 1], at(b, to),
                ).start()
            dkv_ref[which, :, head] = dkvs[j, which, rows(u), :]

    def head_step(j, _):
        compute(j)

        @pl.when(jnp.logical_and(j >= 2, b >= 2))
        def _():
            stage_b(jnp.maximum(j - 2, 0))

        return 0

    def alone_block(h, kc, vc, mask):
        heads = [cols(h * GD + g * D, D) for g in range(GROUP)]
        plane = h // KH
        row = (h - plane * KH) * GROUP
        weights, score_grads = [], []
        for g in range(GROUP):
            lse = stat_ref[plane, pl.ds(row + g, 1), :]
            delta = stat_ref[plane, pl.ds(G + row + g, 1), :]
            w = jnp.exp2(dot_nt(kc, q_ref[:, heads[g]]) * (scale * LOG2_E) - lse + mask)
            ds = w * (dot_nt(vc, do_ref[:, heads[g]]) - delta)
            score_grads.append(ds.astype(jnp.bfloat16))
            weights.append(w.astype(jnp.bfloat16))
        queries = jnp.concatenate([q_ref[:, c] for c in heads], axis=0)
        cotangents = jnp.concatenate([do_ref[:, c] for c in heads], axis=0)
        dv = dot_nn(jnp.concatenate(weights, axis=1), cotangents)
        dk = dot_nn(jnp.concatenate(score_grads, axis=1), queries) * scale
        return dk, dv, [dot_tn(ds, kc) * scale for ds in score_grads]

    def alone_own(j, _):
        for side in range(2):
            h = (u if side == 0 else 1 - u) * KH + j
            head = cols(h * D, D)
            dk, dv, dq = alone_block(
                h, kv_ref[0, :, head], kv_ref[1, :, head], bias[0, rows(u), rows(u)]
            )
            for g in range(GROUP):
                dqt[side, j, :, g * D:(g + 1) * D] = dq[g]
            if side == 0:
                acc0[j, 0, rows(u), :] = dk
                acc0[j, 1, rows(u), :] = dv
            else:
                loc1[j, 0] = dk
                loc1[j, 1] = dv
        return 0

    def alone_store(j, _):
        for side in range(2):
            h = (u if side == 0 else 1 - u) * KH + j
            dq_ref[:, cols(h * GD, GD)] = dqt[side, j].astype(jnp.bfloat16)
        return 0

    def alone_near(j, _):
        head = cols(j * D, D)
        dk, dv, dq = alone_block(
            KH + j, kvb[0, 0, rows(0), head], kvb[0, 1, rows(0), head], bias[0, rows(0), rows(1)]
        )
        for g in range(GROUP):
            dqt[0, j, :, g * D:(g + 1) * D] += dq[g]
        acc0[j, 0, rows(0), :] = dk
        acc0[j, 1, rows(0), :] = dv
        return 0

    def alone_far(j, _):
        head = cols(j * D, D)
        kx_in(j).wait_recv()
        dk, dv, dq = alone_block(j, kx[0, :, head], kx[1, :, head], bias[0, rows(0), rows(1)])
        part[j, 0] = dk.astype(jnp.bfloat16)
        part[j, 1] = dv.astype(jnp.bfloat16)
        px_in(j).start()
        for g in range(GROUP):
            dqt[1, j, :, g * D:(g + 1) * D] += dq[g]
        return 0

    def alone_merge(j, _):
        give1(j).wait_recv()
        acc0[j] += in1[j].astype(jnp.float32)
        dkvs[j] = acc0[j].astype(jnp.bfloat16)
        okv(1, j, 1 - u, at(b, 1 - u)).start()
        return 0

    def alone_finish(j, _):
        mine = cols((u * KH + j) * D, D)
        other = cols(((1 - u) * KH + j) * D, D)

        @pl.when(has_up2)
        def _():
            await_bytes(in2.at[j], r2_r.at[j])
            acc0[j, :, rows(u), :] += in2[j, :, rows(u), :].astype(jnp.float32)
            loc1[j] += in2[j, :, rows(1 - u), :].astype(jnp.float32)

        dkv_ref[:, :, mine] = acc0[j, :, rows(u), :].astype(jnp.bfloat16)
        dkv_ref[:, :, other] = (dkv_ref[:, :, other].astype(jnp.float32) + loc1[j]).astype(jnp.bfloat16)
        return 0

    @pl.when(grouped)
    def _():
        lax.fori_loop(0, KH, head_step, 0)
        late = min(2, KH)

        def last_step(j, _):
            stage_b(j)
            return 0

        lax.fori_loop(jnp.where(first, 0, KH - late), KH - 1, last_step, 0)
        stage_b_last()

    if U == 2:
        @pl.when(alone)
        def _():
            load_q.wait()
            alone_own(0, 0)
            for j in range(3, KH):
                forward(j)
            lax.fori_loop(1, KH, alone_own, 0)

            @pl.when(u == 0)
            def _():
                for j in range(KH):
                    acc0[j, :, rows(1), :] = jnp.zeros((2, T, D), jnp.float32)

            @pl.when(u == 1)
            def _():
                lax.fori_loop(0, KH, alone_near, 0)
                lax.fori_loop(0, KH, alone_far, 0)

            lax.fori_loop(0, KH, alone_merge, 0)
            lax.fori_loop(0, KH, alone_store, 0)

            @pl.when(u == 0)
            def _():
                await_bytes(px, st_r.at[0])
                for j in range(KH):
                    acc0[j, :, rows(0), :] += px[j].astype(jnp.float32)

            await_bytes(dkv_ref.at[:, :, cols((1 - u) * KH * D, KH * D)], okv_r.at[0])
            lax.fori_loop(0, KH, alone_finish, 0)

            @pl.when(u == 0)
            def _():
                await_bytes(kx, qd_s.at[0])

            @pl.when(u == 1)
            def _():
                await_bytes(part, qd_s.at[0])

    for k, to, _ in peers:
        id_in(k, u, at(b, to)).wait_send()
        await_bytes(kv_ref.at[:, :, cols(to * KH * D, KH * D)], kv_s.at[k - 1])

    @pl.when(grouped)
    def _():
        for k, to, _ in peers:
            st_in(k, u, to, at(b, to)).wait_send()
            await_bytes(qdb.at[:, rows(0), :], qd_s.at[k - 1])

    @pl.when(has_up2)
    def _():
        h2id().wait_send()
        await_bytes(kvb.at[0], h2_s.at[0])

    @pl.when(sends_mate)
    def _():
        ptid().wait_send()
        await_bytes(kvb.at[0], pt_s.at[0])

    @pl.when(b >= 1)
    def _():
        await_bytes(ret1, r1_s.at[0])

    @pl.when(has_down2)
    def _():
        await_bytes(ret2, r2_s.at[0])

    for k, to, _ in peers:
        await_bytes(dkvs.at[:, :, rows(to), :], okv_s.at[k - 1])

    @pl.when(grouped)
    def _():
        for k, to, frm in peers:
            await_bytes(dqs.at[:, rows(to), :], oq_s.at[k - 1])
            await_bytes(dq_ref.at[:, cols(frm * KH * GD, KH * GD)], oq_r.at[k - 1])
            await_bytes(dkv_ref.at[:, :, cols(frm * KH * D, KH * D)], okv_r.at[k - 1])


def close_kernel(q_in, kv_in, q_out, k_out, v_out, sem):
    half = q_in.shape[0] // 2
    moves = [
        (q_in.at[pl.ds(0, half)], q_out.at[pl.ds(0, half)]),
        (q_in.at[pl.ds(half, half)], q_out.at[pl.ds(half, half)]),
        (kv_in.at[0], k_out),
        (kv_in.at[1], v_out),
    ]
    copies = [pltpu.make_async_copy(src, dst, sem.at[i]) for i, (src, dst) in enumerate(moves)]
    for copy in copies:
        copy.start()
    for copy in copies:
        copy.wait()


def per_device(uly_count, blk_count, q, k, v, out, grad, lse_parts, segment_ids):
    U, B = uly_count, blk_count
    T = q.shape[0]
    R = T * U
    KH = KEY_VALUE_HEADS // U
    G = KH * GROUP
    D = HEAD_SIZE
    GD = GROUP * D
    stat_rows = -(-2 * G // 8) * 8
    parts = lse_parts.transpose(1, 2, 0)
    ids = segment_ids.reshape(1, T)
    bf, f32 = jnp.bfloat16, jnp.float32
    n = max(U - 1, 1)
    dma = pltpu.SemaphoreType.DMA
    sems = []
    for send, recv in [
        ((n,), (KH, n)), ((n,), (KH, n)), ((n,), (n,)), ((n,), (n,)),
        ((1,), (KH,)), ((1,), (1,)), ((1,), (KH,)), ((1,), (1,)),
        ((1,), None), ((1,), (KH + 1,)), ((n,), (n,)), ((n,), (n,)),
    ]:
        sems += [dma(shape) for shape in (send, recv) if shape is not None]
    vm = pltpu.VMEM
    in_vmem = pl.BlockSpec(memory_space=pltpu.VMEM)
    in_hbm = pl.BlockSpec(memory_space=pltpu.HBM)
    results = pl.pallas_call(
        functools.partial(kernel, U, B),
        out_shape=(vm(q.shape, bf), vm((2,) + k.shape, bf)),
        in_specs=[in_hbm] * 7,
        out_specs=(in_vmem, in_vmem),
        scratch_shapes=[
            vm((2, R, G * D), bf),
            vm((3, 2, R, KH * D), bf),
            vm((U, stat_rows, T), f32),
            vm((3, U, 1, T), jnp.int32),
            vm((3, R, R), f32),
            vm((R, GROUP * D), f32),
            vm((KH, 2, R, D), f32),
            vm((KH, 2, R, D), f32),
            vm((KH, R, GROUP * D), bf),
            vm((KH, 2, R, D), bf),
            vm((KH, 2, R, D), bf),
            vm((KH, 2, R, D), bf),
            vm((KH, 2, R, D), bf),
            vm((KH, 2, R, D), bf),
            vm(q.shape, bf),
            vm((2,) + k.shape, bf),
            vm(q.shape, bf),
            vm(parts.shape, f32),
            vm((1, T), jnp.int32),
            vm((U, stat_rows, T), f32),
            vm(q.shape, bf),
            vm((2, T, KH * D), bf),
            vm((KH, 2, T, D), f32),
            vm((KH, 2, T, D), bf),
            vm((KH, 2, T, D), bf),
            vm((2, KH, T, GD), f32),
            dma((8,)),
            pltpu.SemaphoreType.REGULAR,
            pltpu.SemaphoreType.REGULAR,
        ] + sems,
        compiler_params=pltpu.CompilerParams(
            collective_id=0, has_side_effects=True, vmem_limit_bytes=56 << 20
        ),
    )(q, grad, k, v, out, parts, ids)
    results = [pltpu.with_memory_space_constraint(r, pltpu.VMEM) for r in results]
    return pl.pallas_call(
        close_kernel,
        out_shape=tuple(jax.ShapeDtypeStruct(r.shape, r.dtype) for r in (q, k, v)),
        in_specs=[in_vmem] * 2,
        out_specs=(in_hbm,) * 3,
        scratch_shapes=[dma((4,))],
        compiler_params=pltpu.CompilerParams(vmem_limit_bytes=8 << 20),
    )(*results)


def solution(mesh):
    spec = P(("blk", "uly"), None)
    body = functools.partial(per_device, mesh.shape["uly"], mesh.shape["blk"])
    return jax.shard_map(
        body,
        mesh=mesh,
        in_specs=(spec, spec, spec, spec, spec, P(("blk", "uly"), None, None), P(("blk", "uly"))),
        out_specs=(spec, spec, spec),
        check_vma=False,
    )
```

```python
import functools
import math

import jax
import jax.numpy as jnp
from jax import lax
from jax.experimental import pallas as pl
from jax.experimental.pallas import tpu as pltpu
from jax.sharding import PartitionSpec as P

HEAD_SIZE = 128
QUERY_HEADS = 16
KEY_VALUE_HEADS = 8
GROUP = QUERY_HEADS // KEY_VALUE_HEADS
TILE = 256
FAR = -1e30
LOG2_E = math.log2(math.e)


def dot_nt(a, b):
    return lax.dot_general(a, b, (((1,), (1,)), ((), ())), preferred_element_type=jnp.float32)


def dot_nn(a, b):
    return lax.dot_general(a, b, (((1,), (0,)), ((), ())), preferred_element_type=jnp.float32)


def dot_tn(a, b):
    return lax.dot_general(a, b, (((0,), (0,)), ((), ())), preferred_element_type=jnp.float32)


def kernel(
    uly_count, blk_count,
    q_hbm, do_hbm, k_hbm, v_hbm, out_hbm, lp_hbm, ids_hbm,
    dq_ref, dkv_ref,
    qdb, kvb, statb, idb, bias,
    dqacc, acc0, acc2, dqs, ret1, ret2, in1, in2, dkvs,
    do_ref, kv_ref, out_ref, lp_ref, ids_ref, stat_ref,
    q_ref, kx, loc1, part, px, dqt,
    loc_sem, ready, relay,
    kv_s, kv_r, qd_s, qd_r, st_s, st_r, id_s, id_r,
    h2_s, h2_r, h2i_s, h2i_r, pt_s, pt_r, pti_s, pti_r,
    r1_s, r2_s, r2_r, oq_s, oq_r, okv_s, okv_r,
):
    U, B = uly_count, blk_count
    T = q_hbm.shape[0]
    R = T * U
    KH = KEY_VALUE_HEADS // U
    D = HEAD_SIZE
    GD = GROUP * D
    G = KH * GROUP
    scale = 1.0 / math.sqrt(D)
    u = lax.axis_index("uly")
    b = lax.axis_index("blk")
    odd = lax.rem(b, 2)
    even = odd == 0
    mate = b + 1 - 2 * odd

    def at(blk, uly):
        return {"blk": blk, "uly": uly}

    def rcopy(src, dst, ssem, rsem, dev):
        return pltpu.make_async_remote_copy(
            src_ref=src, dst_ref=dst, send_sem=ssem, recv_sem=rsem,
            device_id=dev, device_id_type=pl.DeviceIdType.MESH,
        )

    def cols(first, width):
        return pl.ds(pl.multiple_of(first, 128), width)

    def rows(place):
        return pl.ds(pl.multiple_of(place * T, T), T)

    has_up2 = b + 2 < B
    has_down2 = b >= 2
    sends_mate = jnp.logical_or(even, b >= 3)

    def load(src, dst, sem):
        return pltpu.make_async_copy(src, dst, loc_sem.at[sem])

    own_cols = cols(u * KH * D, KH * D)
    own_kv = [
        load(src.at[:, own_cols], kvb.at[0, i, rows(u), :], 0)
        for i, src in enumerate((k_hbm, v_hbm))
    ]
    load_ids = load(ids_hbm, ids_ref, 1)
    load_kv = [
        load(src.at[:, part], kv_ref.at[i, :, part], 2 if k else 0)
        for k in list(range(1, U)) + [0]
        for part in [cols(lax.rem(u + k, U) * KH * D, KH * D)]
        for i, src in enumerate((k_hbm, v_hbm))
    ]
    load_do = load(do_hbm, do_ref, 3)
    load_out = load(out_hbm, out_ref, 4)
    load_lp = load(lp_hbm, lp_ref, 5)
    for copy in [load_ids] + load_kv + own_kv + [load_do, load_out, load_lp]:
        copy.start()

    first = b < 2
    alone = jnp.logical_and(b == 0, U == 2)
    grouped = jnp.logical_not(alone)
    side_pair = lax.rem(b // 2, 2) == 1
    has_up4 = b + 4 < B
    barrier = pltpu.get_barrier_semaphore()

    def greet(sem, blk, uly):
        pl.semaphore_signal(
            sem, inc=1, device_id=at(blk, uly), device_id_type=pl.DeviceIdType.MESH
        )

    for k in range(1, U):
        greet(barrier, b, lax.rem(u + k, U))
    greet(barrier, mate, u)
    main_pair = jnp.logical_not(side_pair)
    hub = u == 0
    tree = u > 0

    @pl.when(jnp.logical_and(jnp.logical_or(hub, main_pair), has_up2))
    def _():
        greet(barrier, b + 2, u)

    @pl.when(jnp.logical_and(hub, has_down2))
    def _():
        greet(barrier, b - 2, u)

    @pl.when(jnp.logical_and(jnp.logical_and(tree, main_pair), has_up4))
    def _():
        greet(barrier, b + 4, u)

    met_up2 = jnp.logical_and(hub, has_up2)
    pl.semaphore_wait(barrier, U + has_down2.astype(jnp.int32) + met_up2.astype(jnp.int32))

    @pl.when(jnp.logical_and(tree, side_pair))
    def _():
        greet(ready, b - 2, u)

    @pl.when(jnp.logical_and(jnp.logical_and(tree, main_pair), b >= 4))
    def _():
        greet(relay, b - 4, u)

    own_q = [
        load(src.at[:, cols(u * KH * GD, KH * GD)], qdb.at[i, rows(u), :], 6)
        for i, src in enumerate((q_hbm, do_hbm))
    ]
    own_id = load(ids_hbm, idb.at[0, u], 7)
    load_q = load(q_hbm, q_ref, 6)

    def id_in(k, place, dev):
        return rcopy(ids_ref, idb.at[0, place], id_s.at[k - 1], id_r.at[k - 1], dev)

    def st_in(k, place, peer, dev):
        return rcopy(stat_ref.at[peer], statb.at[place], st_s.at[k - 1], st_r.at[k - 1], dev)

    def kv_in(k, j, place, peer, dev):
        return rcopy(
            kv_ref.at[:, :, cols((peer * KH + j) * D, D)],
            kvb.at[0, :, rows(place), cols(j * D, D)],
            kv_s.at[k - 1], kv_r.at[j, k - 1], dev,
        )

    def qd_in(k, which, j, place, peer, dev):
        ref = (q_hbm, do_ref)[which]
        return rcopy(
            ref.at[:, cols((peer * KH + j) * GD, GD)],
            qdb.at[which, rows(place), cols(j * GD, GD)],
            qd_s.at[k - 1], qd_r.at[j, k - 1], dev,
        )

    def await_bytes(ref, sem):
        pltpu.make_async_copy(ref, ref, sem).wait()

    def h2(j, place):
        return rcopy(
            kvb.at[0, :, rows(place), cols(j * D, D)], kvb.at[2, :, rows(place), cols(j * D, D)],
            h2_s.at[0], h2_r.at[j], at(b + 2, u),
        )

    peers = [(k, lax.rem(u + k, U), lax.rem(u + U - k, U)) for k in range(1, U)]
    soon = min(3, KH)

    @pl.when(hub)
    def _():
        await_bytes(kv_ref.at[:, :, pl.ds(0, min(2, U) * KH * D)], loc_sem.at[0])

        @pl.when(has_up2)
        def _():
            for j in range(soon):
                h2(j, u).start()

    load_ids.wait()
    for k, to, _ in peers:
        id_in(k, u, at(b, to)).start()
    if U > 1:
        await_bytes(kv_ref.at[:, :, pl.ds(0, (U - 1) * KH * D)], loc_sem.at[2])

    def send_kv(j):
        for k, to, _ in peers:
            kv_in(k, j, u, to, at(b, to)).start()

    def send_qd(j):
        for k, to, _ in peers:
            for which in range(2):
                qd_in(k, which, j, u, to, at(b, to)).start()

    for j in range(soon):
        send_kv(j)
    own_id.start()

    @pl.when(grouped)
    def _():
        for copy in own_q:
            copy.start()

    @pl.when(alone)
    def _():
        load_q.start()

    load_do.wait()
    load_out.wait()
    load_lp.wait()

    @pl.when(grouped)
    def _():
        send_qd(0)

    lane = lax.broadcasted_iota(jnp.int32, (T, 128), 1)
    table = jnp.zeros((T, 128), jnp.float32)
    for h in range(U * G):
        piece = slice(h * D, (h + 1) * D)
        total = jnp.sum(
            do_ref[:, piece].astype(jnp.float32) * out_ref[:, piece].astype(jnp.float32),
            axis=1, keepdims=True,
        )
        table = jnp.where(lane == h, total, table)
    table = table.T
    part0, part1 = lp_ref[:, 0, :], lp_ref[:, 1, :]
    highest = jnp.maximum(part0, part1)
    lse_rows = highest + jnp.log(jnp.exp(part0 - highest) + jnp.exp(part1 - highest))
    for p in range(U):
        stat_ref[p, :G, :] = lse_rows[p * G:(p + 1) * G] * LOG2_E
        stat_ref[p, G:2 * G, :] = table[p * G:(p + 1) * G]
    statb[u] = stat_ref[u]

    @pl.when(grouped)
    def _():
        for k, to, _ in peers:
            st_in(k, u, to, at(b, to)).start()

    for j in range(soon, KH):
        send_kv(j)

    @pl.when(grouped)
    def _():
        for j in range(1, KH):
            send_qd(j)

    def kx_in(j):
        head = cols(j * D, D)
        return rcopy(
            kv_ref.at[:, :, head], kx.at[:, :, head], qd_s.at[0], qd_r.at[j, 0], at(b, 1 - u)
        )

    def px_in(j):
        return rcopy(part.at[j], px.at[j], qd_s.at[0], st_r.at[0], at(b, 1 - u))

    @pl.when(jnp.logical_and(alone, u == 0))
    def _():
        for j in range(KH):
            kx_in(j).start()

    @pl.when(tree)
    def _():
        await_bytes(kv_ref.at[:, :, pl.ds(0, min(2, U) * KH * D)], loc_sem.at[0])

        @pl.when(has_up2)
        def _():
            pl.semaphore_wait(ready, 1)
            for j in range(soon):
                h2(j, u).start()

    @pl.when(jnp.logical_and(jnp.logical_and(tree, main_pair), has_up4))
    def _():
        pl.semaphore_wait(relay, 1)
        greet(ready, b + 2, u)

    def h2id():
        return rcopy(idb.at[0], idb.at[2], h2i_s.at[0], h2i_r.at[0], at(b + 2, u))

    def pt(j):
        return rcopy(
            kvb.at[2 * odd, :, :, cols(j * D, D)], kvb.at[1, :, :, cols(j * D, D)],
            pt_s.at[0], pt_r.at[j], at(mate, u),
        )

    def ptid():
        return rcopy(idb.at[2 * odd], idb.at[1], pti_s.at[0], pti_r.at[0], at(mate, u))

    own_id.wait()
    for k, _, frm in peers:
        id_in(k, frm, at(b, frm)).wait_recv()

    @pl.when(has_up2)
    def _():
        h2id().start()

    @pl.when(even)
    def _():
        ptid().start()

    def forward(j):
        for k, _, frm in peers:
            kv_in(k, j, frm, frm, at(b, frm)).wait_recv()

        @pl.when(has_up2)
        def _():
            for k, _, frm in peers:
                h2(j, frm).start()

        @pl.when(even)
        def _():
            pt(j).start()

    def make_bias(hop):
        for kp in range(U):
            key_ids = jnp.broadcast_to(idb[hop, kp, 0:1, :].astype(jnp.float32), (T, T)).T
            for qp in range(U):
                query_ids = idb[0, qp, 0:1, :].astype(jnp.float32)
                good = key_ids == query_ids
                if hop == 0:
                    kpos = lax.broadcasted_iota(jnp.int32, (T, T), 0) + kp * T
                    qpos = lax.broadcasted_iota(jnp.int32, (T, T), 1) + qp * T
                    good = jnp.logical_and(good, kpos <= qpos)
                bias[hop, kp * T:(kp + 1) * T, qp * T:(qp + 1) * T] = jnp.where(good, 0.0, FAR)

    make_bias(0)
    forward(0)
    if KH > 1:
        forward(1)

    @pl.when(has_up2)
    def _():
        for j in range(soon, KH):
            h2(j, u).start()

    @pl.when(has_down2)
    def _():
        h2id().wait_recv()
        make_bias(2)

        @pl.when(odd == 1)
        def _():
            ptid().start()

    def arrive2(j):
        @pl.when(has_down2)
        def _():
            await_bytes(kvb.at[2, :, :, cols(j * D, D)], h2_r.at[j])

            @pl.when(odd == 1)
            def _():
                pt(j).start()

    @pl.when(b >= 1)
    def _():
        ptid().wait_recv()
        make_bias(1)

    @pl.when(grouped)
    def _():
        await_bytes(qdb.at[:, rows(u), :], loc_sem.at[6])
        for k, _, frm in peers:
            st_in(k, frm, frm, at(b, frm)).wait_recv()

    if KH > 2:
        forward(2)
    arrive2(0)

    tile = min(TILE, R)
    steps = R // tile
    per = tile // T if tile >= T else 1

    def stat_row(row, qt):
        parts = [statb[qt * per + i, pl.ds(row, 1), :] for i in range(per)]
        return parts[0] if per == 1 else jnp.concatenate(parts, axis=1)

    def hop_grads(hop, j, acc):
        def key_step(kt, _):
            krow = pl.ds(pl.multiple_of(kt * tile, tile), tile)
            kc = kvb[hop, 0, krow, cols(j * D, D)]
            vc = kvb[hop, 1, krow, cols(j * D, D)]

            def query_step(qt, carry):
                dk, dv = carry
                qrow = pl.ds(pl.multiple_of(qt * tile, tile), tile)
                heads = [cols(j * GD + g * D, D) for g in range(GROUP)]
                weights, score_grads = [], []
                for g in range(GROUP):
                    lse = stat_row(j * GROUP + g, qt)
                    delta = stat_row(G + j * GROUP + g, qt)
                    w = jnp.exp2(
                        dot_nt(kc, qdb[0, qrow, heads[g]]) * (scale * LOG2_E) - lse + bias[hop, krow, qrow]
                    )
                    ds = w * (dot_nt(vc, qdb[1, qrow, heads[g]]) - delta)
                    score_grads.append(ds.astype(jnp.bfloat16))
                    weights.append(w.astype(jnp.bfloat16))
                queries = jnp.concatenate([qdb[0, qrow, heads[g]] for g in range(GROUP)], axis=0)
                cotangents = jnp.concatenate([qdb[1, qrow, heads[g]] for g in range(GROUP)], axis=0)
                dv = dot_nn(jnp.concatenate(weights, axis=1), cotangents) + dv
                dk = dot_nn(jnp.concatenate(score_grads, axis=1), queries) + dk
                for g in range(GROUP):
                    dqacc[qrow, g * D:(g + 1) * D] += dot_tn(score_grads[g], kc)
                return dk, dv

            if steps == 1:
                dk, dv = query_step(0, (0.0, 0.0))
            else:
                zero = jnp.zeros((tile, D), jnp.float32)
                dk, dv = lax.fori_loop(0, steps, query_step, (zero, zero))
            acc[j, 0, krow, :] = (dk * scale).astype(acc.dtype)
            acc[j, 1, krow, :] = dv.astype(acc.dtype)
            return 0

        if steps == 1:
            key_step(0, 0)
        else:
            lax.fori_loop(0, steps, key_step, 0)

    def give1(j):
        return rcopy(ret1.at[j], in1.at[j], r1_s.at[0], kv_r.at[j, 0], at(mate, u))

    def give2(j):
        return rcopy(ret2.at[j], in2.at[j], r2_s.at[0], r2_r.at[j], at(b - 2, u))

    def give2_part(which):
        return rcopy(
            ret2.at[KH - 1, which], in2.at[KH - 1, which],
            r2_s.at[0], r2_r.at[KH - 1 + which], at(b - 2, u),
        )

    def straight(j, place):
        return rcopy(
            ret2.at[j, :, rows(place), :], in2.at[j, :, rows(u), :],
            r2_s.at[0], r2_r.at[j], at(0, place),
        )

    def oq(k, j, place, dev):
        return rcopy(
            dqs.at[j, rows(place), :], dq_ref.at[:, cols((u * KH + j) * GD, GD)],
            oq_s.at[k - 1], oq_r.at[k - 1], dev,
        )

    def okv(k, j, place, dev):
        return rcopy(
            dkvs.at[j, :, rows(place), :], dkv_ref.at[:, :, cols((u * KH + j) * D, D)],
            okv_s.at[k - 1], okv_r.at[k - 1], dev,
        )

    def compute(j):
        for k, _, frm in peers:
            await_bytes(qdb.at[:, rows(frm), cols(j * GD, GD)], qd_r.at[j, k - 1])
        dqacc[...] = jnp.zeros_like(dqacc)

        @pl.when(b >= 1)
        def _():
            pt(j).wait_recv()
            hop_grads(1, j, ret1)
            give1(j).start()

        @pl.when(j + 3 < KH)
        def _():
            forward(jnp.minimum(j + 3, KH - 1))

        @pl.when(j + 1 < KH)
        def _():
            arrive2(jnp.minimum(j + 1, KH - 1))

        @pl.when(has_down2)
        def _():
            hop_grads(2, j, acc2)

        @pl.when(even)
        def _():
            stage_a(j)

        hop_grads(0, j, acc0)

        dqs[j] = (dqacc[...] * scale).astype(jnp.bfloat16)
        for k, to, _ in peers:
            oq(k, j, to, at(b, to)).start()
        dq_ref[:, cols((u * KH + j) * GD, GD)] = dqs[j, rows(u), :]

        @pl.when(odd == 1)
        def _():
            stage_a(j)

    def stage_a(j):
        @pl.when(jnp.logical_and(odd == 1, has_down2))
        def _():
            give1(j).wait_recv()
            ret2[j] = (acc2[j] + in1[j].astype(jnp.float32)).astype(jnp.bfloat16)

        @pl.when(jnp.logical_and(even, has_down2))
        def _():
            ret2[j] = acc2[j].astype(jnp.bfloat16)

        to_alone = jnp.logical_and(b == 2, U == 2)

        to_grouped = jnp.logical_and(has_down2, jnp.logical_not(to_alone))

        @pl.when(jnp.logical_and(to_grouped, j < KH - 1))
        def _():
            give2(j).start()

        @pl.when(jnp.logical_and(to_grouped, j == KH - 1))
        def _():
            for which in range(2):
                give2_part(which).start()

        @pl.when(to_alone)
        def _():
            straight(j, u).start()
            straight(j, 1 - u).start()

    def stage_b(j):
        @pl.when(even)
        def _():
            give1(j).wait_recv()
            acc0[j] += in1[j].astype(jnp.float32)

        @pl.when(has_up2)
        def _():
            give2(j).wait_recv()
            acc0[j] += in2[j].astype(jnp.float32)

        dkvs[j] = acc0[j].astype(jnp.bfloat16)
        for k, to, _ in peers:
            okv(k, j, to, at(b, to)).start()
        dkv_ref[:, :, cols((u * KH + j) * D, D)] = dkvs[j, :, rows(u), :]

    def stage_b_last():
        j = KH - 1

        @pl.when(even)
        def _():
            give1(j).wait_recv()
            acc0[j] += in1[j].astype(jnp.float32)

        for which in range(2):
            @pl.when(has_up2)
            def _():
                give2_part(which).wait_recv()
                acc0[j, which] += in2[j, which].astype(jnp.float32)

            dkvs[j, which] = acc0[j, which].astype(jnp.bfloat16)
            head = cols((u * KH + j) * D, D)
            for k, to, _ in peers:
                rcopy(
                    dkvs.at[j, which, rows(to), :], dkv_ref.at[which, :, head],
                    okv_s.at[k - 1], okv_r.at[k - 1], at(b, to),
                ).start()
            dkv_ref[which, :, head] = dkvs[j, which, rows(u), :]

    def head_step(j, _):
        compute(j)

        @pl.when(jnp.logical_and(j >= 2, b >= 2))
        def _():
            stage_b(jnp.maximum(j - 2, 0))

        return 0

    def alone_block(h, kc, vc, mask):
        heads = [cols(h * GD + g * D, D) for g in range(GROUP)]
        plane = h // KH
        row = (h - plane * KH) * GROUP
        weights, score_grads = [], []
        for g in range(GROUP):
            lse = stat_ref[plane, pl.ds(row + g, 1), :]
            delta = stat_ref[plane, pl.ds(G + row + g, 1), :]
            w = jnp.exp2(dot_nt(kc, q_ref[:, heads[g]]) * (scale * LOG2_E) - lse + mask)
            ds = w * (dot_nt(vc, do_ref[:, heads[g]]) - delta)
            score_grads.append(ds.astype(jnp.bfloat16))
            weights.append(w.astype(jnp.bfloat16))
        queries = jnp.concatenate([q_ref[:, c] for c in heads], axis=0)
        cotangents = jnp.concatenate([do_ref[:, c] for c in heads], axis=0)
        dv = dot_nn(jnp.concatenate(weights, axis=1), cotangents)
        dk = dot_nn(jnp.concatenate(score_grads, axis=1), queries) * scale
        return dk, dv, [dot_tn(ds, kc) * scale for ds in score_grads]

    def alone_own(j, _):
        for side in range(2):
            h = (u if side == 0 else 1 - u) * KH + j
            head = cols(h * D, D)
            dk, dv, dq = alone_block(
                h, kv_ref[0, :, head], kv_ref[1, :, head], bias[0, rows(u), rows(u)]
            )
            for g in range(GROUP):
                dqt[side, j, :, g * D:(g + 1) * D] = dq[g]
            if side == 0:
                acc0[j, 0, rows(u), :] = dk
                acc0[j, 1, rows(u), :] = dv
            else:
                loc1[j, 0] = dk
                loc1[j, 1] = dv
        return 0

    def alone_store(j, _):
        for side in range(2):
            h = (u if side == 0 else 1 - u) * KH + j
            dq_ref[:, cols(h * GD, GD)] = dqt[side, j].astype(jnp.bfloat16)
        return 0

    def alone_near(j, _):
        head = cols(j * D, D)
        dk, dv, dq = alone_block(
            KH + j, kvb[0, 0, rows(0), head], kvb[0, 1, rows(0), head], bias[0, rows(0), rows(1)]
        )
        for g in range(GROUP):
            dqt[0, j, :, g * D:(g + 1) * D] += dq[g]
        acc0[j, 0, rows(0), :] = dk
        acc0[j, 1, rows(0), :] = dv
        return 0

    def alone_far(j, _):
        head = cols(j * D, D)
        kx_in(j).wait_recv()
        dk, dv, dq = alone_block(j, kx[0, :, head], kx[1, :, head], bias[0, rows(0), rows(1)])
        part[j, 0] = dk.astype(jnp.bfloat16)
        part[j, 1] = dv.astype(jnp.bfloat16)
        px_in(j).start()
        for g in range(GROUP):
            dqt[1, j, :, g * D:(g + 1) * D] += dq[g]
        return 0

    def alone_merge(j, _):
        give1(j).wait_recv()
        acc0[j] += in1[j].astype(jnp.float32)
        dkvs[j] = acc0[j].astype(jnp.bfloat16)
        okv(1, j, 1 - u, at(b, 1 - u)).start()
        return 0

    def alone_finish(j, _):
        mine = cols((u * KH + j) * D, D)
        other = cols(((1 - u) * KH + j) * D, D)

        @pl.when(has_up2)
        def _():
            await_bytes(in2.at[j], r2_r.at[j])
            acc0[j, :, rows(u), :] += in2[j, :, rows(u), :].astype(jnp.float32)
            loc1[j] += in2[j, :, rows(1 - u), :].astype(jnp.float32)

        dkv_ref[:, :, mine] = acc0[j, :, rows(u), :].astype(jnp.bfloat16)
        dkv_ref[:, :, other] = (dkv_ref[:, :, other].astype(jnp.float32) + loc1[j]).astype(jnp.bfloat16)
        return 0

    @pl.when(grouped)
    def _():
        lax.fori_loop(0, KH, head_step, 0)
        late = min(2, KH)

        def last_step(j, _):
            stage_b(j)
            return 0

        lax.fori_loop(jnp.where(first, 0, KH - late), KH - 1, last_step, 0)
        stage_b_last()

    if U == 2:
        @pl.when(alone)
        def _():
            load_q.wait()
            alone_own(0, 0)
            for j in range(3, KH):
                forward(j)
            lax.fori_loop(1, KH, alone_own, 0)

            @pl.when(u == 0)
            def _():
                for j in range(KH):
                    acc0[j, :, rows(1), :] = jnp.zeros((2, T, D), jnp.float32)

            @pl.when(u == 1)
            def _():
                lax.fori_loop(0, KH, alone_near, 0)
                lax.fori_loop(0, KH, alone_far, 0)

            lax.fori_loop(0, KH, alone_merge, 0)
            lax.fori_loop(0, KH, alone_store, 0)

            @pl.when(u == 0)
            def _():
                await_bytes(px, st_r.at[0])
                for j in range(KH):
                    acc0[j, :, rows(0), :] += px[j].astype(jnp.float32)

            await_bytes(dkv_ref.at[:, :, cols((1 - u) * KH * D, KH * D)], okv_r.at[0])
            lax.fori_loop(0, KH, alone_finish, 0)

            @pl.when(u == 0)
            def _():
                await_bytes(kx, qd_s.at[0])

            @pl.when(u == 1)
            def _():
                await_bytes(part, qd_s.at[0])

    for k, to, _ in peers:
        id_in(k, u, at(b, to)).wait_send()
        await_bytes(kv_ref.at[:, :, cols(to * KH * D, KH * D)], kv_s.at[k - 1])

    @pl.when(grouped)
    def _():
        for k, to, _ in peers:
            st_in(k, u, to, at(b, to)).wait_send()
            await_bytes(qdb.at[:, rows(0), :], qd_s.at[k - 1])

    @pl.when(has_up2)
    def _():
        h2id().wait_send()
        await_bytes(kvb.at[0], h2_s.at[0])

    @pl.when(sends_mate)
    def _():
        ptid().wait_send()
        await_bytes(kvb.at[0], pt_s.at[0])

    @pl.when(b >= 1)
    def _():
        await_bytes(ret1, r1_s.at[0])

    @pl.when(has_down2)
    def _():
        await_bytes(ret2, r2_s.at[0])

    for k, to, _ in peers:
        await_bytes(dkvs.at[:, :, rows(to), :], okv_s.at[k - 1])

    @pl.when(grouped)
    def _():
        for k, to, frm in peers:
            await_bytes(dqs.at[:, rows(to), :], oq_s.at[k - 1])
            await_bytes(dq_ref.at[:, cols(frm * KH * GD, KH * GD)], oq_r.at[k - 1])
            await_bytes(dkv_ref.at[:, :, cols(frm * KH * D, KH * D)], okv_r.at[k - 1])


def close_kernel(q_in, kv_in, q_out, k_out, v_out, sem):
    half = q_in.shape[0] // 2
    moves = [
        (q_in.at[pl.ds(0, half)], q_out.at[pl.ds(0, half)]),
        (q_in.at[pl.ds(half, half)], q_out.at[pl.ds(half, half)]),
        (kv_in.at[0], k_out),
        (kv_in.at[1], v_out),
    ]
    copies = [pltpu.make_async_copy(src, dst, sem.at[i]) for i, (src, dst) in enumerate(moves)]
    for copy in copies:
        copy.start()
    for copy in copies:
        copy.wait()


def per_device(uly_count, blk_count, q, k, v, out, grad, lse_parts, segment_ids):
    U, B = uly_count, blk_count
    T = q.shape[0]
    R = T * U
    KH = KEY_VALUE_HEADS // U
    G = KH * GROUP
    D = HEAD_SIZE
    GD = GROUP * D
    stat_rows = -(-2 * G // 8) * 8
    parts = lse_parts.transpose(1, 2, 0)
    ids = segment_ids.reshape(1, T)
    bf, f32 = jnp.bfloat16, jnp.float32
    n = max(U - 1, 1)
    dma = pltpu.SemaphoreType.DMA
    sems = []
    for send, recv in [
        ((n,), (KH, n)), ((n,), (KH, n)), ((n,), (n,)), ((n,), (n,)),
        ((1,), (KH,)), ((1,), (1,)), ((1,), (KH,)), ((1,), (1,)),
        ((1,), None), ((1,), (KH + 1,)), ((n,), (n,)), ((n,), (n,)),
    ]:
        sems += [dma(shape) for shape in (send, recv) if shape is not None]
    vm = pltpu.VMEM
    in_vmem = pl.BlockSpec(memory_space=pltpu.VMEM)
    in_hbm = pl.BlockSpec(memory_space=pltpu.HBM)
    results = pl.pallas_call(
        functools.partial(kernel, U, B),
        out_shape=(vm(q.shape, bf), vm((2,) + k.shape, bf)),
        in_specs=[in_hbm] * 7,
        out_specs=(in_vmem, in_vmem),
        scratch_shapes=[
            vm((2, R, G * D), bf),
            vm((3, 2, R, KH * D), bf),
            vm((U, stat_rows, T), f32),
            vm((3, U, 1, T), jnp.int32),
            vm((3, R, R), f32),
            vm((R, GROUP * D), f32),
            vm((KH, 2, R, D), f32),
            vm((KH, 2, R, D), f32),
            vm((KH, R, GROUP * D), bf),
            vm((KH, 2, R, D), bf),
            vm((KH, 2, R, D), bf),
            vm((KH, 2, R, D), bf),
            vm((KH, 2, R, D), bf),
            vm((KH, 2, R, D), bf),
            vm(q.shape, bf),
            vm((2,) + k.shape, bf),
            vm(q.shape, bf),
            vm(parts.shape, f32),
            vm((1, T), jnp.int32),
            vm((U, stat_rows, T), f32),
            vm(q.shape, bf),
            vm((2, T, KH * D), bf),
            vm((KH, 2, T, D), f32),
            vm((KH, 2, T, D), bf),
            vm((KH, 2, T, D), bf),
            vm((2, KH, T, GD), f32),
            dma((8,)),
            pltpu.SemaphoreType.REGULAR,
            pltpu.SemaphoreType.REGULAR,
        ] + sems,
        compiler_params=pltpu.CompilerParams(
            collective_id=0, has_side_effects=True, vmem_limit_bytes=56 << 20
        ),
    )(q, grad, k, v, out, parts, ids)
    results = [pltpu.with_memory_space_constraint(r, pltpu.VMEM) for r in results]
    return pl.pallas_call(
        close_kernel,
        out_shape=tuple(jax.ShapeDtypeStruct(r.shape, r.dtype) for r in (q, k, v)),
        in_specs=[in_vmem] * 2,
        out_specs=(in_hbm,) * 3,
        scratch_shapes=[dma((4,))],
        compiler_params=pltpu.CompilerParams(vmem_limit_bytes=8 << 20),
    )(*results)


def solution(mesh):
    spec = P(("blk", "uly"), None)
    body = functools.partial(per_device, mesh.shape["uly"], mesh.shape["blk"])
    return jax.shard_map(
        body,
        mesh=mesh,
        in_specs=(spec, spec, spec, spec, spec, P(("blk", "uly"), None, None), P(("blk", "uly"))),
        out_specs=(spec, spec, spec),
        check_vma=False,
    )
```

```python
import functools
import math

import jax
import jax.numpy as jnp
from jax import lax
from jax.experimental import pallas as pl
from jax.experimental.pallas import tpu as pltpu
from jax.sharding import PartitionSpec as P

HEAD_SIZE = 128
QUERY_HEADS = 16
KEY_VALUE_HEADS = 8
GROUP = QUERY_HEADS // KEY_VALUE_HEADS
TILE = 256
FAR = -1e30
LOG2_E = math.log2(math.e)


def dot_nt(a, b):
    return lax.dot_general(a, b, (((1,), (1,)), ((), ())), preferred_element_type=jnp.float32)


def dot_nn(a, b):
    return lax.dot_general(a, b, (((1,), (0,)), ((), ())), preferred_element_type=jnp.float32)


def dot_tn(a, b):
    return lax.dot_general(a, b, (((0,), (0,)), ((), ())), preferred_element_type=jnp.float32)


def kernel(
    uly_count, blk_count,
    q_hbm, do_hbm, k_hbm, v_hbm, out_hbm, lp_hbm, ids_hbm,
    dq_ref, dkv_ref,
    qdb, kvb, statb, idb, bias,
    dqacc, acc0, acc2, dqs, ret1, ret2, in1, in2, dkvs,
    do_ref, kv_ref, out_ref, lp_ref, ids_ref, stat_ref,
    q_ref, kx, loc1, part, px, dqt,
    loc_sem, ready, relay,
    kv_s, kv_r, qd_s, qd_r, st_s, st_r, id_s, id_r,
    h2_s, h2_r, h2i_s, h2i_r, pt_s, pt_r, pti_s, pti_r,
    r1_s, r2_s, r2_r, oq_s, oq_r, okv_s, okv_r,
):
    U, B = uly_count, blk_count
    T = q_hbm.shape[0]
    R = T * U
    KH = KEY_VALUE_HEADS // U
    D = HEAD_SIZE
    GD = GROUP * D
    G = KH * GROUP
    scale = 1.0 / math.sqrt(D)
    u = lax.axis_index("uly")
    b = lax.axis_index("blk")
    odd = lax.rem(b, 2)
    even = odd == 0
    mate = b + 1 - 2 * odd

    def at(blk, uly):
        return {"blk": blk, "uly": uly}

    def rcopy(src, dst, ssem, rsem, dev):
        return pltpu.make_async_remote_copy(
            src_ref=src, dst_ref=dst, send_sem=ssem, recv_sem=rsem,
            device_id=dev, device_id_type=pl.DeviceIdType.MESH,
        )

    def cols(first, width):
        return pl.ds(pl.multiple_of(first, 128), width)

    def rows(place):
        return pl.ds(pl.multiple_of(place * T, T), T)

    has_up2 = b + 2 < B
    has_down2 = b >= 2
    sends_mate = jnp.logical_or(even, b >= 3)

    def load(src, dst, sem):
        return pltpu.make_async_copy(src, dst, loc_sem.at[sem])

    own_cols = cols(u * KH * D, KH * D)
    own_kv = [
        load(src.at[:, own_cols], kvb.at[0, i, rows(u), :], 0)
        for i, src in enumerate((k_hbm, v_hbm))
    ]
    load_ids = load(ids_hbm, ids_ref, 1)
    load_kv = [
        load(src.at[:, part], kv_ref.at[i, :, part], 2 if k else 0)
        for k in list(range(1, U)) + [0]
        for part in [cols(lax.rem(u + k, U) * KH * D, KH * D)]
        for i, src in enumerate((k_hbm, v_hbm))
    ]
    load_do = load(do_hbm, do_ref, 3)
    load_out = load(out_hbm, out_ref, 4)
    load_lp = load(lp_hbm, lp_ref, 5)
    for copy in [load_ids] + load_kv + own_kv + [load_do, load_out, load_lp]:
        copy.start()

    first = b < 2
    alone = jnp.logical_and(b == 0, U == 2)
    grouped = jnp.logical_not(alone)
    side_pair = lax.rem(b // 2, 2) == 1
    has_up4 = b + 4 < B
    barrier = pltpu.get_barrier_semaphore()

    def greet(sem, blk, uly):
        pl.semaphore_signal(
            sem, inc=1, device_id=at(blk, uly), device_id_type=pl.DeviceIdType.MESH
        )

    for k in range(1, U):
        greet(barrier, b, lax.rem(u + k, U))
    greet(barrier, mate, u)
    main_pair = jnp.logical_not(side_pair)
    hub = u == 0
    tree = u > 0

    @pl.when(jnp.logical_and(jnp.logical_or(hub, main_pair), has_up2))
    def _():
        greet(barrier, b + 2, u)

    @pl.when(jnp.logical_and(hub, has_down2))
    def _():
        greet(barrier, b - 2, u)

    @pl.when(jnp.logical_and(jnp.logical_and(tree, main_pair), has_up4))
    def _():
        greet(barrier, b + 4, u)

    met_up2 = jnp.logical_and(hub, has_up2)
    pl.semaphore_wait(barrier, U + has_down2.astype(jnp.int32) + met_up2.astype(jnp.int32))

    @pl.when(jnp.logical_and(tree, side_pair))
    def _():
        greet(ready, b - 2, u)

    @pl.when(jnp.logical_and(jnp.logical_and(tree, main_pair), b >= 4))
    def _():
        greet(relay, b - 4, u)

    own_q = [
        load(src.at[:, cols(u * KH * GD, KH * GD)], qdb.at[i, rows(u), :], 6)
        for i, src in enumerate((q_hbm, do_hbm))
    ]
    own_id = load(ids_hbm, idb.at[0, u], 7)
    load_q = load(q_hbm, q_ref, 6)

    def id_in(k, place, dev):
        return rcopy(ids_ref, idb.at[0, place], id_s.at[k - 1], id_r.at[k - 1], dev)

    def st_in(k, place, peer, dev):
        return rcopy(stat_ref.at[peer], statb.at[place], st_s.at[k - 1], st_r.at[k - 1], dev)

    def kv_in(k, j, place, peer, dev):
        return rcopy(
            kv_ref.at[:, :, cols((peer * KH + j) * D, D)],
            kvb.at[0, :, rows(place), cols(j * D, D)],
            kv_s.at[k - 1], kv_r.at[j, k - 1], dev,
        )

    def qd_in(k, which, j, place, peer, dev):
        ref = (q_hbm, do_ref)[which]
        return rcopy(
            ref.at[:, cols((peer * KH + j) * GD, GD)],
            qdb.at[which, rows(place), cols(j * GD, GD)],
            qd_s.at[k - 1], qd_r.at[j, k - 1], dev,
        )

    def await_bytes(ref, sem):
        pltpu.make_async_copy(ref, ref, sem).wait()

    def h2(j, place):
        return rcopy(
            kvb.at[0, :, rows(place), cols(j * D, D)], kvb.at[2, :, rows(place), cols(j * D, D)],
            h2_s.at[0], h2_r.at[j], at(b + 2, u),
        )

    peers = [(k, lax.rem(u + k, U), lax.rem(u + U - k, U)) for k in range(1, U)]
    soon = min(3, KH)

    @pl.when(hub)
    def _():
        await_bytes(kv_ref.at[:, :, pl.ds(0, min(2, U) * KH * D)], loc_sem.at[0])

        @pl.when(has_up2)
        def _():
            for j in range(soon):
                h2(j, u).start()

    load_ids.wait()
    for k, to, _ in peers:
        id_in(k, u, at(b, to)).start()
    if U > 1:
        await_bytes(kv_ref.at[:, :, pl.ds(0, (U - 1) * KH * D)], loc_sem.at[2])

    def send_kv(j):
        for k, to, _ in peers:
            kv_in(k, j, u, to, at(b, to)).start()

    def send_qd(j):
        for k, to, _ in peers:
            for which in range(2):
                qd_in(k, which, j, u, to, at(b, to)).start()

    for j in range(KH):
        send_kv(j)
    own_id.start()

    @pl.when(grouped)
    def _():
        for copy in own_q:
            copy.start()

    @pl.when(alone)
    def _():
        load_q.start()

    load_do.wait()
    load_out.wait()
    load_lp.wait()

    @pl.when(grouped)
    def _():
        send_qd(0)

    lane = lax.broadcasted_iota(jnp.int32, (T, 128), 1)
    table = jnp.zeros((T, 128), jnp.float32)
    for h in range(U * G):
        piece = slice(h * D, (h + 1) * D)
        total = jnp.sum(
            do_ref[:, piece].astype(jnp.float32) * out_ref[:, piece].astype(jnp.float32),
            axis=1, keepdims=True,
        )
        table = jnp.where(lane == h, total, table)
    table = table.T
    part0, part1 = lp_ref[:, 0, :], lp_ref[:, 1, :]
    highest = jnp.maximum(part0, part1)
    lse_rows = highest + jnp.log(jnp.exp(part0 - highest) + jnp.exp(part1 - highest))
    for p in range(U):
        stat_ref[p, :G, :] = lse_rows[p * G:(p + 1) * G] * LOG2_E
        stat_ref[p, G:2 * G, :] = table[p * G:(p + 1) * G]
    statb[u] = stat_ref[u]

    @pl.when(grouped)
    def _():
        for k, to, _ in peers:
            st_in(k, u, to, at(b, to)).start()


    @pl.when(grouped)
    def _():
        for j in range(1, KH):
            send_qd(j)

    def kx_in(j):
        head = cols(j * D, D)
        return rcopy(
            kv_ref.at[:, :, head], kx.at[:, :, head], qd_s.at[0], qd_r.at[j, 0], at(b, 1 - u)
        )

    def px_in(j):
        return rcopy(part.at[j], px.at[j], qd_s.at[0], st_r.at[0], at(b, 1 - u))

    @pl.when(jnp.logical_and(alone, u == 0))
    def _():
        for j in range(KH):
            kx_in(j).start()

    @pl.when(tree)
    def _():
        await_bytes(kv_ref.at[:, :, pl.ds(0, min(2, U) * KH * D)], loc_sem.at[0])

        @pl.when(has_up2)
        def _():
            pl.semaphore_wait(ready, 1)
            for j in range(soon):
                h2(j, u).start()

    @pl.when(jnp.logical_and(jnp.logical_and(tree, main_pair), has_up4))
    def _():
        pl.semaphore_wait(relay, 1)
        greet(ready, b + 2, u)

    def h2id():
        return rcopy(idb.at[0], idb.at[2], h2i_s.at[0], h2i_r.at[0], at(b + 2, u))

    def pt(j):
        return rcopy(
            kvb.at[2 * odd, :, :, cols(j * D, D)], kvb.at[1, :, :, cols(j * D, D)],
            pt_s.at[0], pt_r.at[j], at(mate, u),
        )

    def ptid():
        return rcopy(idb.at[2 * odd], idb.at[1], pti_s.at[0], pti_r.at[0], at(mate, u))

    own_id.wait()
    for k, _, frm in peers:
        id_in(k, frm, at(b, frm)).wait_recv()

    @pl.when(has_up2)
    def _():
        h2id().start()

    @pl.when(even)
    def _():
        ptid().start()

    def forward(j):
        for k, _, frm in peers:
            kv_in(k, j, frm, frm, at(b, frm)).wait_recv()

        @pl.when(has_up2)
        def _():
            for k, _, frm in peers:
                h2(j, frm).start()

        @pl.when(even)
        def _():
            pt(j).start()

    def make_bias(hop):
        for kp in range(U):
            key_ids = jnp.broadcast_to(idb[hop, kp, 0:1, :].astype(jnp.float32), (T, T)).T
            for qp in range(U):
                query_ids = idb[0, qp, 0:1, :].astype(jnp.float32)
                good = key_ids == query_ids
                if hop == 0:
                    kpos = lax.broadcasted_iota(jnp.int32, (T, T), 0) + kp * T
                    qpos = lax.broadcasted_iota(jnp.int32, (T, T), 1) + qp * T
                    good = jnp.logical_and(good, kpos <= qpos)
                bias[hop, kp * T:(kp + 1) * T, qp * T:(qp + 1) * T] = jnp.where(good, 0.0, FAR)

    make_bias(0)
    forward(0)
    if KH > 1:
        forward(1)

    @pl.when(has_up2)
    def _():
        for j in range(soon, KH):
            h2(j, u).start()

    @pl.when(has_down2)
    def _():
        h2id().wait_recv()
        make_bias(2)

        @pl.when(odd == 1)
        def _():
            ptid().start()

    def arrive2(j):
        @pl.when(has_down2)
        def _():
            await_bytes(kvb.at[2, :, :, cols(j * D, D)], h2_r.at[j])

            @pl.when(odd == 1)
            def _():
                pt(j).start()

    @pl.when(b >= 1)
    def _():
        ptid().wait_recv()
        make_bias(1)

    @pl.when(grouped)
    def _():
        await_bytes(qdb.at[:, rows(u), :], loc_sem.at[6])
        for k, _, frm in peers:
            st_in(k, frm, frm, at(b, frm)).wait_recv()

    for j in range(2, KH):
        forward(j)
    arrive2(0)

    tile = min(TILE, R)
    steps = R // tile
    per = tile // T if tile >= T else 1

    def stat_row(row, qt):
        parts = [statb[qt * per + i, pl.ds(row, 1), :] for i in range(per)]
        return parts[0] if per == 1 else jnp.concatenate(parts, axis=1)

    def hop_grads(hop, j, acc):
        def key_step(kt, _):
            krow = pl.ds(pl.multiple_of(kt * tile, tile), tile)
            kc = kvb[hop, 0, krow, cols(j * D, D)]
            vc = kvb[hop, 1, krow, cols(j * D, D)]

            def query_step(qt, carry):
                dk, dv = carry
                qrow = pl.ds(pl.multiple_of(qt * tile, tile), tile)
                heads = [cols(j * GD + g * D, D) for g in range(GROUP)]
                weights, score_grads = [], []
                for g in range(GROUP):
                    lse = stat_row(j * GROUP + g, qt)
                    delta = stat_row(G + j * GROUP + g, qt)
                    w = jnp.exp2(
                        dot_nt(kc, qdb[0, qrow, heads[g]]) * (scale * LOG2_E) - lse + bias[hop, krow, qrow]
                    )
                    ds = w * (dot_nt(vc, qdb[1, qrow, heads[g]]) - delta)
                    score_grads.append(ds.astype(jnp.bfloat16))
                    weights.append(w.astype(jnp.bfloat16))
                queries = jnp.concatenate([qdb[0, qrow, heads[g]] for g in range(GROUP)], axis=0)
                cotangents = jnp.concatenate([qdb[1, qrow, heads[g]] for g in range(GROUP)], axis=0)
                dv = dot_nn(jnp.concatenate(weights, axis=1), cotangents) + dv
                dk = dot_nn(jnp.concatenate(score_grads, axis=1), queries) + dk
                for g in range(GROUP):
                    dqacc[qrow, g * D:(g + 1) * D] += dot_tn(score_grads[g], kc)
                return dk, dv

            if steps == 1:
                dk, dv = query_step(0, (0.0, 0.0))
            else:
                zero = jnp.zeros((tile, D), jnp.float32)
                dk, dv = lax.fori_loop(0, steps, query_step, (zero, zero))
            acc[j, 0, krow, :] = (dk * scale).astype(acc.dtype)
            acc[j, 1, krow, :] = dv.astype(acc.dtype)
            return 0

        if steps == 1:
            key_step(0, 0)
        else:
            lax.fori_loop(0, steps, key_step, 0)

    def give1(j):
        return rcopy(ret1.at[j], in1.at[j], r1_s.at[0], kv_r.at[j, 0], at(mate, u))

    def give2(j):
        return rcopy(ret2.at[j], in2.at[j], r2_s.at[0], r2_r.at[j], at(b - 2, u))

    def give2_part(which):
        return rcopy(
            ret2.at[KH - 1, which], in2.at[KH - 1, which],
            r2_s.at[0], r2_r.at[KH - 1 + which], at(b - 2, u),
        )

    def straight(j, place):
        return rcopy(
            ret2.at[j, :, rows(place), :], in2.at[j, :, rows(u), :],
            r2_s.at[0], r2_r.at[j], at(0, place),
        )

    def oq(k, j, place, dev):
        return rcopy(
            dqs.at[j, rows(place), :], dq_ref.at[:, cols((u * KH + j) * GD, GD)],
            oq_s.at[k - 1], oq_r.at[k - 1], dev,
        )

    def okv(k, j, place, dev):
        return rcopy(
            dkvs.at[j, :, rows(place), :], dkv_ref.at[:, :, cols((u * KH + j) * D, D)],
            okv_s.at[k - 1], okv_r.at[k - 1], dev,
        )

    def compute(j):
        for k, _, frm in peers:
            await_bytes(qdb.at[:, rows(frm), cols(j * GD, GD)], qd_r.at[j, k - 1])
        dqacc[...] = jnp.zeros_like(dqacc)

        @pl.when(b >= 1)
        def _():
            pt(j).wait_recv()
            hop_grads(1, j, ret1)
            give1(j).start()

        @pl.when(j + 1 < KH)
        def _():
            arrive2(jnp.minimum(j + 1, KH - 1))

        @pl.when(has_down2)
        def _():
            hop_grads(2, j, acc2)

        @pl.when(even)
        def _():
            stage_a(j)

        hop_grads(0, j, acc0)

        dqs[j] = (dqacc[...] * scale).astype(jnp.bfloat16)
        for k, to, _ in peers:
            oq(k, j, to, at(b, to)).start()
        dq_ref[:, cols((u * KH + j) * GD, GD)] = dqs[j, rows(u), :]

        @pl.when(odd == 1)
        def _():
            stage_a(j)

    def stage_a(j):
        @pl.when(jnp.logical_and(odd == 1, has_down2))
        def _():
            give1(j).wait_recv()
            ret2[j] = (acc2[j] + in1[j].astype(jnp.float32)).astype(jnp.bfloat16)

        @pl.when(jnp.logical_and(even, has_down2))
        def _():
            ret2[j] = acc2[j].astype(jnp.bfloat16)

        to_alone = jnp.logical_and(b == 2, U == 2)

        to_grouped = jnp.logical_and(has_down2, jnp.logical_not(to_alone))

        @pl.when(jnp.logical_and(to_grouped, j < KH - 1))
        def _():
            give2(j).start()

        @pl.when(jnp.logical_and(to_grouped, j == KH - 1))
        def _():
            for which in range(2):
                give2_part(which).start()

        @pl.when(to_alone)
        def _():
            straight(j, u).start()
            straight(j, 1 - u).start()

    def stage_b(j):
        @pl.when(even)
        def _():
            give1(j).wait_recv()
            acc0[j] += in1[j].astype(jnp.float32)

        @pl.when(has_up2)
        def _():
            give2(j).wait_recv()
            acc0[j] += in2[j].astype(jnp.float32)

        dkvs[j] = acc0[j].astype(jnp.bfloat16)
        for k, to, _ in peers:
            okv(k, j, to, at(b, to)).start()
        dkv_ref[:, :, cols((u * KH + j) * D, D)] = dkvs[j, :, rows(u), :]

    def stage_b_last():
        j = KH - 1

        @pl.when(even)
        def _():
            give1(j).wait_recv()
            acc0[j] += in1[j].astype(jnp.float32)

        for which in range(2):
            @pl.when(has_up2)
            def _():
                give2_part(which).wait_recv()
                acc0[j, which] += in2[j, which].astype(jnp.float32)

            dkvs[j, which] = acc0[j, which].astype(jnp.bfloat16)
            head = cols((u * KH + j) * D, D)
            for k, to, _ in peers:
                rcopy(
                    dkvs.at[j, which, rows(to), :], dkv_ref.at[which, :, head],
                    okv_s.at[k - 1], okv_r.at[k - 1], at(b, to),
                ).start()
            dkv_ref[which, :, head] = dkvs[j, which, rows(u), :]

    def head_step(j, _):
        compute(j)
        return 0

    def alone_block(h, kc, vc, mask):
        heads = [cols(h * GD + g * D, D) for g in range(GROUP)]
        plane = h // KH
        row = (h - plane * KH) * GROUP
        weights, score_grads = [], []
        for g in range(GROUP):
            lse = stat_ref[plane, pl.ds(row + g, 1), :]
            delta = stat_ref[plane, pl.ds(G + row + g, 1), :]
            w = jnp.exp2(dot_nt(kc, q_ref[:, heads[g]]) * (scale * LOG2_E) - lse + mask)
            ds = w * (dot_nt(vc, do_ref[:, heads[g]]) - delta)
            score_grads.append(ds.astype(jnp.bfloat16))
            weights.append(w.astype(jnp.bfloat16))
        queries = jnp.concatenate([q_ref[:, c] for c in heads], axis=0)
        cotangents = jnp.concatenate([do_ref[:, c] for c in heads], axis=0)
        dv = dot_nn(jnp.concatenate(weights, axis=1), cotangents)
        dk = dot_nn(jnp.concatenate(score_grads, axis=1), queries) * scale
        return dk, dv, [dot_tn(ds, kc) * scale for ds in score_grads]

    def alone_own(j, _):
        for side in range(2):
            h = (u if side == 0 else 1 - u) * KH + j
            head = cols(h * D, D)
            dk, dv, dq = alone_block(
                h, kv_ref[0, :, head], kv_ref[1, :, head], bias[0, rows(u), rows(u)]
            )
            for g in range(GROUP):
                dqt[side, j, :, g * D:(g + 1) * D] = dq[g]
            if side == 0:
                acc0[j, 0, rows(u), :] = dk
                acc0[j, 1, rows(u), :] = dv
            else:
                loc1[j, 0] = dk
                loc1[j, 1] = dv
        return 0

    def alone_store(j, _):
        for side in range(2):
            h = (u if side == 0 else 1 - u) * KH + j
            dq_ref[:, cols(h * GD, GD)] = dqt[side, j].astype(jnp.bfloat16)
        return 0

    def alone_near(j, _):
        head = cols(j * D, D)
        dk, dv, dq = alone_block(
            KH + j, kvb[0, 0, rows(0), head], kvb[0, 1, rows(0), head], bias[0, rows(0), rows(1)]
        )
        for g in range(GROUP):
            dqt[0, j, :, g * D:(g + 1) * D] += dq[g]
        acc0[j, 0, rows(0), :] = dk
        acc0[j, 1, rows(0), :] = dv
        return 0

    def alone_far(j, _):
        head = cols(j * D, D)
        kx_in(j).wait_recv()
        dk, dv, dq = alone_block(j, kx[0, :, head], kx[1, :, head], bias[0, rows(0), rows(1)])
        part[j, 0] = dk.astype(jnp.bfloat16)
        part[j, 1] = dv.astype(jnp.bfloat16)
        px_in(j).start()
        for g in range(GROUP):
            dqt[1, j, :, g * D:(g + 1) * D] += dq[g]
        return 0

    def alone_merge(j, _):
        give1(j).wait_recv()
        acc0[j] += in1[j].astype(jnp.float32)
        dkvs[j] = acc0[j].astype(jnp.bfloat16)
        okv(1, j, 1 - u, at(b, 1 - u)).start()
        return 0

    def alone_finish(j, _):
        mine = cols((u * KH + j) * D, D)
        other = cols(((1 - u) * KH + j) * D, D)

        @pl.when(has_up2)
        def _():
            await_bytes(in2.at[j], r2_r.at[j])
            acc0[j, :, rows(u), :] += in2[j, :, rows(u), :].astype(jnp.float32)
            loc1[j] += in2[j, :, rows(1 - u), :].astype(jnp.float32)

        dkv_ref[:, :, mine] = acc0[j, :, rows(u), :].astype(jnp.bfloat16)
        dkv_ref[:, :, other] = (dkv_ref[:, :, other].astype(jnp.float32) + loc1[j]).astype(jnp.bfloat16)
        return 0

    @pl.when(grouped)
    def _():
        lax.fori_loop(0, KH, head_step, 0)

        def last_step(j, _):
            stage_b(j)
            return 0

        lax.fori_loop(0, KH - 1, last_step, 0)
        stage_b_last()

    if U == 2:
        @pl.when(alone)
        def _():
            load_q.wait()
            lax.fori_loop(0, KH, alone_own, 0)

            @pl.when(u == 0)
            def _():
                for j in range(KH):
                    acc0[j, :, rows(1), :] = jnp.zeros((2, T, D), jnp.float32)

            @pl.when(u == 1)
            def _():
                lax.fori_loop(0, KH, alone_near, 0)
                lax.fori_loop(0, KH, alone_far, 0)

            lax.fori_loop(0, KH, alone_merge, 0)
            lax.fori_loop(0, KH, alone_store, 0)

            @pl.when(u == 0)
            def _():
                await_bytes(px, st_r.at[0])
                for j in range(KH):
                    acc0[j, :, rows(0), :] += px[j].astype(jnp.float32)

            await_bytes(dkv_ref.at[:, :, cols((1 - u) * KH * D, KH * D)], okv_r.at[0])
            lax.fori_loop(0, KH, alone_finish, 0)

            @pl.when(u == 0)
            def _():
                await_bytes(kx, qd_s.at[0])

            @pl.when(u == 1)
            def _():
                await_bytes(part, qd_s.at[0])

    for k, to, _ in peers:
        id_in(k, u, at(b, to)).wait_send()
        await_bytes(kv_ref.at[:, :, cols(to * KH * D, KH * D)], kv_s.at[k - 1])

    @pl.when(grouped)
    def _():
        for k, to, _ in peers:
            st_in(k, u, to, at(b, to)).wait_send()
            await_bytes(qdb.at[:, rows(0), :], qd_s.at[k - 1])

    @pl.when(has_up2)
    def _():
        h2id().wait_send()
        await_bytes(kvb.at[0], h2_s.at[0])

    @pl.when(sends_mate)
    def _():
        ptid().wait_send()
        await_bytes(kvb.at[0], pt_s.at[0])

    @pl.when(b >= 1)
    def _():
        await_bytes(ret1, r1_s.at[0])

    @pl.when(has_down2)
    def _():
        await_bytes(ret2, r2_s.at[0])

    for k, to, _ in peers:
        await_bytes(dkvs.at[:, :, rows(to), :], okv_s.at[k - 1])

    @pl.when(grouped)
    def _():
        for k, to, frm in peers:
            await_bytes(dqs.at[:, rows(to), :], oq_s.at[k - 1])
            await_bytes(dq_ref.at[:, cols(frm * KH * GD, KH * GD)], oq_r.at[k - 1])
            await_bytes(dkv_ref.at[:, :, cols(frm * KH * D, KH * D)], okv_r.at[k - 1])


def close_kernel(q_in, kv_in, q_out, k_out, v_out, sem):
    half = q_in.shape[0] // 2
    moves = [
        (q_in.at[pl.ds(0, half)], q_out.at[pl.ds(0, half)]),
        (q_in.at[pl.ds(half, half)], q_out.at[pl.ds(half, half)]),
        (kv_in.at[0], k_out),
        (kv_in.at[1], v_out),
    ]
    copies = [pltpu.make_async_copy(src, dst, sem.at[i]) for i, (src, dst) in enumerate(moves)]
    for copy in copies:
        copy.start()
    for copy in copies:
        copy.wait()


def per_device(uly_count, blk_count, q, k, v, out, grad, lse_parts, segment_ids):
    U, B = uly_count, blk_count
    T = q.shape[0]
    R = T * U
    KH = KEY_VALUE_HEADS // U
    G = KH * GROUP
    D = HEAD_SIZE
    GD = GROUP * D
    stat_rows = -(-2 * G // 8) * 8
    parts = lse_parts.transpose(1, 2, 0)
    ids = segment_ids.reshape(1, T)
    bf, f32 = jnp.bfloat16, jnp.float32
    n = max(U - 1, 1)
    dma = pltpu.SemaphoreType.DMA
    sems = []
    for send, recv in [
        ((n,), (KH, n)), ((n,), (KH, n)), ((n,), (n,)), ((n,), (n,)),
        ((1,), (KH,)), ((1,), (1,)), ((1,), (KH,)), ((1,), (1,)),
        ((1,), None), ((1,), (KH + 1,)), ((n,), (n,)), ((n,), (n,)),
    ]:
        sems += [dma(shape) for shape in (send, recv) if shape is not None]
    vm = pltpu.VMEM
    in_vmem = pl.BlockSpec(memory_space=pltpu.VMEM)
    in_hbm = pl.BlockSpec(memory_space=pltpu.HBM)
    results = pl.pallas_call(
        functools.partial(kernel, U, B),
        out_shape=(vm(q.shape, bf), vm((2,) + k.shape, bf)),
        in_specs=[in_hbm] * 7,
        out_specs=(in_vmem, in_vmem),
        scratch_shapes=[
            vm((2, R, G * D), bf),
            vm((3, 2, R, KH * D), bf),
            vm((U, stat_rows, T), f32),
            vm((3, U, 1, T), jnp.int32),
            vm((3, R, R), f32),
            vm((R, GROUP * D), f32),
            vm((KH, 2, R, D), f32),
            vm((KH, 2, R, D), f32),
            vm((KH, R, GROUP * D), bf),
            vm((KH, 2, R, D), bf),
            vm((KH, 2, R, D), bf),
            vm((KH, 2, R, D), bf),
            vm((KH, 2, R, D), bf),
            vm((KH, 2, R, D), bf),
            vm(q.shape, bf),
            vm((2,) + k.shape, bf),
            vm(q.shape, bf),
            vm(parts.shape, f32),
            vm((1, T), jnp.int32),
            vm((U, stat_rows, T), f32),
            vm(q.shape, bf),
            vm((2, T, KH * D), bf),
            vm((KH, 2, T, D), f32),
            vm((KH, 2, T, D), bf),
            vm((KH, 2, T, D), bf),
            vm((2, KH, T, GD), f32),
            dma((8,)),
            pltpu.SemaphoreType.REGULAR,
            pltpu.SemaphoreType.REGULAR,
        ] + sems,
        compiler_params=pltpu.CompilerParams(
            collective_id=0, has_side_effects=True, vmem_limit_bytes=56 << 20
        ),
    )(q, grad, k, v, out, parts, ids)
    results = [pltpu.with_memory_space_constraint(r, pltpu.VMEM) for r in results]
    return pl.pallas_call(
        close_kernel,
        out_shape=tuple(jax.ShapeDtypeStruct(r.shape, r.dtype) for r in (q, k, v)),
        in_specs=[in_vmem] * 2,
        out_specs=(in_hbm,) * 3,
        scratch_shapes=[dma((4,))],
        compiler_params=pltpu.CompilerParams(vmem_limit_bytes=8 << 20),
    )(*results)


def solution(mesh):
    spec = P(("blk", "uly"), None)
    body = functools.partial(per_device, mesh.shape["uly"], mesh.shape["blk"])
    return jax.shard_map(
        body,
        mesh=mesh,
        in_specs=(spec, spec, spec, spec, spec, P(("blk", "uly"), None, None), P(("blk", "uly"))),
        out_specs=(spec, spec, spec),
        check_vma=False,
    )
```

```python
import functools
import math

import jax
import jax.numpy as jnp
from jax import lax
from jax.experimental import pallas as pl
from jax.experimental.pallas import tpu as pltpu
from jax.sharding import PartitionSpec as P

HEAD_SIZE = 128
QUERY_HEADS = 16
KEY_VALUE_HEADS = 8
GROUP = QUERY_HEADS // KEY_VALUE_HEADS
TILE = 256
FAR = -1e30
LOG2_E = math.log2(math.e)


def dot_nt(a, b):
    return lax.dot_general(a, b, (((1,), (1,)), ((), ())), preferred_element_type=jnp.float32)


def dot_nn(a, b):
    return lax.dot_general(a, b, (((1,), (0,)), ((), ())), preferred_element_type=jnp.float32)


def dot_tn(a, b):
    return lax.dot_general(a, b, (((0,), (0,)), ((), ())), preferred_element_type=jnp.float32)


def kernel(
    uly_count, blk_count,
    q_hbm, do_hbm, k_hbm, v_hbm, out_hbm, lp_hbm, ids_hbm,
    dq_ref, dkv_ref,
    qdb, kvb, statb, idb, bias,
    dqacc, acc0, acc2, dqs, ret1, ret2, in1, in2, dkvs,
    do_ref, kv_ref, out_ref, lp_ref, ids_ref, stat_ref,
    q_ref, kx, loc1, part, px, dqt,
    loc_sem, ready, relay,
    kv_s, kv_r, qd_s, qd_r, st_s, st_r, id_s, id_r,
    h2_s, h2_r, h2i_s, h2i_r, pt_s, pt_r, pti_s, pti_r,
    r1_s, r2_s, r2_r, oq_s, oq_r, okv_s, okv_r,
):
    U, B = uly_count, blk_count
    T = q_hbm.shape[0]
    R = T * U
    KH = KEY_VALUE_HEADS // U
    D = HEAD_SIZE
    GD = GROUP * D
    G = KH * GROUP
    scale = 1.0 / math.sqrt(D)
    u = lax.axis_index("uly")
    b = lax.axis_index("blk")
    odd = lax.rem(b, 2)
    even = odd == 0
    mate = b + 1 - 2 * odd

    def at(blk, uly):
        return {"blk": blk, "uly": uly}

    def rcopy(src, dst, ssem, rsem, dev):
        return pltpu.make_async_remote_copy(
            src_ref=src, dst_ref=dst, send_sem=ssem, recv_sem=rsem,
            device_id=dev, device_id_type=pl.DeviceIdType.MESH,
        )

    def cols(first, width):
        return pl.ds(pl.multiple_of(first, 128), width)

    def rows(place):
        return pl.ds(pl.multiple_of(place * T, T), T)

    has_up2 = b + 2 < B
    has_down2 = b >= 2
    sends_mate = jnp.logical_or(even, b >= 3)

    def load(src, dst, sem):
        return pltpu.make_async_copy(src, dst, loc_sem.at[sem])

    own_cols = cols(u * KH * D, KH * D)
    own_kv = [
        load(src.at[:, own_cols], kvb.at[0, i, rows(u), :], 0)
        for i, src in enumerate((k_hbm, v_hbm))
    ]
    load_ids = load(ids_hbm, ids_ref, 1)
    others = list(range(1, U))
    load_kv = [
        load(src.at[:, part], kv_ref.at[i, :, part], sem)
        for sem, places, head, count in [
            (8, others, 0, 1), (2, others if KH > 1 else [], 1, KH - 1), (0, [0], 0, KH)
        ]
        for k in places
        for part in [cols((lax.rem(u + k, U) * KH + head) * D, count * D)]
        for i, src in enumerate((k_hbm, v_hbm))
    ]
    load_do = load(do_hbm, do_ref, 3)
    load_out = load(out_hbm, out_ref, 4)
    load_lp = load(lp_hbm, lp_ref, 5)
    for copy in load_kv[:2 * (U - 1)] + [load_ids] + load_kv[2 * (U - 1):] + own_kv + [load_do, load_out, load_lp]:
        copy.start()

    first = b < 2
    alone = jnp.logical_and(b == 0, U == 2)
    grouped = jnp.logical_not(alone)
    side_pair = lax.rem(b // 2, 2) == 1
    has_up4 = b + 4 < B
    barrier = pltpu.get_barrier_semaphore()

    def greet(sem, blk, uly):
        pl.semaphore_signal(
            sem, inc=1, device_id=at(blk, uly), device_id_type=pl.DeviceIdType.MESH
        )

    for k in range(1, U):
        greet(barrier, b, lax.rem(u + k, U))
    greet(barrier, mate, u)
    main_pair = jnp.logical_not(side_pair)
    hub = u == 0
    tree = u > 0

    @pl.when(jnp.logical_and(jnp.logical_or(hub, main_pair), has_up2))
    def _():
        greet(barrier, b + 2, u)

    @pl.when(jnp.logical_and(hub, has_down2))
    def _():
        greet(barrier, b - 2, u)

    @pl.when(jnp.logical_and(jnp.logical_and(tree, main_pair), has_up4))
    def _():
        greet(barrier, b + 4, u)

    met_up2 = jnp.logical_and(hub, has_up2)
    pl.semaphore_wait(barrier, U + has_down2.astype(jnp.int32) + met_up2.astype(jnp.int32))

    @pl.when(jnp.logical_and(tree, side_pair))
    def _():
        greet(ready, b - 2, u)

    @pl.when(jnp.logical_and(jnp.logical_and(tree, main_pair), b >= 4))
    def _():
        greet(relay, b - 4, u)

    own_q = [
        load(src.at[:, cols(u * KH * GD, KH * GD)], qdb.at[i, rows(u), :], 6)
        for i, src in enumerate((q_hbm, do_hbm))
    ]
    own_id = load(ids_hbm, idb.at[0, u], 7)
    load_q = load(q_hbm, q_ref, 6)

    def id_in(k, place, dev):
        return rcopy(ids_ref, idb.at[0, place], id_s.at[k - 1], id_r.at[k - 1], dev)

    def st_in(k, place, peer, dev):
        return rcopy(stat_ref.at[peer], statb.at[place], st_s.at[k - 1], st_r.at[k - 1], dev)

    def kv_in(k, j, place, peer, dev):
        return rcopy(
            kv_ref.at[:, :, cols((peer * KH + j) * D, D)],
            kvb.at[0, :, rows(place), cols(j * D, D)],
            kv_s.at[k - 1], kv_r.at[j, k - 1], dev,
        )

    def qd_in(k, which, j, place, peer, dev):
        ref = (q_hbm, do_ref)[which]
        return rcopy(
            ref.at[:, cols((peer * KH + j) * GD, GD)],
            qdb.at[which, rows(place), cols(j * GD, GD)],
            qd_s.at[k - 1], qd_r.at[j, k - 1], dev,
        )

    def await_bytes(ref, sem):
        pltpu.make_async_copy(ref, ref, sem).wait()

    def h2(j, place):
        return rcopy(
            kvb.at[0, :, rows(place), cols(j * D, D)], kvb.at[2, :, rows(place), cols(j * D, D)],
            h2_s.at[0], h2_r.at[j], at(b + 2, u),
        )

    peers = [(k, lax.rem(u + k, U), lax.rem(u + U - k, U)) for k in range(1, U)]
    soon = min(3, KH)

    @pl.when(hub)
    def _():
        await_bytes(kv_ref.at[:, :, pl.ds(0, min(2, U) * KH * D)], loc_sem.at[0])

        @pl.when(has_up2)
        def _():
            for j in range(soon):
                h2(j, u).start()

    def send_kv(j):
        for k, to, _ in peers:
            kv_in(k, j, u, to, at(b, to)).start()

    def send_qd(j):
        for k, to, _ in peers:
            for which in range(2):
                qd_in(k, which, j, u, to, at(b, to)).start()

    if U > 1:
        await_bytes(kv_ref.at[:, :, pl.ds(0, (U - 1) * D)], loc_sem.at[8])
    send_kv(0)
    load_ids.wait()
    for k, to, _ in peers:
        id_in(k, u, at(b, to)).start()
    if U > 1 and KH > 1:
        await_bytes(kv_ref.at[:, :, pl.ds(0, (U - 1) * (KH - 1) * D)], loc_sem.at[2])
    for j in range(1, KH):
        send_kv(j)
    own_id.start()

    @pl.when(grouped)
    def _():
        for copy in own_q:
            copy.start()

    @pl.when(alone)
    def _():
        load_q.start()

    load_do.wait()
    load_out.wait()
    load_lp.wait()

    @pl.when(grouped)
    def _():
        send_qd(0)

    lane = lax.broadcasted_iota(jnp.int32, (T, 128), 1)
    table = jnp.zeros((T, 128), jnp.float32)
    for h in range(U * G):
        piece = slice(h * D, (h + 1) * D)
        total = jnp.sum(
            do_ref[:, piece].astype(jnp.float32) * out_ref[:, piece].astype(jnp.float32),
            axis=1, keepdims=True,
        )
        table = jnp.where(lane == h, total, table)
    table = table.T
    part0, part1 = lp_ref[:, 0, :], lp_ref[:, 1, :]
    highest = jnp.maximum(part0, part1)
    lse_rows = highest + jnp.log(jnp.exp(part0 - highest) + jnp.exp(part1 - highest))
    for p in range(U):
        stat_ref[p, :G, :] = lse_rows[p * G:(p + 1) * G] * LOG2_E
        stat_ref[p, G:2 * G, :] = table[p * G:(p + 1) * G]
    statb[u] = stat_ref[u]

    @pl.when(grouped)
    def _():
        for k, to, _ in peers:
            st_in(k, u, to, at(b, to)).start()


    @pl.when(grouped)
    def _():
        for j in range(1, KH):
            send_qd(j)

    def kx_in(j):
        head = cols(j * D, D)
        return rcopy(
            kv_ref.at[:, :, head], kx.at[:, :, head], qd_s.at[0], qd_r.at[j, 0], at(b, 1 - u)
        )

    def px_in(j):
        return rcopy(part.at[j], px.at[j], qd_s.at[0], st_r.at[0], at(b, 1 - u))

    @pl.when(jnp.logical_and(alone, u == 0))
    def _():
        for j in range(KH):
            kx_in(j).start()

    @pl.when(tree)
    def _():
        await_bytes(kv_ref.at[:, :, pl.ds(0, min(2, U) * KH * D)], loc_sem.at[0])

        @pl.when(has_up2)
        def _():
            pl.semaphore_wait(ready, 1)
            for j in range(soon):
                h2(j, u).start()

    @pl.when(jnp.logical_and(jnp.logical_and(tree, main_pair), has_up4))
    def _():
        pl.semaphore_wait(relay, 1)
        greet(ready, b + 2, u)

    def h2id():
        return rcopy(idb.at[0], idb.at[2], h2i_s.at[0], h2i_r.at[0], at(b + 2, u))

    def pt(j):
        return rcopy(
            kvb.at[2 * odd, :, :, cols(j * D, D)], kvb.at[1, :, :, cols(j * D, D)],
            pt_s.at[0], pt_r.at[j], at(mate, u),
        )

    def ptid():
        return rcopy(idb.at[2 * odd], idb.at[1], pti_s.at[0], pti_r.at[0], at(mate, u))

    own_id.wait()
    for k, _, frm in peers:
        id_in(k, frm, at(b, frm)).wait_recv()

    @pl.when(has_up2)
    def _():
        h2id().start()

    @pl.when(even)
    def _():
        ptid().start()

    def forward(j):
        for k, _, frm in peers:
            kv_in(k, j, frm, frm, at(b, frm)).wait_recv()

        @pl.when(has_up2)
        def _():
            for k, _, frm in peers:
                h2(j, frm).start()

        @pl.when(even)
        def _():
            pt(j).start()

    def make_bias(hop):
        for kp in range(U):
            key_ids = jnp.broadcast_to(idb[hop, kp, 0:1, :].astype(jnp.float32), (T, T)).T
            for qp in range(U):
                query_ids = idb[0, qp, 0:1, :].astype(jnp.float32)
                good = key_ids == query_ids
                if hop == 0:
                    kpos = lax.broadcasted_iota(jnp.int32, (T, T), 0) + kp * T
                    qpos = lax.broadcasted_iota(jnp.int32, (T, T), 1) + qp * T
                    good = jnp.logical_and(good, kpos <= qpos)
                bias[hop, kp * T:(kp + 1) * T, qp * T:(qp + 1) * T] = jnp.where(good, 0.0, FAR)

    make_bias(0)
    forward(0)
    if KH > 1:
        forward(1)

    @pl.when(has_up2)
    def _():
        for j in range(soon, KH):
            h2(j, u).start()

    @pl.when(has_down2)
    def _():
        h2id().wait_recv()
        make_bias(2)

        @pl.when(odd == 1)
        def _():
            ptid().start()

    def arrive2(j):
        @pl.when(has_down2)
        def _():
            await_bytes(kvb.at[2, :, :, cols(j * D, D)], h2_r.at[j])

            @pl.when(odd == 1)
            def _():
                pt(j).start()

    @pl.when(b >= 1)
    def _():
        ptid().wait_recv()
        make_bias(1)

    @pl.when(grouped)
    def _():
        await_bytes(qdb.at[:, rows(u), :], loc_sem.at[6])
        for k, _, frm in peers:
            st_in(k, frm, frm, at(b, frm)).wait_recv()

    for j in range(2, KH):
        forward(j)
    arrive2(0)

    tile = min(TILE, R)
    steps = R // tile
    per = tile // T if tile >= T else 1

    def stat_row(row, qt):
        parts = [statb[qt * per + i, pl.ds(row, 1), :] for i in range(per)]
        return parts[0] if per == 1 else jnp.concatenate(parts, axis=1)

    def hop_grads(hop, j, acc):
        def key_step(kt, _):
            krow = pl.ds(pl.multiple_of(kt * tile, tile), tile)
            kc = kvb[hop, 0, krow, cols(j * D, D)]
            vc = kvb[hop, 1, krow, cols(j * D, D)]

            def query_step(qt, carry):
                dk, dv = carry
                qrow = pl.ds(pl.multiple_of(qt * tile, tile), tile)
                heads = [cols(j * GD + g * D, D) for g in range(GROUP)]
                weights, score_grads = [], []
                for g in range(GROUP):
                    lse = stat_row(j * GROUP + g, qt)
                    delta = stat_row(G + j * GROUP + g, qt)
                    w = jnp.exp2(
                        dot_nt(kc, qdb[0, qrow, heads[g]]) * (scale * LOG2_E) - lse + bias[hop, krow, qrow]
                    )
                    ds = w * (dot_nt(vc, qdb[1, qrow, heads[g]]) - delta)
                    score_grads.append(ds.astype(jnp.bfloat16))
                    weights.append(w.astype(jnp.bfloat16))
                queries = jnp.concatenate([qdb[0, qrow, heads[g]] for g in range(GROUP)], axis=0)
                cotangents = jnp.concatenate([qdb[1, qrow, heads[g]] for g in range(GROUP)], axis=0)
                dv = dot_nn(jnp.concatenate(weights, axis=1), cotangents) + dv
                dk = dot_nn(jnp.concatenate(score_grads, axis=1), queries) + dk
                for g in range(GROUP):
                    dqacc[qrow, g * D:(g + 1) * D] += dot_tn(score_grads[g], kc)
                return dk, dv

            if steps == 1:
                dk, dv = query_step(0, (0.0, 0.0))
            else:
                zero = jnp.zeros((tile, D), jnp.float32)
                dk, dv = lax.fori_loop(0, steps, query_step, (zero, zero))
            acc[j, 0, krow, :] = (dk * scale).astype(acc.dtype)
            acc[j, 1, krow, :] = dv.astype(acc.dtype)
            return 0

        if steps == 1:
            key_step(0, 0)
        else:
            lax.fori_loop(0, steps, key_step, 0)

    def give1(j):
        return rcopy(ret1.at[j], in1.at[j], r1_s.at[0], kv_r.at[j, 0], at(mate, u))

    def give2(j):
        return rcopy(ret2.at[j], in2.at[j], r2_s.at[0], r2_r.at[j], at(b - 2, u))

    def give2_part(which):
        return rcopy(
            ret2.at[KH - 1, which], in2.at[KH - 1, which],
            r2_s.at[0], r2_r.at[KH - 1 + which], at(b - 2, u),
        )

    def straight(j, place):
        return rcopy(
            ret2.at[j, :, rows(place), :], in2.at[j, :, rows(u), :],
            r2_s.at[0], r2_r.at[j], at(0, place),
        )

    def oq(k, j, place, dev):
        return rcopy(
            dqs.at[j, rows(place), :], dq_ref.at[:, cols((u * KH + j) * GD, GD)],
            oq_s.at[k - 1], oq_r.at[k - 1], dev,
        )

    def okv(k, j, place, dev):
        return rcopy(
            dkvs.at[j, :, rows(place), :], dkv_ref.at[:, :, cols((u * KH + j) * D, D)],
            okv_s.at[k - 1], okv_r.at[k - 1], dev,
        )

    def compute(j):
        for k, _, frm in peers:
            await_bytes(qdb.at[:, rows(frm), cols(j * GD, GD)], qd_r.at[j, k - 1])
        dqacc[...] = jnp.zeros_like(dqacc)

        @pl.when(b >= 1)
        def _():
            pt(j).wait_recv()
            hop_grads(1, j, ret1)
            give1(j).start()

        @pl.when(j + 1 < KH)
        def _():
            arrive2(jnp.minimum(j + 1, KH - 1))

        @pl.when(has_down2)
        def _():
            hop_grads(2, j, acc2)

        @pl.when(even)
        def _():
            stage_a(j)

        hop_grads(0, j, acc0)

        dqs[j] = (dqacc[...] * scale).astype(jnp.bfloat16)
        for k, to, _ in peers:
            oq(k, j, to, at(b, to)).start()
        dq_ref[:, cols((u * KH + j) * GD, GD)] = dqs[j, rows(u), :]

        @pl.when(odd == 1)
        def _():
            stage_a(j)

    def stage_a(j):
        @pl.when(jnp.logical_and(odd == 1, has_down2))
        def _():
            give1(j).wait_recv()
            ret2[j] = (acc2[j] + in1[j].astype(jnp.float32)).astype(jnp.bfloat16)

        @pl.when(jnp.logical_and(even, has_down2))
        def _():
            ret2[j] = acc2[j].astype(jnp.bfloat16)

        to_alone = jnp.logical_and(b == 2, U == 2)

        to_grouped = jnp.logical_and(has_down2, jnp.logical_not(to_alone))

        @pl.when(jnp.logical_and(to_grouped, j < KH - 1))
        def _():
            give2(j).start()

        @pl.when(jnp.logical_and(to_grouped, j == KH - 1))
        def _():
            for which in range(2):
                give2_part(which).start()

        @pl.when(to_alone)
        def _():
            straight(j, u).start()
            straight(j, 1 - u).start()

    def stage_b(j):
        @pl.when(even)
        def _():
            give1(j).wait_recv()
            acc0[j] += in1[j].astype(jnp.float32)

        @pl.when(has_up2)
        def _():
            give2(j).wait_recv()
            acc0[j] += in2[j].astype(jnp.float32)

        dkvs[j] = acc0[j].astype(jnp.bfloat16)
        for k, to, _ in peers:
            okv(k, j, to, at(b, to)).start()
        dkv_ref[:, :, cols((u * KH + j) * D, D)] = dkvs[j, :, rows(u), :]

    def stage_b_last():
        j = KH - 1

        @pl.when(even)
        def _():
            give1(j).wait_recv()
            acc0[j] += in1[j].astype(jnp.float32)

        for which in range(2):
            @pl.when(has_up2)
            def _():
                give2_part(which).wait_recv()
                acc0[j, which] += in2[j, which].astype(jnp.float32)

            dkvs[j, which] = acc0[j, which].astype(jnp.bfloat16)
            head = cols((u * KH + j) * D, D)
            for k, to, _ in peers:
                rcopy(
                    dkvs.at[j, which, rows(to), :], dkv_ref.at[which, :, head],
                    okv_s.at[k - 1], okv_r.at[k - 1], at(b, to),
                ).start()
            dkv_ref[which, :, head] = dkvs[j, which, rows(u), :]

    def head_step(j, _):
        compute(j)
        return 0

    def alone_block(h, kc, vc, mask):
        heads = [cols(h * GD + g * D, D) for g in range(GROUP)]
        plane = h // KH
        row = (h - plane * KH) * GROUP
        weights, score_grads = [], []
        for g in range(GROUP):
            lse = stat_ref[plane, pl.ds(row + g, 1), :]
            delta = stat_ref[plane, pl.ds(G + row + g, 1), :]
            w = jnp.exp2(dot_nt(kc, q_ref[:, heads[g]]) * (scale * LOG2_E) - lse + mask)
            ds = w * (dot_nt(vc, do_ref[:, heads[g]]) - delta)
            score_grads.append(ds.astype(jnp.bfloat16))
            weights.append(w.astype(jnp.bfloat16))
        queries = jnp.concatenate([q_ref[:, c] for c in heads], axis=0)
        cotangents = jnp.concatenate([do_ref[:, c] for c in heads], axis=0)
        dv = dot_nn(jnp.concatenate(weights, axis=1), cotangents)
        dk = dot_nn(jnp.concatenate(score_grads, axis=1), queries) * scale
        return dk, dv, [dot_tn(ds, kc) * scale for ds in score_grads]

    def alone_own(j, _):
        for side in range(2):
            h = (u if side == 0 else 1 - u) * KH + j
            head = cols(h * D, D)
            dk, dv, dq = alone_block(
                h, kv_ref[0, :, head], kv_ref[1, :, head], bias[0, rows(u), rows(u)]
            )
            for g in range(GROUP):
                dqt[side, j, :, g * D:(g + 1) * D] = dq[g]
            if side == 0:
                acc0[j, 0, rows(u), :] = dk
                acc0[j, 1, rows(u), :] = dv
            else:
                loc1[j, 0] = dk
                loc1[j, 1] = dv
        return 0

    def alone_store(j, _):
        for side in range(2):
            h = (u if side == 0 else 1 - u) * KH + j
            dq_ref[:, cols(h * GD, GD)] = dqt[side, j].astype(jnp.bfloat16)
        return 0

    def alone_near(j, _):
        head = cols(j * D, D)
        dk, dv, dq = alone_block(
            KH + j, kvb[0, 0, rows(0), head], kvb[0, 1, rows(0), head], bias[0, rows(0), rows(1)]
        )
        for g in range(GROUP):
            dqt[0, j, :, g * D:(g + 1) * D] += dq[g]
        acc0[j, 0, rows(0), :] = dk
        acc0[j, 1, rows(0), :] = dv
        return 0

    def alone_far(j, _):
        head = cols(j * D, D)
        kx_in(j).wait_recv()
        dk, dv, dq = alone_block(j, kx[0, :, head], kx[1, :, head], bias[0, rows(0), rows(1)])
        part[j, 0] = dk.astype(jnp.bfloat16)
        part[j, 1] = dv.astype(jnp.bfloat16)
        px_in(j).start()
        for g in range(GROUP):
            dqt[1, j, :, g * D:(g + 1) * D] += dq[g]
        return 0

    def alone_merge(j, _):
        give1(j).wait_recv()
        acc0[j] += in1[j].astype(jnp.float32)
        dkvs[j] = acc0[j].astype(jnp.bfloat16)
        okv(1, j, 1 - u, at(b, 1 - u)).start()
        return 0

    def alone_finish(j, _):
        mine = cols((u * KH + j) * D, D)
        other = cols(((1 - u) * KH + j) * D, D)

        @pl.when(has_up2)
        def _():
            await_bytes(in2.at[j], r2_r.at[j])
            acc0[j, :, rows(u), :] += in2[j, :, rows(u), :].astype(jnp.float32)
            loc1[j] += in2[j, :, rows(1 - u), :].astype(jnp.float32)

        dkv_ref[:, :, mine] = acc0[j, :, rows(u), :].astype(jnp.bfloat16)
        dkv_ref[:, :, other] = (dkv_ref[:, :, other].astype(jnp.float32) + loc1[j]).astype(jnp.bfloat16)
        return 0

    @pl.when(grouped)
    def _():
        lax.fori_loop(0, KH, head_step, 0)

        def last_step(j, _):
            stage_b(j)
            return 0

        lax.fori_loop(0, KH - 1, last_step, 0)
        stage_b_last()

    if U == 2:
        @pl.when(alone)
        def _():
            load_q.wait()
            lax.fori_loop(0, KH, alone_own, 0)

            @pl.when(u == 0)
            def _():
                for j in range(KH):
                    acc0[j, :, rows(1), :] = jnp.zeros((2, T, D), jnp.float32)

            @pl.when(u == 1)
            def _():
                lax.fori_loop(0, KH, alone_near, 0)
                lax.fori_loop(0, KH, alone_far, 0)

            lax.fori_loop(0, KH, alone_merge, 0)
            lax.fori_loop(0, KH, alone_store, 0)

            @pl.when(u == 0)
            def _():
                await_bytes(px, st_r.at[0])
                for j in range(KH):
                    acc0[j, :, rows(0), :] += px[j].astype(jnp.float32)

            await_bytes(dkv_ref.at[:, :, cols((1 - u) * KH * D, KH * D)], okv_r.at[0])
            lax.fori_loop(0, KH, alone_finish, 0)

            @pl.when(u == 0)
            def _():
                await_bytes(kx, qd_s.at[0])

            @pl.when(u == 1)
            def _():
                await_bytes(part, qd_s.at[0])

    for k, to, _ in peers:
        id_in(k, u, at(b, to)).wait_send()
        await_bytes(kv_ref.at[:, :, cols(to * KH * D, KH * D)], kv_s.at[k - 1])

    @pl.when(grouped)
    def _():
        for k, to, _ in peers:
            st_in(k, u, to, at(b, to)).wait_send()
            await_bytes(qdb.at[:, rows(0), :], qd_s.at[k - 1])

    @pl.when(has_up2)
    def _():
        h2id().wait_send()
        await_bytes(kvb.at[0], h2_s.at[0])

    @pl.when(sends_mate)
    def _():
        ptid().wait_send()
        await_bytes(kvb.at[0], pt_s.at[0])

    @pl.when(b >= 1)
    def _():
        await_bytes(ret1, r1_s.at[0])

    @pl.when(has_down2)
    def _():
        await_bytes(ret2, r2_s.at[0])

    for k, to, _ in peers:
        await_bytes(dkvs.at[:, :, rows(to), :], okv_s.at[k - 1])

    @pl.when(grouped)
    def _():
        for k, to, frm in peers:
            await_bytes(dqs.at[:, rows(to), :], oq_s.at[k - 1])
            await_bytes(dq_ref.at[:, cols(frm * KH * GD, KH * GD)], oq_r.at[k - 1])
            await_bytes(dkv_ref.at[:, :, cols(frm * KH * D, KH * D)], okv_r.at[k - 1])


def close_kernel(q_in, kv_in, q_out, k_out, v_out, sem):
    half = q_in.shape[0] // 2
    moves = [
        (q_in.at[pl.ds(0, half)], q_out.at[pl.ds(0, half)]),
        (q_in.at[pl.ds(half, half)], q_out.at[pl.ds(half, half)]),
        (kv_in.at[0], k_out),
        (kv_in.at[1], v_out),
    ]
    copies = [pltpu.make_async_copy(src, dst, sem.at[i]) for i, (src, dst) in enumerate(moves)]
    for copy in copies:
        copy.start()
    for copy in copies:
        copy.wait()


def per_device(uly_count, blk_count, q, k, v, out, grad, lse_parts, segment_ids):
    U, B = uly_count, blk_count
    T = q.shape[0]
    R = T * U
    KH = KEY_VALUE_HEADS // U
    G = KH * GROUP
    D = HEAD_SIZE
    GD = GROUP * D
    stat_rows = -(-2 * G // 8) * 8
    parts = lse_parts.transpose(1, 2, 0)
    ids = segment_ids.reshape(1, T)
    bf, f32 = jnp.bfloat16, jnp.float32
    n = max(U - 1, 1)
    dma = pltpu.SemaphoreType.DMA
    sems = []
    for send, recv in [
        ((n,), (KH, n)), ((n,), (KH, n)), ((n,), (n,)), ((n,), (n,)),
        ((1,), (KH,)), ((1,), (1,)), ((1,), (KH,)), ((1,), (1,)),
        ((1,), None), ((1,), (KH + 1,)), ((n,), (n,)), ((n,), (n,)),
    ]:
        sems += [dma(shape) for shape in (send, recv) if shape is not None]
    vm = pltpu.VMEM
    in_vmem = pl.BlockSpec(memory_space=pltpu.VMEM)
    in_hbm = pl.BlockSpec(memory_space=pltpu.HBM)
    results = pl.pallas_call(
        functools.partial(kernel, U, B),
        out_shape=(vm(q.shape, bf), vm((2,) + k.shape, bf)),
        in_specs=[in_hbm] * 7,
        out_specs=(in_vmem, in_vmem),
        scratch_shapes=[
            vm((2, R, G * D), bf),
            vm((3, 2, R, KH * D), bf),
            vm((U, stat_rows, T), f32),
            vm((3, U, 1, T), jnp.int32),
            vm((3, R, R), f32),
            vm((R, GROUP * D), f32),
            vm((KH, 2, R, D), f32),
            vm((KH, 2, R, D), f32),
            vm((KH, R, GROUP * D), bf),
            vm((KH, 2, R, D), bf),
            vm((KH, 2, R, D), bf),
            vm((KH, 2, R, D), bf),
            vm((KH, 2, R, D), bf),
            vm((KH, 2, R, D), bf),
            vm(q.shape, bf),
            vm((2,) + k.shape, bf),
            vm(q.shape, bf),
            vm(parts.shape, f32),
            vm((1, T), jnp.int32),
            vm((U, stat_rows, T), f32),
            vm(q.shape, bf),
            vm((2, T, KH * D), bf),
            vm((KH, 2, T, D), f32),
            vm((KH, 2, T, D), bf),
            vm((KH, 2, T, D), bf),
            vm((2, KH, T, GD), f32),
            dma((9,)),
            pltpu.SemaphoreType.REGULAR,
            pltpu.SemaphoreType.REGULAR,
        ] + sems,
        compiler_params=pltpu.CompilerParams(
            collective_id=0, has_side_effects=True, vmem_limit_bytes=56 << 20
        ),
    )(q, grad, k, v, out, parts, ids)
    results = [pltpu.with_memory_space_constraint(r, pltpu.VMEM) for r in results]
    return pl.pallas_call(
        close_kernel,
        out_shape=tuple(jax.ShapeDtypeStruct(r.shape, r.dtype) for r in (q, k, v)),
        in_specs=[in_vmem] * 2,
        out_specs=(in_hbm,) * 3,
        scratch_shapes=[dma((4,))],
        compiler_params=pltpu.CompilerParams(vmem_limit_bytes=8 << 20),
    )(*results)


def solution(mesh):
    spec = P(("blk", "uly"), None)
    body = functools.partial(per_device, mesh.shape["uly"], mesh.shape["blk"])
    return jax.shard_map(
        body,
        mesh=mesh,
        in_specs=(spec, spec, spec, spec, spec, P(("blk", "uly"), None, None), P(("blk", "uly"))),
        out_specs=(spec, spec, spec),
        check_vma=False,
    )
```
